16 devices in a mesh: dp: 4 (over z, y), tp: 4 (over x, core).
Axes of the slice: x: 2, y: 2, z: 2, core: 2. Of those that a mesh axis runs over, the one named last changes fastest.
Arguments:
- x_steps: bfloat16 [4, 4096, 512], P(None, 'dp'), parts along dimension 1
- conv_state: bfloat16 [4096, 1024, 3], P('dp', 'tp'), parts along dimension 0
- ssm_state: float32 [4096, 1024, 16], P('dp', 'tp'), parts along dimension 0
- expert_ids: int32 [4, 4096, 1], P(None, 'dp'), parts along dimension 1
- g_in: bfloat16 [512], replicated
- w_in: bfloat16 [512, 2, 1024], P(None, None, 'tp')
- conv_w: bfloat16 [1024, 4], P('tp')
- conv_b: bfloat16 [1024], P('tp')
- w_xp: bfloat16 [1024, 64], P('tp')
- g_dt: bfloat16 [32], replicated
- g_b: bfloat16 [16], replicated
- g_c: bfloat16 [16], replicated
- w_dt: bfloat16 [32, 1024], P(None, 'tp')
- b_dt: bfloat16 [1024], P('tp')
- a_log: float32 [1024, 16], P('tp')
- d_skip: float32 [1024], P('tp')
- w_out: bfloat16 [1024, 512], P('tp')
- g_ff: bfloat16 [512], replicated
- w_router: bfloat16 [512, 16], replicated
- w_gate: bfloat16 [16, 512, 2048], P(None, None, 'tp')
- w_up: bfloat16 [16, 512, 2048], P(None, None, 'tp')
- w_down: bfloat16 [16, 2048, 512], P(None, 'tp')
Outputs:
- output 1: bfloat16 [4, 4096, 512], P(None, 'dp'), parts along dimension 1
- output 2: bfloat16 [4096, 1024, 3], P('dp', 'tp'), parts along dimension 0
- output 3: float32 [4096, 1024, 16], P('dp', 'tp'), parts along dimension 0
There are 4 independent parts. The reference program is written for one: setup_inputs(seed, part) draws one part's arguments, and reference() takes and returns one part's arrays. A program takes and returns all parts, laid end to end along the dimension named above; an argument that names none is the same for every part.
All inputs are finite; a program needn't handle non-finite values.
Results may differ from the reference program's by a relative error of at most 0.0141754.
Values are sent between devices in bfloat16 or wider.
A program may use at most 1 GiB of HBM per device.

```python
import jax
import jax.numpy as jnp
from jax import lax

D_MODEL = 512
INNER = 1024
STATE_DIM = 16
DT_RANK = 32
FFN_DIM = 2048
EXPERTS = 16
TOP_K = 1
BATCH_SIZE = 1024
NUM_STEPS = 4
CONV_WIDTH = 4
EPSILON = 1e-6


def gauss_draw(rng_key, arr_shape, std_scale):
    return jax.random.normal(rng_key, arr_shape, jnp.float32) * std_scale


def range_draw(rng_key, arr_shape, lower_end, upper_end):
    return jax.random.uniform(rng_key, arr_shape, jnp.float32, lower_end, upper_end)


def draw_routes(rng_key):
    key_jitter, key_skew = jax.random.split(rng_key)
    route_jitter = jax.random.randint(key_jitter, (NUM_STEPS, BATCH_SIZE, EXPERTS), 0, 64)
    expert_skew = jax.random.randint(key_skew, (EXPERTS,), 0, 96)
    cover_mask = (jnp.arange(NUM_STEPS)[:, None, None] == 0) & (jnp.arange(BATCH_SIZE)[None, :, None] == jnp.arange(EXPERTS)[None, None, :])
    scores = route_jitter + expert_skew[None, None, :] + jnp.where(cover_mask, 1000, 0)
    scores = scores * EXPERTS + jnp.arange(EXPERTS)[None, None, :]
    return lax.top_k(scores, TOP_K)[1].astype(jnp.int32)


def setup_inputs(seed: int = 0, part: int = 0) -> dict:
    base_key = jax.random.key(seed)
    part_keys = jax.random.split(jax.random.fold_in(base_key, part), 4)
    shared_keys = jax.random.split(base_key, 18)
    return {
        "x_steps": gauss_draw(part_keys[0], (NUM_STEPS, BATCH_SIZE, D_MODEL), 1.0).astype(jnp.bfloat16),
        "conv_state": gauss_draw(part_keys[1], (BATCH_SIZE, INNER, CONV_WIDTH - 1), 1.0).astype(jnp.bfloat16),
        "ssm_state": gauss_draw(part_keys[2], (BATCH_SIZE, INNER, STATE_DIM), 0.2),
        "expert_ids": draw_routes(part_keys[3]),
        "g_in": range_draw(shared_keys[0], (D_MODEL,), 0.4, 1.6).astype(jnp.bfloat16),
        "w_in": gauss_draw(shared_keys[1], (D_MODEL, 2, INNER), D_MODEL ** -0.5).astype(jnp.bfloat16),
        "conv_w": gauss_draw(shared_keys[2], (INNER, CONV_WIDTH), 0.5).astype(jnp.bfloat16),
        "conv_b": gauss_draw(shared_keys[3], (INNER,), 0.5).astype(jnp.bfloat16),
        "w_xp": gauss_draw(shared_keys[4], (INNER, DT_RANK + 2 * STATE_DIM), INNER ** -0.5).astype(jnp.bfloat16),
        "g_dt": range_draw(shared_keys[5], (DT_RANK,), 0.4, 1.6).astype(jnp.bfloat16),
        "g_b": range_draw(shared_keys[6], (STATE_DIM,), 0.4, 1.6).astype(jnp.bfloat16),
        "g_c": range_draw(shared_keys[7], (STATE_DIM,), 0.4, 1.6).astype(jnp.bfloat16),
        "w_dt": gauss_draw(shared_keys[8], (DT_RANK, INNER), 0.8 * DT_RANK ** -0.5).astype(jnp.bfloat16),
        "b_dt": (gauss_draw(shared_keys[9], (INNER,), 0.3) - 2.25).astype(jnp.bfloat16),
        "a_log": range_draw(shared_keys[10], (INNER, STATE_DIM), -0.7, 0.7),
        "d_skip": range_draw(shared_keys[11], (INNER,), 0.5, 1.5),
        "w_out": gauss_draw(shared_keys[12], (INNER, D_MODEL), INNER ** -0.5).astype(jnp.bfloat16),
        "g_ff": range_draw(shared_keys[13], (D_MODEL,), 0.4, 1.6).astype(jnp.bfloat16),
        "w_router": gauss_draw(shared_keys[14], (D_MODEL, EXPERTS), D_MODEL ** -0.5).astype(jnp.bfloat16),
        "w_gate": gauss_draw(shared_keys[15], (EXPERTS, D_MODEL, FFN_DIM), D_MODEL ** -0.5).astype(jnp.bfloat16),
        "w_up": gauss_draw(shared_keys[16], (EXPERTS, D_MODEL, FFN_DIM), D_MODEL ** -0.5).astype(jnp.bfloat16),
        "w_down": gauss_draw(shared_keys[17], (EXPERTS, FFN_DIM, D_MODEL), EXPERTS * (TOP_K * FFN_DIM) ** -0.5).astype(jnp.bfloat16),
    }


def rms_norm(tensor_in, gain_vec):
    in_f32 = tensor_in.astype(jnp.float32)
    return in_f32 * lax.rsqrt(jnp.mean(in_f32 * in_f32, axis=-1, keepdims=True) + EPSILON) * gain_vec.astype(jnp.float32)


def reference(x_steps, conv_state, ssm_state, expert_ids, g_in, w_in, conv_w, conv_b, w_xp, g_dt, g_b, g_c, w_dt, b_dt, a_log, d_skip, w_out, g_ff, w_router, w_gate, w_up, w_down):
    a_mat = -jnp.exp(a_log)
    w_in_flat = w_in.reshape(D_MODEL, 2 * INNER)

    def expert_body(moe_acc, expert_w):
        w_gate_e, w_up_e, w_down_e, coef_e, moe_in = expert_w
        gate_h = jnp.dot(moe_in, w_gate_e, preferred_element_type=jnp.float32)
        up_h = jnp.dot(moe_in, w_up_e, preferred_element_type=jnp.float32)
        hidden = (jax.nn.silu(gate_h) * up_h).astype(jnp.bfloat16)
        return moe_acc + coef_e[:, None] * jnp.dot(hidden, w_down_e, preferred_element_type=jnp.float32), None

    def one_step(state_pair, step_in):
        conv_st, ssm_st = state_pair
        x_now, ids_now = step_in
        norm_in = rms_norm(x_now, g_in).astype(jnp.bfloat16)
        proj_xz = jnp.dot(norm_in, w_in_flat, preferred_element_type=jnp.float32).astype(jnp.bfloat16).reshape(BATCH_SIZE, 2, INNER)
        x_inner = proj_xz[:, 0]
        z_gate = proj_xz[:, 1]
        conv_win = jnp.concatenate([conv_st, x_inner[:, :, None]], axis=2)
        conv_pre = jnp.sum(conv_win.astype(jnp.float32) * conv_w.astype(jnp.float32)[None], axis=2) + conv_b.astype(jnp.float32)[None]
        x_conv = jax.nn.silu(conv_pre).astype(jnp.bfloat16)
        proj_sum = jnp.dot(x_conv, w_xp, preferred_element_type=jnp.float32)
        dt_low = rms_norm(proj_sum[:, :DT_RANK], g_dt)
        b_vec = rms_norm(proj_sum[:, DT_RANK:DT_RANK + STATE_DIM], g_b)
        c_vec = rms_norm(proj_sum[:, DT_RANK + STATE_DIM:], g_c)
        delta_t = jax.nn.softplus(jnp.dot(dt_low.astype(jnp.bfloat16), w_dt, preferred_element_type=jnp.float32) + b_dt.astype(jnp.float32)[None])
        xc_f32 = x_conv.astype(jnp.float32)
        new_ssm = jnp.exp(delta_t[:, :, None] * a_mat[None]) * ssm_st + (delta_t * xc_f32)[:, :, None] * b_vec[:, None, :]
        y_gated = (jnp.sum(new_ssm * c_vec[:, None, :], axis=2) + d_skip[None] * xc_f32) * jax.nn.silu(z_gate.astype(jnp.float32))
        mix_out = jnp.dot(y_gated.astype(jnp.bfloat16), w_out, preferred_element_type=jnp.float32)
        resid_mid = (x_now.astype(jnp.float32) + mix_out).astype(jnp.bfloat16)
        moe_in = rms_norm(resid_mid, g_ff).astype(jnp.bfloat16)
        route_prob = jax.nn.softmax(jnp.dot(moe_in, w_router, preferred_element_type=jnp.float32), axis=-1)
        pick_count = jnp.sum((ids_now[:, :, None] == jnp.arange(EXPERTS)[None, None, :]).astype(jnp.float32), axis=1)
        combine_w = route_prob * pick_count
        moe_stack = jnp.broadcast_to(moe_in[None], (EXPERTS, BATCH_SIZE, D_MODEL))
        moe_out, _ = lax.scan(expert_body, jnp.zeros((BATCH_SIZE, D_MODEL), jnp.float32), (w_gate, w_up, w_down, combine_w.T, moe_stack))
        out_now = (resid_mid.astype(jnp.float32) + moe_out).astype(jnp.bfloat16)
        return (conv_win[:, :, 1:], new_ssm), out_now

    final_pair, y_steps = lax.scan(one_step, (conv_state, ssm_state), (x_steps, expert_ids))
    return y_steps, final_pair[0], final_pair[1]
```

```python
import functools

import jax
import jax.numpy as jnp
from jax import lax
from jax.experimental import pallas as pl
from jax.experimental.pallas import tpu as pltpu
from jax.sharding import PartitionSpec as P

EPSILON = 1e-6
CHUNKS = 4
ROW_ALIGN = 16
TILE = 128
F32 = jnp.float32
BF16 = jnp.bfloat16
HBM = pl.BlockSpec(memory_space=pl.ANY)


def whole(shape):
    return pl.BlockSpec(shape, lambda *_: (0,) * len(shape))


def params(**kw):
    return pltpu.CompilerParams(vmem_limit_bytes=56 * 1024 * 1024, **kw)


def silu(v):
    return v * jax.nn.sigmoid(v)


def routes_kernel(ids_ref, pos_ref, tab_ref):
    chunks, _, tokens = ids_ref.shape
    experts = tab_ref.shape[1]
    upper = (lax.broadcasted_iota(jnp.int32, (tokens, tokens), 0) <= lax.broadcasted_iota(jnp.int32, (tokens, tokens), 1)).astype(F32).astype(BF16)
    before = (lax.broadcasted_iota(jnp.int32, (experts, experts), 1) < lax.broadcasted_iota(jnp.int32, (experts, experts), 0)).astype(F32)
    lane = lax.broadcasted_iota(jnp.int32, (experts, 128), 1)
    for c in range(chunks):
        hit = lax.broadcasted_iota(jnp.int32, (experts, tokens), 0) == ids_ref[c]
        hot = hit.astype(F32)
        rank = jnp.dot(hot.astype(BF16), upper, preferred_element_type=F32)
        count = jnp.sum(hot, axis=1, keepdims=True)
        blocks = jnp.floor((count + (ROW_ALIGN - 1)) * (1.0 / ROW_ALIGN))
        start = ROW_ALIGN * jnp.dot(before.astype(BF16), jnp.broadcast_to(blocks, (experts, 128)).astype(BF16), preferred_element_type=F32)
        pos_ref[c] = jnp.sum(hot * (start[:, :1] + rank - 1.0), axis=0, keepdims=True).astype(jnp.int32)
        tab_ref[c] = jnp.where(lane == 0, start, jnp.broadcast_to(count, (experts, 128))).astype(jnp.int32)


def in_kernel(x_ref, cs_ref, g_ref, win_ref, cw_ref, cb_ref, wxp_ref, *rest):
    xc_ref, z_ref, pk_ref, ps_ref, co_ref = rest[-5:]
    steps, rows, d_model = x_ref.shape
    inner = cs_ref.shape[2]
    core = lax.rem(lax.axis_index("tp"), 2)
    gain = g_ref[...].astype(F32)
    seq = [cs_ref[j].astype(F32) for j in range(3)]
    part = []
    for s in range(steps):
        x = x_ref[s].astype(F32)
        n = (x * lax.rsqrt(jnp.mean(x * x, axis=-1, keepdims=True) + EPSILON) * gain).astype(BF16)
        xz = jnp.dot(n, win_ref[...], preferred_element_type=F32).astype(BF16)
        z_ref[s] = xz[:, inner:]
        xi = xz[:, :inner]
        if s > 0:
            co_ref[s - 1] = xi
        seq.append(xi.astype(F32))
        acc = seq[s] * cw_ref[0:1, :].astype(F32)
        for j in range(1, 4):
            acc = acc + seq[s + j] * cw_ref[j:j + 1, :].astype(F32)
        xc = silu(acc + cb_ref[...].astype(F32)).astype(BF16)
        xc_ref[s] = xc
        part.append(lax.dot_general(xc, wxp_ref[...], (((1,), (1,)), ((), ())), preferred_element_type=F32))
    low = jnp.concatenate(part[:2], axis=1)
    high = jnp.concatenate(part[2:], axis=1)
    pk_ref[...] = jnp.where(core == 0, low, high)
    ps_ref[...] = jnp.where(core == 0, high, low)


def scan_kernel(po_ref, pb_ref, xc_ref, z_ref, h_ref, g4_ref, wdt_ref, bdt_ref, alog_ref, dskip_ref, wout_ref, *rest):
    mk_ref, ms_ref, ho_ref, wdt4, norm_s, delta_s, dx_s, y_s = rest[-8:]
    steps, rows, inner = xc_ref.shape
    state = alog_ref.shape[0]
    rank = wdt_ref.shape[0]
    width = rank + 2 * state
    core = lax.rem(lax.axis_index("tp"), 2)

    @pl.when((pl.program_id(0) == 0) & (pl.program_id(1) == 0))
    def _():
        wdt4[...] = jnp.zeros_like(wdt4)
        for s in range(steps):
            wdt4[s * width:s * width + rank, s * inner:(s + 1) * inner] = wdt_ref[...]

    lanes = steps * width

    def group(v):
        step, col = v // width, v % width
        return step * 4 + (col >= rank).astype(jnp.int32) + (col >= rank + state).astype(jnp.int32)

    @pl.when(pl.program_id(1) == 0)
    def _():
        own, sib = po_ref[...], pb_ref[...]
        p = jnp.concatenate([jnp.where(core == 0, own, sib), jnp.where(core == 0, sib, own)], axis=1)
        gi = group(lax.broadcasted_iota(jnp.int32, (lanes, lanes), 0))
        gj = group(lax.broadcasted_iota(jnp.int32, (lanes, lanes), 1))
        inv = jnp.where(lax.rem(gj, 4) == 0, 1.0 / rank, 1.0 / state)
        mean = jnp.dot(p * p, jnp.where(gi == gj, inv, 0.0), precision=lax.Precision.HIGHEST, preferred_element_type=F32)
        norm = p * lax.rsqrt(mean + EPSILON) * g4_ref[...]
        norm_s[...] = norm
        pre = jnp.dot(norm.astype(BF16), wdt4[...], preferred_element_type=F32)
        bias = bdt_ref[...].astype(F32)
        for s in range(steps):
            v = pre[:, s * inner:(s + 1) * inner] + bias
            delta = jnp.maximum(v, 0.0) + jnp.log1p(jnp.exp(-jnp.abs(v)))
            xc = xc_ref[s].astype(F32)
            for l in range(inner // 128):
                cut = slice(l * 128, (l + 1) * 128)
                delta_s[l, s] = delta[:, cut]
                dx_s[l, s] = delta[:, cut] * xc[:, cut]

    lt = pl.program_id(1)
    a_neg = -jnp.exp(alog_ref[...])

    def tile(i, carry):
        r = pl.multiple_of(i * 8, 8)
        q = norm_s[pl.ds(r, 8), :]
        dl = [delta_s[lt, s, pl.ds(r, 8), :] for s in range(steps)]
        dx = [dx_s[lt, s, pl.ds(r, 8), :] for s in range(steps)]
        ys = [jnp.zeros((8, 128), F32) for _ in range(steps)]
        for n in range(state):
            a = a_neg[n:n + 1, :]
            h = h_ref[pl.ds(r * state + n, 8, stride=state), :]
            for s in range(steps):
                b0 = s * width + rank + n
                c0 = b0 + state
                h = jnp.exp(dl[s] * a) * h + dx[s] * q[:, b0:b0 + 1]
                ys[s] = ys[s] + h * q[:, c0:c0 + 1]
            ho_ref[pl.ds(r * state + n, 8, stride=state), :] = h
        for s in range(steps):
            y_s[lt, s, pl.ds(r, 8), :] = ys[s]
        return carry

    lax.fori_loop(0, rows // 8, tile, 0)
    half = steps // 2

    @pl.when(lt == inner // 128 - 1)
    def _():
        for s in range(steps):
            xc = xc_ref[s].astype(F32)
            y = jnp.concatenate([y_s[l, s] for l in range(inner // 128)], axis=1)
            yg = ((y + dskip_ref[...] * xc) * silu(z_ref[s].astype(F32))).astype(BF16)
            out = jnp.dot(yg, wout_ref[...], preferred_element_type=F32).astype(BF16)
            mine = core == s // half

            @pl.when(mine)
            def _():
                mk_ref[s % half] = out

            @pl.when(jnp.logical_not(mine))
            def _():
                ms_ref[s % half] = out


def moe_kernel(tab_ref, pos_ref, uo_ref, ub_ref, gff_ref, wr_ref, wg_ref, wu_ref, wd_ref, ok_ref, os_ref, wg, wu, wd, sems, m_s, hot_s, in_s, out_s):
    half, rows, d_model = uo_ref.shape
    experts = wg.shape[0]
    tokens = 2 * half * rows
    slots = hot_s.shape[0]
    core = lax.rem(lax.axis_index("tp"), 2)

    def copies(e):
        return [pltpu.make_async_copy(src.at[e], dst.at[e], sems.at[k, e]) for k, (src, dst) in enumerate(((wg_ref, wg), (wu_ref, wu), (wd_ref, wd)))]

    def fetch(e, carry):
        @pl.when(tab_ref[e, 1] > 0)
        def _():
            for cp in copies(e):
                cp.start()
        return carry

    lax.fori_loop(0, experts, fetch, 0)
    gain = gff_ref[...].astype(F32)
    for k in range(2):
        src = (uo_ref, ub_ref)[k]
        first = jnp.where(core == k, 0, half * rows)
        for s in range(half):
            u = src[s].astype(F32)
            m = u * lax.rsqrt(jnp.mean(u * u, axis=-1, keepdims=True) + EPSILON) * gain
            m_s[pl.ds(pl.multiple_of(first + s * rows, rows), rows), :] = m.astype(BF16)

    pos = pos_ref[...]

    def order(i, carry):
        r = pl.multiple_of(i * 256, 256)
        hot = (lax.broadcasted_iota(jnp.int32, (256, tokens), 0) + r == pos).astype(F32).astype(BF16)
        hot_s[pl.ds(r, 256), :] = hot
        in_s[pl.ds(r, 256), :] = jnp.dot(hot, m_s[...], preferred_element_type=F32).astype(BF16)
        out_s[pl.ds(r, 256), :] = jnp.zeros((256, d_model), BF16)
        return carry

    lax.fori_loop(0, slots // 256, order, 0)
    lane = lax.broadcasted_iota(jnp.int32, (TILE, experts), 1)

    def expert(e, carry):
        count = tab_ref[e, 1]
        start = tab_ref[e, 0]

        @pl.when(count > 0)
        def _():
            for cp in copies(e):
                cp.wait()

            def tile(i, c2):
                r = pl.multiple_of(start + i * TILE, ROW_ALIGN)
                m = in_s[pl.ds(r, TILE), :]
                logits = jnp.dot(m, wr_ref[...], preferred_element_type=F32)
                ex = jnp.exp(logits - jnp.max(logits, axis=-1, keepdims=True))
                prob = jnp.sum(jnp.where(lane == e, ex, 0.0), axis=-1, keepdims=True) / jnp.sum(ex, axis=-1, keepdims=True)
                gate = jnp.dot(m, wg[e], preferred_element_type=F32)
                up = jnp.dot(m, wu[e], preferred_element_type=F32)
                q = (silu(gate) * up).astype(BF16)
                out_s[pl.ds(r, TILE), :] = (prob * jnp.dot(q, wd[e], preferred_element_type=F32)).astype(BF16)
                return c2

            lax.fori_loop(0, (count + TILE - 1) // TILE, tile, 0)
        return carry

    lax.fori_loop(0, experts, expert, 0)

    def restore(k, dst):
        first = jnp.where(core == k, 0, half * rows)
        for s in range(half):
            hot = hot_s[:, pl.ds(pl.multiple_of(first + s * rows, rows), rows)]
            got = lax.dot_general(hot, out_s[:slots, :], (((0,), (0,)), ((), ())), preferred_element_type=F32)
            dst[s] = got.astype(BF16)

    restore(0, ok_ref)
    restore(1, os_ref)


def solution(mesh):
    act_spec = P(None, "dp", None)
    state_spec = P("dp", "tp", None)
    in_specs = (act_spec, state_spec, state_spec, act_spec, P(None), P(None, None, "tp"), P("tp", None), P("tp"), P("tp", None), P(None), P(None), P(None), P(None, "tp"), P("tp"), P("tp", None), P("tp"), P("tp", None), P(None), P(None, None), P(None, None, "tp"), P(None, None, "tp"), P(None, "tp", None))
    out_specs = (act_spec, state_spec, state_spec)
    across = [(0, 2), (2, 0), (1, 3), (3, 1)]
    beside = [(0, 1), (1, 0), (2, 3), (3, 2)]

    def layer_steps(x_steps, conv_state, ssm_state, expert_ids, g_in, w_in, conv_w, conv_b, w_xp, g_dt, g_b, g_c, w_dt, b_dt, a_log, d_skip, w_out, g_ff, w_router, w_gate, w_up, w_down):
        steps, batch, d_model = x_steps.shape
        inner = w_in.shape[2]
        rank = w_dt.shape[0]
        state = a_log.shape[1]
        experts, _, ffn = w_gate.shape
        width = rank + 2 * state
        half = steps // 2
        rows = batch // CHUNKS
        tokens = steps * rows
        slots = tokens + experts * ROW_ALIGN
        core = lax.rem(lax.axis_index("tp"), 2)

        conv_t = jnp.transpose(conv_state, (2, 0, 1))
        h_rows = jnp.transpose(ssm_state, (0, 2, 1)).reshape(batch * state, inner)
        alog_t = a_log.T
        w_in_flat = w_in.reshape(d_model, 2 * inner)
        g4 = jnp.tile(jnp.concatenate([g_dt, g_b, g_c]).astype(F32), steps).reshape(1, steps * width)

        ids = expert_ids.reshape(steps, CHUNKS, rows).transpose(1, 0, 2).reshape(CHUNKS, 1, tokens)
        pos, table = pl.pallas_call(
            routes_kernel,
            out_shape=(jax.ShapeDtypeStruct((CHUNKS, 1, tokens), jnp.int32), jax.ShapeDtypeStruct((CHUNKS, experts, 128), jnp.int32)),
            compiler_params=params(),
            name="routes",
        )(ids)
        table = table[:, :, :2]

        rb = min(rows, 128)
        nb = rows // rb

        def run_in(c, conv_out):
            extra = [] if conv_out is None else [conv_out]
            return pl.pallas_call(
                in_kernel,
                grid=(nb,),
                in_specs=[
                    pl.BlockSpec((steps, rb, d_model), lambda i: (0, c * nb + i, 0)),
                    pl.BlockSpec((3, rb, inner), lambda i: (0, c * nb + i, 0)),
                    whole((1, d_model)), whole((d_model, 2 * inner)), whole((4, inner)), whole((1, inner)), whole((width, inner)),
                ] + [HBM] * len(extra),
                out_specs=[
                    pl.BlockSpec((steps, rb, inner), lambda i: (0, i, 0)),
                    pl.BlockSpec((steps, rb, inner), lambda i: (0, i, 0)),
                    pl.BlockSpec((rb, 2 * width), lambda i: (i, 0)),
                    pl.BlockSpec((rb, 2 * width), lambda i: (i, 0)),
                    pl.BlockSpec((3, rb, inner), lambda i: (0, c * nb + i, 0)),
                ],
                out_shape=[
                    jax.ShapeDtypeStruct((steps, rows, inner), BF16),
                    jax.ShapeDtypeStruct((steps, rows, inner), BF16),
                    jax.ShapeDtypeStruct((rows, 2 * width), F32),
                    jax.ShapeDtypeStruct((rows, 2 * width), F32),
                    jax.ShapeDtypeStruct((3, batch, inner), BF16),
                ],
                input_output_aliases={7: 4} if extra else {},
                compiler_params=params(),
                cost_estimate=pl.CostEstimate(flops=int(2e9 / CHUNKS), bytes_accessed=int(10e6 / CHUNKS), transcendentals=0),
                name=f"inproj{c}",
            )(x_steps, conv_t, g_in.reshape(1, -1), w_in_flat, conv_w.T, conv_b.reshape(1, -1), w_xp.T, *extra)

        hb = min(rows, 128)
        nh = rows // hb

        def run_scan(c, p_own, p_sib, xc, z, ssm_out):
            extra = [] if ssm_out is None else [ssm_out]
            return pl.pallas_call(
                scan_kernel,
                grid=(nh, inner // 128),
                in_specs=[
                    pl.BlockSpec((hb, 2 * width), lambda i, l: (i, 0)),
                    pl.BlockSpec((hb, 2 * width), lambda i, l: (i, 0)),
                    pl.BlockSpec((steps, hb, inner), lambda i, l: (0, i, 0)),
                    pl.BlockSpec((steps, hb, inner), lambda i, l: (0, i, 0)),
                    pl.BlockSpec((hb * state, 128), lambda i, l: (c * nh + i, l)),
                    whole((1, steps * width)), whole((rank, inner)), whole((1, inner)), pl.BlockSpec((state, 128), lambda i, l: (0, l)), whole((1, inner)), whole((inner, d_model)),
                ] + [HBM] * len(extra),
                out_specs=[
                    pl.BlockSpec((half, hb, d_model), lambda i, l: (0, i, 0)),
                    pl.BlockSpec((half, hb, d_model), lambda i, l: (0, i, 0)),
                    pl.BlockSpec((hb * state, 128), lambda i, l: (c * nh + i, l)),
                ],
                out_shape=[
                    jax.ShapeDtypeStruct((half, rows, d_model), BF16),
                    jax.ShapeDtypeStruct((half, rows, d_model), BF16),
                    jax.ShapeDtypeStruct((batch * state, inner), F32),
                ],
                scratch_shapes=[
                    pltpu.VMEM((steps * width, steps * inner), BF16),
                    pltpu.VMEM((hb, steps * width), F32),
                    pltpu.VMEM((inner // 128, steps, hb, 128), F32),
                    pltpu.VMEM((inner // 128, steps, hb, 128), F32),
                    pltpu.VMEM((inner // 128, steps, hb, 128), F32),
                ],
                input_output_aliases={11: 2} if extra else {},
                compiler_params=params(),
                cost_estimate=pl.CostEstimate(flops=int(6e9 / CHUNKS), bytes_accessed=int(40e6 / CHUNKS), transcendentals=0),
                name=f"scan{c}",
            )(p_own, p_sib, xc, z, h_rows, g4, w_dt, b_dt.reshape(1, -1), alog_t, d_skip.reshape(1, -1), w_out, *extra)

        def run_moe(c, u_own, u_sib):
            vmem = pl.BlockSpec(memory_space=pltpu.VMEM)
            return pl.pallas_call(
                moe_kernel,
                in_specs=[pl.BlockSpec(memory_space=pltpu.SMEM), vmem, vmem, vmem, vmem, vmem, HBM, HBM, HBM],
                out_specs=[vmem, vmem],
                out_shape=[jax.ShapeDtypeStruct((half, rows, d_model), BF16)] * 2,
                scratch_shapes=[
                    pltpu.VMEM((experts, d_model, ffn), BF16),
                    pltpu.VMEM((experts, d_model, ffn), BF16),
                    pltpu.VMEM((experts, ffn, d_model), BF16),
                    pltpu.SemaphoreType.DMA((3, experts)),
                    pltpu.VMEM((tokens, d_model), BF16),
                    pltpu.VMEM((slots, tokens), BF16),
                    pltpu.VMEM((slots + TILE, d_model), BF16),
                    pltpu.VMEM((slots + TILE, d_model), BF16),
                ],
                compiler_params=params(),
                cost_estimate=pl.CostEstimate(flops=int(12e9 / CHUNKS), bytes_accessed=int(40e6 / CHUNKS), transcendentals=0),
                name=f"moe{c}",
            )(table[c], pos[c], u_own, u_sib, g_ff.reshape(1, -1), w_router, w_gate, w_up, w_down)

        def both(keep, send, dtype):
            got = lax.ppermute(send, "tp", beside)
            chip = (keep.astype(F32) + got.astype(F32)).astype(dtype)
            return chip, lax.ppermute(chip, "tp", across)

        firsts = []
        conv_out = None
        for c in range(CHUNKS):
            xc, z, p_keep, p_send, conv_out = run_in(c, conv_out)
            chip, far = both(p_keep, p_send, F32)
            p_own = chip + far
            firsts.append((xc, z, p_own, lax.ppermute(p_own, "tp", beside)))

        mids = []
        ssm_out = None
        for c in range(CHUNKS):
            xc, z, p_own, p_sib = firsts[c]
            m_keep, m_send, ssm_out = run_scan(c, p_own, p_sib, xc, z, ssm_out)
            chip, far = both(m_keep, m_send, BF16)
            x_own = lax.dynamic_slice(x_steps, (half * core, c * rows, 0), (half, rows, d_model))
            u_own = (x_own.astype(F32) + (chip.astype(F32) + far.astype(F32))).astype(BF16)
            mids.append((u_own, lax.ppermute(u_own, "tp", beside)))

        owns, sibs = [], []
        for c in range(CHUNKS):
            u_own, u_sib = mids[c]
            o_keep, o_send = run_moe(c, u_own, u_sib)
            chip, far = both(o_keep, o_send, BF16)
            y_own = (u_own.astype(F32) + (chip.astype(F32) + far.astype(F32))).astype(BF16)
            owns.append(y_own)
            sibs.append(lax.ppermute(y_own, "tp", beside))
        own = jnp.concatenate(owns, axis=1)
        sib = jnp.concatenate(sibs, axis=1)
        y_steps = jnp.concatenate([jnp.where(core == 0, own, sib), jnp.where(core == 0, sib, own)], axis=0)
        ssm_fin = jnp.transpose(ssm_out.reshape(batch, state, inner), (0, 2, 1))
        return y_steps, jnp.transpose(conv_out, (1, 2, 0)), ssm_fin

    return jax.shard_map(layer_steps, mesh=mesh, in_specs=in_specs, out_specs=out_specs, check_vma=False)
```

```python
import functools

import jax
import jax.numpy as jnp
from jax import lax
from jax.experimental import pallas as pl
from jax.experimental.pallas import tpu as pltpu
from jax.sharding import PartitionSpec as P

EPSILON = 1e-6
CHUNKS = 4
ROW_ALIGN = 16
TILE = 128
WHOLE = 2
F32 = jnp.float32
BF16 = jnp.bfloat16
HBM = pl.BlockSpec(memory_space=pl.ANY)


def whole(shape):
    return pl.BlockSpec(shape, lambda *_: (0,) * len(shape))


def params(**kw):
    return pltpu.CompilerParams(vmem_limit_bytes=56 * 1024 * 1024, **kw)


def silu(v):
    return v * jax.nn.sigmoid(v)


def routes_kernel(ids_ref, pos_ref, tab_ref):
    chunks, _, tokens = ids_ref.shape
    experts = tab_ref.shape[1]
    upper = (lax.broadcasted_iota(jnp.int32, (tokens, tokens), 0) <= lax.broadcasted_iota(jnp.int32, (tokens, tokens), 1)).astype(F32).astype(BF16)
    before = (lax.broadcasted_iota(jnp.int32, (experts, experts), 1) < lax.broadcasted_iota(jnp.int32, (experts, experts), 0)).astype(F32)
    lane = lax.broadcasted_iota(jnp.int32, (experts, 128), 1)
    for c in range(chunks):
        hit = lax.broadcasted_iota(jnp.int32, (experts, tokens), 0) == ids_ref[c]
        hot = hit.astype(F32)
        rank = jnp.dot(hot.astype(BF16), upper, preferred_element_type=F32)
        count = jnp.sum(hot, axis=1, keepdims=True)
        blocks = jnp.floor((count + (ROW_ALIGN - 1)) * (1.0 / ROW_ALIGN))
        start = ROW_ALIGN * jnp.dot(before.astype(BF16), jnp.broadcast_to(blocks, (experts, 128)).astype(BF16), preferred_element_type=F32)
        pos_ref[c] = jnp.sum(hot * (start[:, :1] + rank - 1.0), axis=0, keepdims=True).astype(jnp.int32)
        tab_ref[c] = jnp.where(lane == 0, start, jnp.broadcast_to(count, (experts, 128))).astype(jnp.int32)


LOG2E = 1.4426950408889634


def mamba_kernel(x_hbm, cs_hbm, h_hbm, g_ref, win_ref, cw_ref, cb_ref, wxp_ref, g4_ref, wdt_ref, bdt_ref, alog_ref, dskip_ref, wout_ref,
                 uo_hbm, us_hbm, chip_hbm, co_hbm, ho_hbm,
                 x_s, cs_s, co_s, h_s, xc_s, z_s, p_s, m_s, u_s, wdt4, ones_s, a_s, norm_s, delta_s, dx_s, y_s,
                 in_sem, h_sem, out_sem, ho_sem, psend, precv, msend, mrecv):
    steps, batch, d_model = x_s.shape
    inner = cs_s.shape[2]
    state = alog_ref.shape[0]
    rank = wdt_ref.shape[0]
    width = rank + 2 * state
    lanes = steps * width
    half = steps // 2
    rows = batch // CHUNKS
    tiles = inner // 128
    me = lax.axis_index("tp")
    core = lax.rem(me, 2)
    sibling = me + 1 - 2 * core
    partner = lax.rem(me + 2, 4)

    barrier = pltpu.get_barrier_semaphore()
    for peer in (sibling, partner):
        pl.semaphore_signal(barrier, inc=1, device_id={"tp": peer}, device_id_type=pl.DeviceIdType.MESH)

    def span(c):
        return pl.ds(c * rows, rows)

    def loads(c):
        return [
            pltpu.make_async_copy(x_hbm.at[:, span(c), :], x_s.at[:, span(c), :], in_sem.at[0, c]),
            pltpu.make_async_copy(cs_hbm.at[:, span(c), :], cs_s.at[:, span(c), :], in_sem.at[1, c]),
        ]

    def state_rows(c):
        return pl.ds(c * rows * state, rows * state)

    def h_loads(c):
        return [pltpu.make_async_copy(h_hbm.at[state_rows(c), pl.ds(l * 128, 128)], h_s.at[l, state_rows(c), :], h_sem.at[l, c]) for l in range(tiles)]

    def h_stores(c):
        return [pltpu.make_async_copy(h_s.at[l, state_rows(c), :], ho_hbm.at[state_rows(c), pl.ds(l * 128, 128)], ho_sem.at[l, c]) for l in range(tiles)]

    def co_store(c):
        return pltpu.make_async_copy(co_s.at[:, span(c), :], co_hbm.at[:, span(c), :], out_sem.at[0, c])

    def remote(buf, c, src, dst, send, recv, stage, peer):
        return pltpu.make_async_remote_copy(
            src_ref=buf.at[src, c], dst_ref=buf.at[dst, c], send_sem=send.at[stage, c], recv_sem=recv.at[stage, c],
            device_id={"tp": peer}, device_id_type=pl.DeviceIdType.MESH)

    def p_beside(c):
        return remote(p_s, c, 1, 2, psend, precv, 0, sibling)

    def p_across(c):
        return remote(p_s, c, 3, 4, psend, precv, 1, partner)

    def p_back(c):
        return remote(p_s, c, 5, 6, psend, precv, 2, sibling)

    def m_beside(c):
        return remote(m_s, c, 1, 2, msend, mrecv, 0, sibling)

    def m_across(c):
        return remote(m_s, c, 3, 4, msend, mrecv, 1, partner)

    def u_back(c):
        return pltpu.make_async_remote_copy(
            src_ref=u_s.at[0, c], dst_ref=u_s.at[1, c], send_sem=msend.at[2, c], recv_sem=mrecv.at[2, c],
            device_id={"tp": sibling}, device_id_type=pl.DeviceIdType.MESH)

    for c in range(CHUNKS):
        for cp in loads(c):
            cp.start()
    for c in range(CHUNKS):
        for cp in h_loads(c):
            cp.start()

    gain = g_ref[...].astype(F32)

    def project(c):
        for cp in loads(c):
            cp.wait()

        def block(i, carry):
            r = pl.multiple_of(c * rows + i * 128, 128)
            seq = [cs_s[j, pl.ds(r, 128), :].astype(F32) for j in range(3)]
            part = []
            for s in range(steps):
                x = x_s[s, pl.ds(r, 128), :].astype(F32)
                n = (x * lax.rsqrt(jnp.mean(x * x, axis=-1, keepdims=True) + EPSILON) * gain).astype(BF16)
                xz = jnp.dot(n, win_ref[...], preferred_element_type=F32).astype(BF16)
                z_s[s, pl.ds(r, 128), :] = xz[:, inner:]
                xi = xz[:, :inner]
                if s > 0:
                    co_s[s - 1, pl.ds(r, 128), :] = xi
                seq.append(xi.astype(F32))
                acc = seq[s] * cw_ref[0:1, :].astype(F32)
                for j in range(1, 4):
                    acc = acc + seq[s + j] * cw_ref[j:j + 1, :].astype(F32)
                xc = silu(acc + cb_ref[...].astype(F32)).astype(BF16)
                xc_s[s, pl.ds(r, 128), :] = xc
                part.append(lax.dot_general(xc, wxp_ref[...], (((1,), (1,)), ((), ())), preferred_element_type=F32))
            low = jnp.concatenate(part[:2], axis=1)
            high = jnp.concatenate(part[2:], axis=1)
            q = pl.multiple_of(i * 128, 128)
            p_s[0, c, pl.ds(q, 128), :] = jnp.where(core == 0, low, high)
            p_s[1, c, pl.ds(q, 128), :] = jnp.where(core == 0, high, low)
            return carry

        lax.fori_loop(0, rows // 128, block, 0)
        co_store(c).start()

    def p_sum(c):
        p_beside(c).wait_recv()
        p_s[3, c] = p_s[0, c] + p_s[2, c]
        p_across(c).start()

    def p_whole(c):
        p_across(c).wait_recv()
        p_s[5, c] = p_s[3, c] + p_s[4, c]
        p_back(c).start()

    def scan(c):
        p_back(c).wait_recv()
        for cp in h_loads(c):
            cp.wait()

        def block(i, carry):
            r = pl.multiple_of(i * 128, 128)
            g = pl.multiple_of(c * rows + i * 128, 128)
            own, sib = p_s[5, c, pl.ds(r, 128), :], p_s[6, c, pl.ds(r, 128), :]
            p = jnp.concatenate([jnp.where(core == 0, own, sib), jnp.where(core == 0, sib, own)], axis=1)
            sq = p * p
            s1 = sq.astype(BF16)
            rest = sq - s1.astype(F32)
            s2 = rest.astype(BF16)
            s3 = (rest - s2.astype(F32)).astype(BF16)
            mean = sum(jnp.dot(v, ones_s[...], preferred_element_type=F32) for v in (s3, s2, s1))
            norm = p * lax.rsqrt(mean + EPSILON) * g4_ref[...]
            norm_s[...] = norm
            pre = jnp.dot(norm.astype(BF16), wdt4[...], preferred_element_type=F32)
            bias = bdt_ref[...].astype(F32)
            for s in range(steps):
                v = pre[:, s * inner:(s + 1) * inner] + bias
                delta = jnp.maximum(v, 0.0) + jnp.log1p(jnp.exp(-jnp.abs(v)))
                delta_s[s] = delta
                dx_s[s] = delta * xc_s[s, pl.ds(g, 128), :].astype(F32)

            def tile(t, carry2):
                b = pl.multiple_of(t * 8, 8)
                base = (g + b) * state
                q = norm_s[pl.ds(b, 8), :]
                cut = [slice(l * 128, (l + 1) * 128) for l in range(tiles)]
                dl = [[delta_s[s, pl.ds(b, 8), k] for k in cut] for s in range(steps)]
                dx = [[dx_s[s, pl.ds(b, 8), k] for k in cut] for s in range(steps)]
                ys = [[jnp.zeros((8, 128), F32) for _ in cut] for _ in range(steps)]
                for n in range(state):
                    cols = []
                    for s in range(steps):
                        b0 = s * width + rank + n
                        cols.append((jnp.broadcast_to(q[:, b0:b0 + 1], (8, 128)), jnp.broadcast_to(q[:, b0 + state:b0 + state + 1], (8, 128))))
                    for l in range(tiles):
                        a = a_s[n:n + 1, cut[l]]
                        h = h_s[l, pl.ds(base + n, 8, stride=state), :]
                        for s in range(steps):
                            h = jnp.exp2(dl[s][l] * a) * h + dx[s][l] * cols[s][0]
                            ys[s][l] = ys[s][l] + h * cols[s][1]
                        h_s[l, pl.ds(base + n, 8, stride=state), :] = h
                for s in range(steps):
                    for l in range(tiles):
                        y_s[s, pl.ds(b, 8), cut[l]] = ys[s][l]
                return carry2

            lax.fori_loop(0, 16, tile, 0)
            for s in range(steps):
                xc = xc_s[s, pl.ds(g, 128), :].astype(F32)
                yg = ((y_s[s] + dskip_ref[...] * xc) * silu(z_s[s, pl.ds(g, 128), :].astype(F32))).astype(BF16)
                out = jnp.dot(yg, wout_ref[...], preferred_element_type=F32).astype(BF16)
                m_s[lax.rem(core + s // half, 2), c, s % half, pl.ds(r, 128), :] = out
            return carry

        lax.fori_loop(0, rows // 128, block, 0)
        for cp in h_stores(c):
            cp.start()
        m_beside(c).start()

    def chip_out(c):
        return pltpu.make_async_copy(m_s.at[3, c], chip_hbm.at[c - WHOLE], out_sem.at[1, c])

    def m_sum(c):
        m_beside(c).wait_recv()
        for s in range(half):
            m_s[3, c, s] = (m_s[0, c, s].astype(F32) + m_s[2, c, s].astype(F32)).astype(BF16)
        if c < WHOLE:
            m_across(c).start()
        else:
            chip_out(c).start()

    def uo_out(c):
        return pltpu.make_async_copy(u_s.at[0, c], uo_hbm.at[c], out_sem.at[1, c])

    def us_out(c):
        return pltpu.make_async_copy(u_s.at[1, c], us_hbm.at[c], out_sem.at[2, c])

    def m_whole(c):
        m_across(c).wait_recv()
        for s in range(half):
            x = x_s[core * half + s, span(c), :].astype(F32)
            u_s[0, c, s] = (x + (m_s[3, c, s].astype(F32) + m_s[4, c, s].astype(F32))).astype(BF16)
        u_back(c).start()
        uo_out(c).start()

    project(0)
    pl.semaphore_wait(barrier, 2)
    p_beside(0).start()
    project(1)
    p_beside(1).start()
    p_sum(0)

    wdt4[...] = jnp.zeros_like(wdt4)
    for s in range(steps):
        wdt4[s * width:s * width + rank, s * inner:(s + 1) * inner] = wdt_ref[...]

    def group(v):
        step, col = v // width, lax.rem(v, width)
        return step * 4 + (col >= rank).astype(jnp.int32) + (col >= rank + state).astype(jnp.int32)

    gi = group(lax.broadcasted_iota(jnp.int32, (lanes, lanes), 0))
    gj = group(lax.broadcasted_iota(jnp.int32, (lanes, lanes), 1))
    inv = jnp.where(lax.rem(gj, 4) == 0, 1.0 / rank, 1.0 / state)
    ones_s[...] = jnp.where(gi == gj, inv, 0.0).astype(BF16)
    a_s[...] = -LOG2E * jnp.exp(alog_ref[...])

    project(2)
    p_beside(2).start()
    p_whole(0)
    p_sum(1)
    project(3)
    p_beside(3).start()
    p_whole(1)
    p_sum(2)
    scan(0)
    p_whole(2)
    p_sum(3)
    m_sum(0)
    scan(1)
    p_whole(3)
    m_sum(1)
    scan(2)
    m_sum(2)
    m_whole(0)
    scan(3)
    m_sum(3)
    for c in range(1, WHOLE):
        m_whole(c)
    for c in range(WHOLE):
        u_back(c).wait_recv()
        us_out(c).start()
    for c in range(CHUNKS):
        p_beside(c).wait_send()
        p_across(c).wait_send()
        p_back(c).wait_send()
        m_beside(c).wait_send()
        co_store(c).wait()
        for cp in h_stores(c):
            cp.wait()
        if c < WHOLE:
            m_across(c).wait_send()
            u_back(c).wait_send()
            uo_out(c).wait()
            us_out(c).wait()
        else:
            chip_out(c).wait()


def moe_kernel(c, chunks, tab_ref, pos_ref, uo_ref, ub_ref, gff_ref, wr_ref, wg_ref, wu_ref, wd_ref, h_hbm, cv_hbm, *rest):
    ok_ref, os_ref, ho_hbm, co_hbm, wg, wu, wd, sems, m_s, hot_s, in_s, out_s, h_s, cv_s, st_sem = rest[-15:]
    half, rows, d_model = uo_ref.shape
    experts = wg.shape[0]
    tokens = 2 * half * rows
    slots = hot_s.shape[0]
    core = lax.rem(lax.axis_index("tp"), 2)

    def copies(e):
        return [pltpu.make_async_copy(src.at[e], dst.at[e], sems.at[k, e]) for k, (src, dst) in enumerate(((wg_ref, wg), (wu_ref, wu), (wd_ref, wd)))]

    def fetch(e, carry):
        @pl.when(tab_ref[c, e, 1] > 0)
        def _():
            for cp in copies(e):
                cp.start()
        return carry

    h_span = pl.ds(c * h_s.shape[0], h_s.shape[0])
    cv_span = pl.ds(c * cv_s.shape[1], cv_s.shape[1])
    pulls = [pltpu.make_async_copy(h_hbm.at[h_span, :], h_s, st_sem.at[0]), pltpu.make_async_copy(cv_hbm.at[:, cv_span, :], cv_s, st_sem.at[1])]
    pushes = [pltpu.make_async_copy(h_s, ho_hbm.at[h_span, :], st_sem.at[2]), pltpu.make_async_copy(cv_s, co_hbm.at[:, cv_span, :], st_sem.at[3])]
    lax.fori_loop(0, experts, fetch, 0)
    for cp in pulls:
        cp.start()
    gain = gff_ref[...].astype(F32)
    for k in range(2):
        src = (uo_ref, ub_ref)[k]
        first = jnp.where(core == k, 0, half * rows)
        for s in range(half):
            u = src[s].astype(F32)
            m = u * lax.rsqrt(jnp.mean(u * u, axis=-1, keepdims=True) + EPSILON) * gain
            m_s[pl.ds(pl.multiple_of(first + s * rows, rows), rows), :] = m.astype(BF16)

    pos = pos_ref[0]

    def order(i, carry):
        r = pl.multiple_of(i * 256, 256)
        hot = (lax.broadcasted_iota(jnp.int32, (256, tokens), 0) + r == pos).astype(F32).astype(BF16)
        hot_s[pl.ds(r, 256), :] = hot
        in_s[pl.ds(r, 256), :] = jnp.dot(hot, m_s[...], preferred_element_type=F32).astype(BF16)
        out_s[pl.ds(r, 256), :] = jnp.zeros((256, d_model), BF16)
        return carry

    lax.fori_loop(0, slots // 256, order, 0)
    for pull, push in zip(pulls, pushes):
        pull.wait()
        push.start()
    lane = lax.broadcasted_iota(jnp.int32, (TILE, experts), 1)

    def expert(e, carry):
        count = tab_ref[c, e, 1]
        start = tab_ref[c, e, 0]

        @pl.when(count > 0)
        def _():
            for cp in copies(e):
                cp.wait()

            def tile(i, c2):
                r = pl.multiple_of(start + i * TILE, ROW_ALIGN)
                m = in_s[pl.ds(r, TILE), :]
                logits = jnp.dot(m, wr_ref[...], preferred_element_type=F32)
                ex = jnp.exp(logits - jnp.max(logits, axis=-1, keepdims=True))
                prob = jnp.sum(jnp.where(lane == e, ex, 0.0), axis=-1, keepdims=True) / jnp.sum(ex, axis=-1, keepdims=True)
                gate = jnp.dot(m, wg[e], preferred_element_type=F32)
                up = jnp.dot(m, wu[e], preferred_element_type=F32)
                q = (silu(gate) * up).astype(BF16)
                out_s[pl.ds(r, TILE), :] = (prob * jnp.dot(q, wd[e], preferred_element_type=F32)).astype(BF16)
                return c2

            lax.fori_loop(0, (count + TILE - 1) // TILE, tile, 0)
        return carry

    lax.fori_loop(0, experts, expert, 0)

    def restore(k, dst):
        first = jnp.where(core == k, 0, half * rows)
        for s in range(half):
            hot = hot_s[:, pl.ds(pl.multiple_of(first + s * rows, rows), rows)]
            got = lax.dot_general(hot, out_s[:slots, :], (((0,), (0,)), ((), ())), preferred_element_type=F32)
            dst[s] = got.astype(BF16)

    restore(0, ok_ref)
    restore(1, os_ref)
    for cp in pushes:
        cp.wait()


def solution(mesh):
    act_spec = P(None, "dp", None)
    state_spec = P("dp", "tp", None)
    in_specs = (act_spec, state_spec, state_spec, act_spec, P(None), P(None, None, "tp"), P("tp", None), P("tp"), P("tp", None), P(None), P(None), P(None), P(None, "tp"), P("tp"), P("tp", None), P("tp"), P("tp", None), P(None), P(None, None), P(None, None, "tp"), P(None, None, "tp"), P(None, "tp", None))
    out_specs = (act_spec, state_spec, state_spec)
    across = [(0, 2), (2, 0), (1, 3), (3, 1)]
    beside = [(0, 1), (1, 0), (2, 3), (3, 2)]

    def layer_steps(x_steps, conv_state, ssm_state, expert_ids, g_in, w_in, conv_w, conv_b, w_xp, g_dt, g_b, g_c, w_dt, b_dt, a_log, d_skip, w_out, g_ff, w_router, w_gate, w_up, w_down):
        steps, batch, d_model = x_steps.shape
        inner = w_in.shape[2]
        rank = w_dt.shape[0]
        state = a_log.shape[1]
        experts, _, ffn = w_gate.shape
        width = rank + 2 * state
        half = steps // 2
        rows = batch // CHUNKS
        tokens = steps * rows
        slots = tokens + experts * ROW_ALIGN
        core = lax.rem(lax.axis_index("tp"), 2)

        conv_t = jnp.transpose(conv_state, (2, 0, 1))
        h_rows = jnp.transpose(ssm_state, (0, 2, 1)).reshape(batch * state, inner)
        alog_t = a_log.T
        w_in_flat = w_in.reshape(d_model, 2 * inner)
        g4 = jnp.tile(jnp.concatenate([g_dt, g_b, g_c]).astype(F32), steps).reshape(1, steps * width)

        ids = expert_ids.reshape(steps, CHUNKS, rows).transpose(1, 0, 2).reshape(CHUNKS, 1, tokens)
        pos, table = pl.pallas_call(
            routes_kernel,
            out_shape=(jax.ShapeDtypeStruct((CHUNKS, 1, tokens), jnp.int32), jax.ShapeDtypeStruct((CHUNKS, experts, 128), jnp.int32)),
            compiler_params=params(),
            name="routes",
        )(ids)

        vmem = pl.BlockSpec(memory_space=pltpu.VMEM)
        rest = CHUNKS - WHOLE
        piece = (half, rows, d_model)
        u_first, u_second, chips, conv_mid, h_mid = pl.pallas_call(
            mamba_kernel,
            in_specs=[HBM, HBM, HBM] + [vmem] * 11,
            out_specs=[HBM] * 5,
            out_shape=[
                jax.ShapeDtypeStruct((WHOLE,) + piece, BF16),
                jax.ShapeDtypeStruct((WHOLE,) + piece, BF16),
                jax.ShapeDtypeStruct((rest,) + piece, BF16),
                jax.ShapeDtypeStruct((3, batch, inner), BF16),
                jax.ShapeDtypeStruct((batch * state, inner), F32),
            ],
            scratch_shapes=[
                pltpu.VMEM((steps, batch, d_model), BF16),
                pltpu.VMEM((3, batch, inner), BF16),
                pltpu.VMEM((3, batch, inner), BF16),
                pltpu.VMEM((inner // 128, batch * state, 128), F32),
                pltpu.VMEM((steps, batch, inner), BF16),
                pltpu.VMEM((steps, batch, inner), BF16),
                pltpu.VMEM((7, CHUNKS, rows, 2 * width), F32),
                pltpu.VMEM((5, CHUNKS) + piece, BF16),
                pltpu.VMEM((2, CHUNKS) + piece, BF16),
                pltpu.VMEM((steps * width, steps * inner), BF16),
                pltpu.VMEM((steps * width, steps * width), BF16),
                pltpu.VMEM((state, inner), F32),
                pltpu.VMEM((128, steps * width), F32),
                pltpu.VMEM((steps, 128, inner), F32),
                pltpu.VMEM((steps, 128, inner), F32),
                pltpu.VMEM((steps, 128, inner), F32),
                pltpu.SemaphoreType.DMA((2, CHUNKS)),
                pltpu.SemaphoreType.DMA((inner // 128, CHUNKS)),
                pltpu.SemaphoreType.DMA((3, CHUNKS)),
                pltpu.SemaphoreType.DMA((inner // 128, CHUNKS)),
                pltpu.SemaphoreType.DMA((3, CHUNKS)),
                pltpu.SemaphoreType.DMA((3, CHUNKS)),
                pltpu.SemaphoreType.DMA((3, CHUNKS)),
                pltpu.SemaphoreType.DMA((3, CHUNKS)),
            ],
            compiler_params=params(collective_id=0, has_side_effects=True),
            cost_estimate=pl.CostEstimate(flops=int(8e9), bytes_accessed=int(45e6), transcendentals=0),
            name="mamba",
        )(x_steps, conv_t, h_rows, g_in.reshape(1, -1), w_in_flat, conv_w.T, conv_b.reshape(1, -1), w_xp.T, g4, w_dt, b_dt.reshape(1, -1), alog_t, d_skip.reshape(1, -1), w_out)

        def run_moe(c, u_own, u_sib, states):
            extra = [] if states is None else list(states)
            return pl.pallas_call(
                functools.partial(moe_kernel, c, CHUNKS),
                grid=(1,),
                in_specs=[pl.BlockSpec(memory_space=pltpu.SMEM), pl.BlockSpec((1, 1, tokens), lambda i: (c, 0, 0)), vmem, vmem, vmem, vmem] + [HBM] * (5 + len(extra)),
                out_specs=[vmem, vmem, HBM, HBM],
                out_shape=[jax.ShapeDtypeStruct(piece, BF16)] * 2 + [jax.ShapeDtypeStruct(h_mid.shape, F32), jax.ShapeDtypeStruct(conv_mid.shape, BF16)],
                scratch_shapes=[
                    pltpu.VMEM((experts, d_model, ffn), BF16),
                    pltpu.VMEM((experts, d_model, ffn), BF16),
                    pltpu.VMEM((experts, ffn, d_model), BF16),
                    pltpu.SemaphoreType.DMA((3, experts)),
                    pltpu.VMEM((tokens, d_model), BF16),
                    pltpu.VMEM((slots, tokens), BF16),
                    pltpu.VMEM((slots + TILE, d_model), BF16),
                    pltpu.VMEM((slots + TILE, d_model), BF16),
                    pltpu.VMEM((rows * state, inner), F32),
                    pltpu.VMEM((3, rows, inner), BF16),
                    pltpu.SemaphoreType.DMA((4,)),
                ],
                input_output_aliases={11: 2, 12: 3} if extra else {},
                compiler_params=params(),
                cost_estimate=pl.CostEstimate(flops=int(12e9 / CHUNKS), bytes_accessed=int(40e6 / CHUNKS), transcendentals=0),
                name=f"moe{c}",
            )(table, pos, u_own, u_sib, g_ff.reshape(1, -1), w_router, w_gate, w_up, w_down, h_mid, conv_mid, *extra)

        def both(keep, send, dtype):
            got = lax.ppermute(send, "tp", beside)
            chip = (keep.astype(F32) + got.astype(F32)).astype(dtype)
            return chip, lax.ppermute(chip, "tp", across)

        mids = [(u_first[c], u_second[c]) for c in range(WHOLE)]
        for c in range(WHOLE, CHUNKS):
            chip = chips[c - WHOLE]
            far = lax.ppermute(chip, "tp", across)
            x_own = lax.dynamic_slice(x_steps, (half * core, c * rows, 0), (half, rows, d_model))
            u_own = (x_own.astype(F32) + (chip.astype(F32) + far.astype(F32))).astype(BF16)
            mids.append((u_own, lax.ppermute(u_own, "tp", beside)))

        owns, sibs = [], []
        states = None
        for c in range(CHUNKS):
            u_own, u_sib = mids[c]
            o_keep, o_send, *states = run_moe(c, u_own, u_sib, states)
            chip, far = both(o_keep, o_send, BF16)
            y_own = (u_own.astype(F32) + (chip.astype(F32) + far.astype(F32))).astype(BF16)
            owns.append(y_own)
            sibs.append(lax.ppermute(y_own, "tp", beside))
        ssm_out, conv_out = states
        own = jnp.concatenate(owns, axis=1)
        sib = jnp.concatenate(sibs, axis=1)
        y_steps = jnp.concatenate([jnp.where(core == 0, own, sib), jnp.where(core == 0, sib, own)], axis=0)
        ssm_fin = jnp.transpose(ssm_out.reshape(batch, state, inner), (0, 2, 1))
        return y_steps, jnp.transpose(conv_out, (1, 2, 0)), ssm_fin

    return jax.shard_map(layer_steps, mesh=mesh, in_specs=in_specs, out_specs=out_specs, check_vma=False)
```

```python
import functools

import jax
import jax.numpy as jnp
from jax import lax
from jax.experimental import pallas as pl
from jax.experimental.pallas import tpu as pltpu
from jax.sharding import PartitionSpec as P

EPSILON = 1e-6
CHUNKS = 4
ROW_ALIGN = 16
TILE = 128
AHEAD = 4
WHOLE = 2
F32 = jnp.float32
BF16 = jnp.bfloat16
HBM = pl.BlockSpec(memory_space=pl.ANY)


def whole(shape):
    return pl.BlockSpec(shape, lambda *_: (0,) * len(shape))


def params(**kw):
    return pltpu.CompilerParams(vmem_limit_bytes=56 * 1024 * 1024, **kw)


def silu(v):
    return v * jax.nn.sigmoid(v)


def routes_kernel(ids_ref, pos_ref, tab_ref):
    chunks, _, tokens = pos_ref.shape
    steps = ids_ref.shape[0]
    rows = tokens // steps
    experts = 16
    upper = (lax.broadcasted_iota(jnp.int32, (tokens, tokens), 0) <= lax.broadcasted_iota(jnp.int32, (tokens, tokens), 1)).astype(F32).astype(BF16)
    before = (lax.broadcasted_iota(jnp.int32, (experts, experts), 1) < lax.broadcasted_iota(jnp.int32, (experts, experts), 0)).astype(F32).astype(BF16)
    lane = lax.broadcasted_iota(jnp.int32, (experts, 128), 1)
    number = lax.broadcasted_iota(jnp.int32, (experts, 128), 0).astype(F32)
    for c in range(chunks):
        ids = jnp.concatenate([ids_ref[s, :, c * rows:(c + 1) * rows] for s in range(steps)], axis=1)
        hit = lax.broadcasted_iota(jnp.int32, (experts, tokens), 0) == ids
        hot = hit.astype(F32)
        rank = jnp.dot(hot.astype(BF16), upper, preferred_element_type=F32)
        count = jnp.broadcast_to(jnp.sum(hot, axis=1, keepdims=True), (experts, 128))
        blocks = jnp.floor((count + (ROW_ALIGN - 1)) * (1.0 / ROW_ALIGN))
        start = ROW_ALIGN * jnp.dot(before, blocks.astype(BF16), preferred_element_type=F32)
        active = (count > 0.0).astype(F32)
        place = jnp.dot(before, active.astype(BF16), preferred_element_type=F32)
        listed = jnp.sum(jnp.where((place == lane.astype(F32)) & (active > 0.0), number, 0.0), axis=0, keepdims=True)
        pos_ref[c] = jnp.sum(hot * (start[:, :1] + rank - 1.0), axis=0, keepdims=True).astype(jnp.int32)
        tab_ref[c, 0:16, :] = jnp.where(lane == 0, start, count).astype(jnp.int32)
        tab_ref[c, 16:17, :] = listed.astype(jnp.int32)
        tab_ref[c, 17:18, :] = jnp.sum(active, axis=0, keepdims=True).astype(jnp.int32)


LOG2E = 1.4426950408889634


def mamba_kernel(x_hbm, cs_hbm, h_hbm, g_ref, win3_ref, cw_ref, cb_ref, wxp_ref, gdt_ref, gb_ref, gc_ref, wdt_ref, bdt_ref, alog_ref, dskip_ref, wout_ref,
                 uo_hbm, us_hbm, chip_hbm, co_hbm, ho_hbm,
                 x_s, cs_s, co_s, h_s, xc_s, z_s, p_s, m_s, u_s, win_ref, g4_ref, wdt4, ones_s, spread_s, left_s, wide_s, a_s, q_s, delta_s, dx_s, y_s,
                 in_sem, h_sem, out_sem, ho_sem, psend, precv, msend, mrecv):
    steps, batch, d_model = x_s.shape
    inner = cs_s.shape[2]
    state = alog_ref.shape[0]
    rank = wdt_ref.shape[0]
    width = rank + 2 * state
    lanes = steps * width
    half = steps // 2
    rows = batch // CHUNKS
    tiles = inner // 128
    me = lax.axis_index("tp")
    core = lax.rem(me, 2)
    sibling = me + 1 - 2 * core
    partner = lax.rem(me + 2, 4)

    barrier = pltpu.get_barrier_semaphore()
    for peer in (sibling, partner):
        pl.semaphore_signal(barrier, inc=1, device_id={"tp": peer}, device_id_type=pl.DeviceIdType.MESH)

    def span(c):
        return pl.ds(c * rows, rows)

    def loads(c):
        return [
            pltpu.make_async_copy(x_hbm.at[:, span(c), :], x_s.at[:, span(c), :], in_sem.at[0, c]),
            pltpu.make_async_copy(cs_hbm.at[:, span(c), :], cs_s.at[:, span(c), :], in_sem.at[1, c]),
        ]

    def state_rows(c):
        return pl.ds(c * rows * state, rows * state)

    def h_loads(c):
        return [pltpu.make_async_copy(h_hbm.at[state_rows(c), pl.ds(l * 128, 128)], h_s.at[l, state_rows(c), :], h_sem.at[l, c]) for l in range(tiles)]

    def h_stores(c):
        return [pltpu.make_async_copy(h_s.at[l, state_rows(c), :], ho_hbm.at[state_rows(c), pl.ds(l * 128, 128)], ho_sem.at[l, c]) for l in range(tiles)]

    def co_store(c):
        return pltpu.make_async_copy(co_s.at[:, span(c), :], co_hbm.at[:, span(c), :], out_sem.at[0, c])

    def remote(buf, c, src, dst, send, recv, stage, peer):
        return pltpu.make_async_remote_copy(
            src_ref=buf.at[src, c], dst_ref=buf.at[dst, c], send_sem=send.at[stage, c], recv_sem=recv.at[stage, c],
            device_id={"tp": peer}, device_id_type=pl.DeviceIdType.MESH)

    def p_beside(c):
        return remote(p_s, c, 1, 2, psend, precv, 0, sibling)

    def p_across(c):
        return remote(p_s, c, 3, 4, psend, precv, 1, partner)

    def p_back(c):
        return remote(p_s, c, 5, 6, psend, precv, 2, sibling)

    def m_beside(c):
        return remote(m_s, c, 1, 2, msend, mrecv, 0, sibling)

    def m_across(c):
        return remote(m_s, c, 3, 4, msend, mrecv, 1, partner)

    def u_back(c):
        return pltpu.make_async_remote_copy(
            src_ref=u_s.at[0, c], dst_ref=u_s.at[1, c], send_sem=msend.at[2, c], recv_sem=mrecv.at[2, c],
            device_id={"tp": sibling}, device_id_type=pl.DeviceIdType.MESH)

    for c in range(CHUNKS):
        for cp in loads(c):
            cp.start()
    for c in range(CHUNKS):
        for cp in h_loads(c):
            cp.start()

    gain = g_ref[...].astype(F32)[None, :]
    for k in range(2):
        win_ref[:, k * inner:(k + 1) * inner] = win3_ref[:, k, :]

    def project(c):
        for cp in loads(c):
            cp.wait()

        def block(i, carry):
            r = pl.multiple_of(c * rows + i * 128, 128)
            seq = [cs_s[j, pl.ds(r, 128), :].astype(F32) for j in range(3)]
            part = []
            for s in range(steps):
                x = x_s[s, pl.ds(r, 128), :].astype(F32)
                n = (x * lax.rsqrt(jnp.mean(x * x, axis=-1, keepdims=True) + EPSILON) * gain).astype(BF16)
                xz = jnp.dot(n, win_ref[...], preferred_element_type=F32).astype(BF16)
                z_s[s, pl.ds(r, 128), :] = xz[:, inner:]
                xi = xz[:, :inner]
                if s > 0:
                    co_s[s - 1, pl.ds(r, 128), :] = xi
                seq.append(xi.astype(F32))
                acc = seq[s] * cw_ref[0:1, :].astype(F32)
                for j in range(1, 4):
                    acc = acc + seq[s + j] * cw_ref[j:j + 1, :].astype(F32)
                xc = silu(acc + cb_ref[...].astype(F32)[None, :]).astype(BF16)
                xc_s[s, pl.ds(r, 128), :] = xc
                part.append(lax.dot_general(xc, wxp_ref[...], (((1,), (1,)), ((), ())), preferred_element_type=F32))
            low = jnp.concatenate(part[:2], axis=1)
            high = jnp.concatenate(part[2:], axis=1)
            q = pl.multiple_of(i * 128, 128)
            p_s[0, c, pl.ds(q, 128), :] = jnp.where(core == 0, low, high)
            p_s[1, c, pl.ds(q, 128), :] = jnp.where(core == 0, high, low)
            return carry

        lax.fori_loop(0, rows // 128, block, 0)
        co_store(c).start()

    def p_sum(c):
        p_beside(c).wait_recv()
        p_s[3, c] = p_s[0, c] + p_s[2, c]
        p_across(c).start()

    def p_whole(c):
        p_across(c).wait_recv()
        p_s[5, c] = p_s[3, c] + p_s[4, c]
        p_back(c).start()

    def scan(c):
        p_back(c).wait_recv()
        for cp in h_loads(c):
            cp.wait()

        def block(i, carry):
            r = pl.multiple_of(i * 128, 128)
            g = pl.multiple_of(c * rows + i * 128, 128)
            own, sib = p_s[5, c, pl.ds(r, 128), :], p_s[6, c, pl.ds(r, 128), :]
            p = jnp.concatenate([jnp.where(core == 0, own, sib), jnp.where(core == 0, sib, own)], axis=1)
            sq = p * p
            s1 = sq.astype(BF16)
            rest = sq - s1.astype(F32)
            s2 = rest.astype(BF16)
            s3 = (rest - s2.astype(F32)).astype(BF16)
            mean = sum(jnp.dot(v, ones_s[...], preferred_element_type=F32) for v in (s3, s2, s1))
            norm = p * lax.rsqrt(mean + EPSILON) * g4_ref[...]
            for s in range(steps):
                first = s * width + rank
                part = jnp.concatenate([norm[:, first:first + 2 * state], jnp.zeros((128, 128 - 2 * state), F32)], axis=1)
                q_s[s] = part
                hi = part.astype(BF16).astype(F32)
                mid = (part - hi).astype(BF16).astype(F32)
                low = part - hi - mid
                left_s[s * 128:(s + 1) * 128, :] = (hi + pltpu.roll(mid, 2 * state, 1) + pltpu.roll(low, 4 * state, 1)).astype(BF16)
            pre = jnp.dot(norm.astype(BF16), wdt4[...], preferred_element_type=F32)
            bias = bdt_ref[...].astype(F32)[None, :]
            for s in range(steps):
                v = pre[:, s * inner:(s + 1) * inner] + bias
                delta = jnp.maximum(v, 0.0) + jnp.log1p(jnp.exp(-jnp.abs(v)))
                delta_s[s] = delta
                dx_s[s] = delta * xc_s[s, pl.ds(g, 128), :].astype(F32)

            def widen(j, carry2):
                cols = pl.ds(pl.multiple_of(j * 256, 256), 256)
                wide_s[:, cols] = jnp.dot(left_s[...], spread_s[:, cols], preferred_element_type=F32)
                return carry2

            lax.fori_loop(0, state // 2, widen, 0)

            def tile(t, carry2):
                b = pl.multiple_of(t * 8, 8)
                base = (g + b) * state
                cut = [slice(l * 128, (l + 1) * 128) for l in range(tiles)]
                dl = [[delta_s[s, pl.ds(b, 8), k] for k in cut] for s in range(steps)]
                dx = [[dx_s[s, pl.ds(b, 8), k] for k in cut] for s in range(steps)]
                ys = [[jnp.zeros((8, 128), F32) for _ in cut] for _ in range(steps)]
                qs = [q_s[s, pl.ds(b, 8), :] for s in range(steps)]
                for n in range(state):
                    bs = [jnp.broadcast_to(qs[s][:, n:n + 1], (8, 128)) for s in range(steps)]
                    cs = [wide_s[pl.ds(s * 128 + b, 8), n * 128:(n + 1) * 128] for s in range(steps)]
                    cols = list(zip(bs, cs))
                    for l in range(tiles):
                        a = a_s[n:n + 1, cut[l]]
                        h = h_s[l, pl.ds(base + n, 8, stride=state), :]
                        for s in range(steps):
                            h = jnp.exp2(dl[s][l] * a) * h + dx[s][l] * cols[s][0]
                            ys[s][l] = ys[s][l] + h * cols[s][1]
                        h_s[l, pl.ds(base + n, 8, stride=state), :] = h
                for s in range(steps):
                    for l in range(tiles):
                        y_s[s, pl.ds(b, 8), cut[l]] = ys[s][l]
                return carry2

            lax.fori_loop(0, 16, tile, 0)
            for s in range(steps):
                xc = xc_s[s, pl.ds(g, 128), :].astype(F32)
                yg = ((y_s[s] + dskip_ref[...][None, :] * xc) * silu(z_s[s, pl.ds(g, 128), :].astype(F32))).astype(BF16)
                out = jnp.dot(yg, wout_ref[...], preferred_element_type=F32).astype(BF16)
                m_s[lax.rem(core + s // half, 2), c, s % half, pl.ds(r, 128), :] = out
            return carry

        lax.fori_loop(0, rows // 128, block, 0)
        for cp in h_stores(c):
            cp.start()
        m_beside(c).start()

    def chip_out(c):
        return pltpu.make_async_copy(m_s.at[3, c], chip_hbm.at[c - WHOLE], out_sem.at[1, c])

    def m_sum(c):
        m_beside(c).wait_recv()
        for s in range(half):
            m_s[3, c, s] = (m_s[0, c, s].astype(F32) + m_s[2, c, s].astype(F32)).astype(BF16)
        if c < WHOLE:
            m_across(c).start()
        else:
            chip_out(c).start()

    def uo_out(c):
        return pltpu.make_async_copy(u_s.at[0, c], uo_hbm.at[c], out_sem.at[1, c])

    def us_out(c):
        return pltpu.make_async_copy(u_s.at[1, c], us_hbm.at[c], out_sem.at[2, c])

    def m_whole(c):
        m_across(c).wait_recv()
        for s in range(half):
            x = x_s[core * half + s, span(c), :].astype(F32)
            u_s[0, c, s] = (x + (m_s[3, c, s].astype(F32) + m_s[4, c, s].astype(F32))).astype(BF16)
        u_back(c).start()
        uo_out(c).start()

    project(0)
    pl.semaphore_wait(barrier, 2)
    p_beside(0).start()
    project(1)
    p_beside(1).start()
    p_sum(0)

    wdt4[...] = jnp.zeros_like(wdt4)
    for s in range(steps):
        wdt4[s * width:s * width + rank, s * inner:(s + 1) * inner] = wdt_ref[...]

    def group(v):
        step, col = v // width, lax.rem(v, width)
        return step * 4 + (col >= rank).astype(jnp.int32) + (col >= rank + state).astype(jnp.int32)

    gi = group(lax.broadcasted_iota(jnp.int32, (lanes, lanes), 0))
    gj = group(lax.broadcasted_iota(jnp.int32, (lanes, lanes), 1))
    inv = jnp.where(lax.rem(gj, 4) == 0, 1.0 / rank, 1.0 / state)
    ones_s[...] = jnp.where(gi == gj, inv, 0.0).astype(BF16)
    ki = lax.broadcasted_iota(jnp.int32, spread_s.shape, 0)
    kj = lax.broadcasted_iota(jnp.int32, spread_s.shape, 1)
    spread_s[...] = ((lax.rem(ki, 2 * state) == state + kj // 128) & (ki < 6 * state)).astype(F32).astype(BF16)
    for s in range(steps):
        for ref, at in ((gdt_ref, 0), (gb_ref, rank), (gc_ref, rank + state)):
            g4_ref[:, s * width + at:s * width + at + ref.shape[0]] = ref[...].astype(F32)[None, :]
    a_s[...] = -LOG2E * jnp.exp(alog_ref[...])

    project(2)
    p_beside(2).start()
    p_whole(0)
    p_sum(1)
    project(3)
    p_beside(3).start()
    p_whole(1)
    p_sum(2)
    scan(0)
    p_whole(2)
    p_sum(3)
    m_sum(0)
    scan(1)
    p_whole(3)
    m_sum(1)
    scan(2)
    m_sum(2)
    m_whole(0)
    scan(3)
    m_sum(3)
    for c in range(1, WHOLE):
        m_whole(c)
    for c in range(WHOLE):
        u_back(c).wait_recv()
        us_out(c).start()
    for c in range(CHUNKS):
        p_beside(c).wait_send()
        p_across(c).wait_send()
        p_back(c).wait_send()
        m_beside(c).wait_send()
        co_store(c).wait()
        for cp in h_stores(c):
            cp.wait()
        if c < WHOLE:
            m_across(c).wait_send()
            u_back(c).wait_send()
            uo_out(c).wait()
            us_out(c).wait()
        else:
            chip_out(c).wait()


def bounce(c, chunks, total):
    unit = total // 8
    counts = [0] * chunks
    for k in range(8):
        counts[1 + k % (chunks - 1)] += unit
    return sum(counts[:c]), counts[c], max(counts)


def moe_kernel(c, chunks, tab_ref, pos_ref, uo_ref, ub_ref, gff_ref, wr_ref, wg_ref, wu_ref, wd_ref, h_hbm, cv_hbm, *rest):
    ok_ref, os_ref, ho_hbm, co_hbm, wg, wu, wd, sems, m_s, hot_s, in_s, out_s, prob_s, h_s, cv_s, st_sem = rest[-16:]
    half, rows, d_model = uo_ref.shape
    experts = wg.shape[0]
    tokens = 2 * half * rows
    slots = hot_s.shape[0]
    core = lax.rem(lax.axis_index("tp"), 2)
    listed = tab_ref[0, 17, 0]

    def copies(e):
        return [pltpu.make_async_copy(src.at[e], dst.at[e], sems.at[k, e]) for k, (src, dst) in enumerate(((wg_ref, wg), (wu_ref, wu), (wd_ref, wd)))]

    def fetch(i):
        @pl.when(i < listed)
        def _():
            for cp in copies(tab_ref[0, 16, i]):
                cp.start()

    for i in range(AHEAD):
        fetch(i)
    pulls, pushes = [], []
    for k, (src, buf, dst) in enumerate(((h_hbm, h_s, ho_hbm), (cv_hbm, cv_s, co_hbm))):
        first, size, _ = bounce(c, chunks, src.shape[k])
        if size:
            pick = (lambda ref, f, n: ref.at[pl.ds(f, n), :]) if k == 0 else (lambda ref, f, n: ref.at[:, pl.ds(f, n), :])
            pulls.append(pltpu.make_async_copy(pick(src, first, size), pick(buf, 0, size), st_sem.at[2 * k]))
            pushes.append(pltpu.make_async_copy(pick(buf, 0, size), pick(dst, first, size), st_sem.at[2 * k + 1]))
    for cp in pulls:
        cp.start()
    gain = gff_ref[...].astype(F32)[None, :]
    for k in range(2):
        src = (uo_ref, ub_ref)[k]
        first = jnp.where(core == k, 0, half * rows)
        for s in range(half):
            u = src[s].astype(F32)
            m = u * lax.rsqrt(jnp.mean(u * u, axis=-1, keepdims=True) + EPSILON) * gain
            m_s[pl.ds(pl.multiple_of(first + s * rows, rows), rows), :] = m.astype(BF16)

    pos = pos_ref[0]
    down = lax.broadcasted_iota(jnp.int32, (256, tokens), 0).astype(F32).astype(BF16)

    def order(i, carry):
        r = pl.multiple_of(i * 256, 256)
        local = jnp.where((pos >= r) & (pos < r + 256), pos - r, -1).astype(F32).astype(BF16)
        hot = jnp.where(down == local, jnp.ones((), BF16), jnp.zeros((), BF16))
        hot_s[pl.ds(r, 256), :] = hot
        m = jnp.dot(hot, m_s[...], preferred_element_type=F32).astype(BF16)
        in_s[pl.ds(r, 256), :] = m
        out_s[pl.ds(r, 256), :] = jnp.zeros((256, d_model), BF16)
        logits = lax.dot_general(m, wr_ref[...], (((1,), (1,)), ((), ())), preferred_element_type=F32)
        ex = jnp.exp(logits - jnp.max(logits, axis=-1, keepdims=True))
        prob_s[pl.ds(r, 256), :] = ex / jnp.sum(ex, axis=-1, keepdims=True)
        return carry

    lax.fori_loop(0, slots // 256, order, 0)
    for pull, push in zip(pulls, pushes):
        pull.wait()
        push.start()

    def feed(e, r, size):
        m = in_s[pl.ds(r, size), :]
        gate = jnp.dot(m, wg[e], preferred_element_type=F32)
        up = jnp.dot(m, wu[e], preferred_element_type=F32)
        q = (silu(gate) * up).astype(BF16)
        lane = lax.broadcasted_iota(jnp.int32, (size, experts), 1)
        prob = jnp.sum(jnp.where(lane == e, prob_s[pl.ds(r, size), :], 0.0), axis=-1, keepdims=True)
        out_s[pl.ds(r, size), :] = (prob * jnp.dot(q, wd[e], preferred_element_type=F32)).astype(BF16)

    def expert(i, carry):
        e = tab_ref[0, 16, i]
        start = tab_ref[0, e, 0]
        count = tab_ref[0, e, 1]
        fetch(i + AHEAD)
        for cp in copies(e):
            cp.wait()
        big = (count + TILE - 1) // (2 * TILE)

        def tile(k, c2):
            feed(e, pl.multiple_of(start + k * (2 * TILE), ROW_ALIGN), 2 * TILE)
            return c2

        lax.fori_loop(0, big, tile, 0)

        @pl.when(count > big * (2 * TILE))
        def _():
            feed(e, pl.multiple_of(start + big * (2 * TILE), ROW_ALIGN), TILE)

        return carry

    lax.fori_loop(0, listed, expert, 0)

    def restore(k, dst):
        first = jnp.where(core == k, 0, half * rows)
        for s in range(half):
            hot = hot_s[:, pl.ds(pl.multiple_of(first + s * rows, rows), rows)]
            got = lax.dot_general(hot, out_s[:slots, :], (((0,), (0,)), ((), ())), preferred_element_type=F32)
            dst[s] = got.astype(BF16)

    restore(0, ok_ref)
    restore(1, os_ref)
    for cp in pushes:
        cp.wait()


def solution(mesh):
    act_spec = P(None, "dp", None)
    state_spec = P("dp", "tp", None)
    in_specs = (act_spec, state_spec, state_spec, act_spec, P(None), P(None, None, "tp"), P("tp", None), P("tp"), P("tp", None), P(None), P(None), P(None), P(None, "tp"), P("tp"), P("tp", None), P("tp"), P("tp", None), P(None), P(None, None), P(None, None, "tp"), P(None, None, "tp"), P(None, "tp", None))
    out_specs = (act_spec, state_spec, state_spec)
    across = [(0, 2), (2, 0), (1, 3), (3, 1)]
    beside = [(0, 1), (1, 0), (2, 3), (3, 2)]

    def layer_steps(x_steps, conv_state, ssm_state, expert_ids, g_in, w_in, conv_w, conv_b, w_xp, g_dt, g_b, g_c, w_dt, b_dt, a_log, d_skip, w_out, g_ff, w_router, w_gate, w_up, w_down):
        steps, batch, d_model = x_steps.shape
        inner = w_in.shape[2]
        rank = w_dt.shape[0]
        state = a_log.shape[1]
        experts, _, ffn = w_gate.shape
        width = rank + 2 * state
        half = steps // 2
        rows = batch // CHUNKS
        tokens = steps * rows
        slots = tokens + experts * ROW_ALIGN
        core = lax.rem(lax.axis_index("tp"), 2)

        conv_t = jnp.transpose(conv_state, (2, 0, 1))
        h_rows = jnp.transpose(ssm_state, (0, 2, 1)).reshape(batch * state, inner)
        alog_t = a_log.T

        ids = jnp.transpose(expert_ids, (0, 2, 1))
        pos, table = pl.pallas_call(
            routes_kernel,
            out_shape=(jax.ShapeDtypeStruct((CHUNKS, 1, tokens), jnp.int32), jax.ShapeDtypeStruct((CHUNKS, 24, 128), jnp.int32)),
            compiler_params=params(),
            name="routes",
        )(ids)

        vmem = pl.BlockSpec(memory_space=pltpu.VMEM)
        rest = CHUNKS - WHOLE
        piece = (half, rows, d_model)
        u_first, u_second, chips, conv_mid, h_mid = pl.pallas_call(
            mamba_kernel,
            in_specs=[HBM, HBM, HBM] + [vmem] * 13,
            out_specs=[HBM] * 5,
            out_shape=[
                jax.ShapeDtypeStruct((WHOLE,) + piece, BF16),
                jax.ShapeDtypeStruct((WHOLE,) + piece, BF16),
                jax.ShapeDtypeStruct((rest,) + piece, BF16),
                jax.ShapeDtypeStruct((3, batch, inner), BF16),
                jax.ShapeDtypeStruct((batch * state, inner), F32),
            ],
            scratch_shapes=[
                pltpu.VMEM((steps, batch, d_model), BF16),
                pltpu.VMEM((3, batch, inner), BF16),
                pltpu.VMEM((3, batch, inner), BF16),
                pltpu.VMEM((inner // 128, batch * state, 128), F32),
                pltpu.VMEM((steps, batch, inner), BF16),
                pltpu.VMEM((steps, batch, inner), BF16),
                pltpu.VMEM((7, CHUNKS, rows, 2 * width), F32),
                pltpu.VMEM((5, CHUNKS) + piece, BF16),
                pltpu.VMEM((2, CHUNKS) + piece, BF16),
                pltpu.VMEM((d_model, 2 * inner), BF16),
                pltpu.VMEM((1, steps * width), F32),
                pltpu.VMEM((steps * width, steps * inner), BF16),
                pltpu.VMEM((steps * width, steps * width), BF16),
                pltpu.VMEM((128, state * 128), BF16),
                pltpu.VMEM((steps * 128, 128), BF16),
                pltpu.VMEM((steps * 128, state * 128), F32),
                pltpu.VMEM((state, inner), F32),
                pltpu.VMEM((steps, 128, 128), F32),
                pltpu.VMEM((steps, 128, inner), F32),
                pltpu.VMEM((steps, 128, inner), F32),
                pltpu.VMEM((steps, 128, inner), F32),
                pltpu.SemaphoreType.DMA((2, CHUNKS)),
                pltpu.SemaphoreType.DMA((inner // 128, CHUNKS)),
                pltpu.SemaphoreType.DMA((3, CHUNKS)),
                pltpu.SemaphoreType.DMA((inner // 128, CHUNKS)),
                pltpu.SemaphoreType.DMA((3, CHUNKS)),
                pltpu.SemaphoreType.DMA((3, CHUNKS)),
                pltpu.SemaphoreType.DMA((3, CHUNKS)),
                pltpu.SemaphoreType.DMA((3, CHUNKS)),
            ],
            compiler_params=params(collective_id=0, has_side_effects=True),
            cost_estimate=pl.CostEstimate(flops=int(8e9), bytes_accessed=int(45e6), transcendentals=0),
            name="mamba",
        )(x_steps, conv_t, h_rows, g_in, w_in, conv_w.T, conv_b, w_xp.T, g_dt, g_b, g_c, w_dt, b_dt, alog_t, d_skip, w_out)

        def run_moe(c, u_own, u_sib, states):
            extra = [] if states is None else list(states)
            return pl.pallas_call(
                functools.partial(moe_kernel, c, CHUNKS),
                grid=(1,),
                in_specs=[pl.BlockSpec((1, 24, 128), lambda i: (c, 0, 0), memory_space=pltpu.SMEM), pl.BlockSpec((1, 1, tokens), lambda i: (c, 0, 0)), vmem, vmem, vmem, vmem] + [HBM] * (5 + len(extra)),
                out_specs=[vmem, vmem, HBM, HBM],
                out_shape=[jax.ShapeDtypeStruct(piece, BF16)] * 2 + [jax.ShapeDtypeStruct(h_mid.shape, F32), jax.ShapeDtypeStruct(conv_mid.shape, BF16)],
                scratch_shapes=[
                    pltpu.VMEM((experts, d_model, ffn), BF16),
                    pltpu.VMEM((experts, d_model, ffn), BF16),
                    pltpu.VMEM((experts, ffn, d_model), BF16),
                    pltpu.SemaphoreType.DMA((3, experts)),
                    pltpu.VMEM((tokens, d_model), BF16),
                    pltpu.VMEM((slots, tokens), BF16),
                    pltpu.VMEM((slots + 2 * TILE, d_model), BF16),
                    pltpu.VMEM((slots + 2 * TILE, d_model), BF16),
                    pltpu.VMEM((slots + 2 * TILE, experts), F32),
                    pltpu.VMEM((bounce(c, CHUNKS, batch * state)[2], inner), F32),
                    pltpu.VMEM((3, bounce(c, CHUNKS, batch)[2], inner), BF16),
                    pltpu.SemaphoreType.DMA((4,)),
                ],
                input_output_aliases={11: 2, 12: 3} if extra else {},
                compiler_params=params(),
                cost_estimate=pl.CostEstimate(flops=int(12e9 / CHUNKS), bytes_accessed=int(40e6 / CHUNKS), transcendentals=0),
                name=f"moe{c}",
            )(table, pos, u_own, u_sib, g_ff, w_router.T, w_gate, w_up, w_down, h_mid, conv_mid, *extra)

        def both(keep, send, dtype):
            got = lax.ppermute(send, "tp", beside)
            chip = (keep.astype(F32) + got.astype(F32)).astype(dtype)
            return chip, lax.ppermute(chip, "tp", across)

        mids = [(u_first[c], u_second[c]) for c in range(WHOLE)]
        for c in range(WHOLE, CHUNKS):
            chip = chips[c - WHOLE]
            far = lax.ppermute(chip, "tp", across)
            x_own = lax.dynamic_slice(x_steps, (half * core, c * rows, 0), (half, rows, d_model))
            u_own = (x_own.astype(F32) + (chip.astype(F32) + far.astype(F32))).astype(BF16)
            mids.append((u_own, lax.ppermute(u_own, "tp", beside)))

        y_steps = jnp.zeros((steps, batch, d_model), BF16)
        states = None
        for c in range(CHUNKS):
            u_own, u_sib = mids[c]
            o_keep, o_send, *states = run_moe(c, u_own, u_sib, states)
            chip, far = both(o_keep, o_send, BF16)
            y_own = (u_own.astype(F32) + (chip.astype(F32) + far.astype(F32))).astype(BF16)
            y_sib = lax.ppermute(y_own, "tp", beside)
            y_steps = lax.dynamic_update_slice(y_steps, y_own, (half * core, c * rows, 0))
            y_steps = lax.dynamic_update_slice(y_steps, y_sib, (half * (1 - core), c * rows, 0))
        ssm_out, conv_out = states
        ssm_fin = jnp.transpose(ssm_out.reshape(batch, state, inner), (0, 2, 1))
        return y_steps, jnp.transpose(conv_out, (1, 2, 0)), ssm_fin

    return jax.shard_map(layer_steps, mesh=mesh, in_specs=in_specs, out_specs=out_specs, check_vma=False)
```

```python
import functools

import jax
import jax.numpy as jnp
from jax import lax
from jax.experimental import pallas as pl
from jax.experimental.pallas import tpu as pltpu
from jax.sharding import PartitionSpec as P

EPSILON = 1e-6
CHUNKS = 4
ROW_ALIGN = 16
TILE = 128
GROUP = 2
RING = 6
WHOLE = 2
F32 = jnp.float32
BF16 = jnp.bfloat16
HBM = pl.BlockSpec(memory_space=pl.ANY)


def whole(shape):
    return pl.BlockSpec(shape, lambda *_: (0,) * len(shape))


def params(**kw):
    return pltpu.CompilerParams(vmem_limit_bytes=56 * 1024 * 1024, **kw)


def silu(v):
    return v * jax.nn.sigmoid(v)


def routes_kernel(ids_ref, pos_ref, tab_ref):
    chunks, _, tokens = pos_ref.shape
    steps = ids_ref.shape[0]
    rows = tokens // steps
    experts = 16
    upper = (lax.broadcasted_iota(jnp.int32, (tokens, tokens), 0) <= lax.broadcasted_iota(jnp.int32, (tokens, tokens), 1)).astype(F32).astype(BF16)
    before = (lax.broadcasted_iota(jnp.int32, (experts, experts), 1) < lax.broadcasted_iota(jnp.int32, (experts, experts), 0)).astype(F32).astype(BF16)
    lane = lax.broadcasted_iota(jnp.int32, (experts, 128), 1)
    number = lax.broadcasted_iota(jnp.int32, (experts, 128), 0).astype(F32)
    for c in range(chunks):
        g, k = c // GROUP, c % GROUP
        ids = jnp.concatenate([ids_ref[s, :, c * rows:(c + 1) * rows] for s in range(steps)], axis=1)
        hit = lax.broadcasted_iota(jnp.int32, (experts, tokens), 0) == ids
        hot = hit.astype(F32)
        rank = jnp.dot(hot.astype(BF16), upper, preferred_element_type=F32)
        count = jnp.broadcast_to(jnp.sum(hot, axis=1, keepdims=True), (experts, 128))
        blocks = jnp.floor((count + (ROW_ALIGN - 1)) * (1.0 / ROW_ALIGN))
        start = ROW_ALIGN * jnp.dot(before, blocks.astype(BF16), preferred_element_type=F32)
        pos_ref[c] = jnp.sum(hot * (start[:, :1] + rank - 1.0), axis=0, keepdims=True).astype(jnp.int32)
        tab_ref[g, 16 * k:16 * k + 16, :] = jnp.where(lane == 0, start, count).astype(jnp.int32)
        total = count if k == 0 else total + count
        if k == GROUP - 1:
            active = (total > 0.0).astype(F32)
            place = jnp.dot(before, active.astype(BF16), preferred_element_type=F32)
            listed = jnp.sum(jnp.where((place == lane.astype(F32)) & (active > 0.0), number, 0.0), axis=0, keepdims=True)
            tab_ref[g, 16 * GROUP:16 * GROUP + 1, :] = listed.astype(jnp.int32)
            tab_ref[g, 16 * GROUP + 1:16 * GROUP + 2, :] = jnp.sum(active, axis=0, keepdims=True).astype(jnp.int32)


LOG2E = 1.4426950408889634


def mamba_kernel(x_hbm, cs_hbm, h_hbm, g_ref, win3_ref, cw_ref, cb_ref, wxp_ref, gdt_ref, gb_ref, gc_ref, wdt_ref, bdt_ref, alog_ref, dskip_ref, wout_ref,
                 uo_hbm, us_hbm, chip2_hbm, chip3_hbm, co_hbm, ho_hbm,
                 x_s, cs_s, co_s, h_s, xc_s, z_s, p_s, m_s, u_s, win_ref, g4_ref, wdt4, ones_s, spread_s, left_s, wide_s, a_s, q_s, delta_s, dx_s, y_s,
                 in_sem, h_sem, out_sem, ho_sem, psend, precv, msend, mrecv):
    steps, batch, d_model = x_s.shape
    inner = cs_s.shape[2]
    state = alog_ref.shape[0]
    rank = wdt_ref.shape[0]
    width = rank + 2 * state
    lanes = steps * width
    half = steps // 2
    rows = batch // CHUNKS
    tiles = inner // 128
    me = lax.axis_index("tp")
    core = lax.rem(me, 2)
    sibling = me + 1 - 2 * core
    partner = lax.rem(me + 2, 4)

    barrier = pltpu.get_barrier_semaphore()
    for peer in (sibling, partner):
        pl.semaphore_signal(barrier, inc=1, device_id={"tp": peer}, device_id_type=pl.DeviceIdType.MESH)

    def span(c):
        return pl.ds(c * rows, rows)

    def loads(c):
        return [
            pltpu.make_async_copy(x_hbm.at[:, span(c), :], x_s.at[:, span(c), :], in_sem.at[0, c]),
            pltpu.make_async_copy(cs_hbm.at[:, span(c), :], cs_s.at[:, span(c), :], in_sem.at[1, c]),
        ]

    def state_rows(c):
        return pl.ds(c * rows * state, rows * state)

    def h_loads(c):
        return [pltpu.make_async_copy(h_hbm.at[state_rows(c), pl.ds(l * 128, 128)], h_s.at[l, state_rows(c), :], h_sem.at[l, c]) for l in range(tiles)]

    def h_stores(c):
        return [pltpu.make_async_copy(h_s.at[l, state_rows(c), :], ho_hbm.at[state_rows(c), pl.ds(l * 128, 128)], ho_sem.at[l, c]) for l in range(tiles)]

    def co_store(c):
        return pltpu.make_async_copy(co_s.at[:, span(c), :], co_hbm.at[:, span(c), :], out_sem.at[0, c])

    def remote(buf, c, src, dst, send, recv, stage, peer):
        return pltpu.make_async_remote_copy(
            src_ref=buf.at[src, c], dst_ref=buf.at[dst, c], send_sem=send.at[stage, c], recv_sem=recv.at[stage, c],
            device_id={"tp": peer}, device_id_type=pl.DeviceIdType.MESH)

    def p_beside(c):
        return remote(p_s, c, 1, 2, psend, precv, 0, sibling)

    def p_across(c):
        return remote(p_s, c, 3, 4, psend, precv, 1, partner)

    def p_back(c):
        return remote(p_s, c, 5, 6, psend, precv, 2, sibling)

    def m_beside(c):
        return remote(m_s, c, 1, 2, msend, mrecv, 0, sibling)

    def m_across(c):
        return remote(m_s, c, 3, 4, msend, mrecv, 1, partner)

    def u_back(c):
        return pltpu.make_async_remote_copy(
            src_ref=u_s.at[0, c], dst_ref=u_s.at[1, c], send_sem=msend.at[2, c], recv_sem=mrecv.at[2, c],
            device_id={"tp": sibling}, device_id_type=pl.DeviceIdType.MESH)

    for c in range(CHUNKS):
        for cp in loads(c):
            cp.start()
    for c in range(CHUNKS):
        for cp in h_loads(c):
            cp.start()

    gain = g_ref[...].astype(F32)[None, :]
    for k in range(2):
        win_ref[:, k * inner:(k + 1) * inner] = win3_ref[:, k, :]

    def project(c):
        for cp in loads(c):
            cp.wait()

        def block(i, carry):
            r = pl.multiple_of(c * rows + i * 128, 128)
            seq = [cs_s[j, pl.ds(r, 128), :].astype(F32) for j in range(3)]
            part = []
            for s in range(steps):
                x = x_s[s, pl.ds(r, 128), :].astype(F32)
                n = (x * lax.rsqrt(jnp.mean(x * x, axis=-1, keepdims=True) + EPSILON) * gain).astype(BF16)
                xz = jnp.dot(n, win_ref[...], preferred_element_type=F32).astype(BF16)
                z_s[s, pl.ds(r, 128), :] = xz[:, inner:]
                xi = xz[:, :inner]
                if s > 0:
                    co_s[s - 1, pl.ds(r, 128), :] = xi
                seq.append(xi.astype(F32))
                acc = seq[s] * cw_ref[0:1, :].astype(F32)
                for j in range(1, 4):
                    acc = acc + seq[s + j] * cw_ref[j:j + 1, :].astype(F32)
                xc = silu(acc + cb_ref[...].astype(F32)[None, :]).astype(BF16)
                xc_s[s, pl.ds(r, 128), :] = xc
                part.append(lax.dot_general(xc, wxp_ref[...], (((1,), (1,)), ((), ())), preferred_element_type=F32))
            low = jnp.concatenate(part[:2], axis=1)
            high = jnp.concatenate(part[2:], axis=1)
            q = pl.multiple_of(i * 128, 128)
            p_s[0, c, pl.ds(q, 128), :] = jnp.where(core == 0, low, high)
            p_s[1, c, pl.ds(q, 128), :] = jnp.where(core == 0, high, low)
            return carry

        lax.fori_loop(0, rows // 128, block, 0)
        co_store(c).start()

    def p_sum(c):
        p_beside(c).wait_recv()
        p_s[3, c] = p_s[0, c] + p_s[2, c]
        p_across(c).start()

    def p_whole(c):
        p_across(c).wait_recv()
        p_s[5, c] = p_s[3, c] + p_s[4, c]
        p_back(c).start()

    def scan(c):
        p_back(c).wait_recv()
        for cp in h_loads(c):
            cp.wait()

        def block(i, carry):
            r = pl.multiple_of(i * 128, 128)
            g = pl.multiple_of(c * rows + i * 128, 128)
            own, sib = p_s[5, c, pl.ds(r, 128), :], p_s[6, c, pl.ds(r, 128), :]
            p = jnp.concatenate([jnp.where(core == 0, own, sib), jnp.where(core == 0, sib, own)], axis=1)
            sq = p * p
            s1 = sq.astype(BF16)
            rest = sq - s1.astype(F32)
            s2 = rest.astype(BF16)
            s3 = (rest - s2.astype(F32)).astype(BF16)
            mean = sum(jnp.dot(v, ones_s[...], preferred_element_type=F32) for v in (s3, s2, s1))
            norm = p * lax.rsqrt(mean + EPSILON) * g4_ref[...]
            for s in range(steps):
                first = s * width + rank
                part = jnp.concatenate([norm[:, first:first + 2 * state], jnp.zeros((128, 128 - 2 * state), F32)], axis=1)
                q_s[s] = part
                hi = part.astype(BF16).astype(F32)
                mid = (part - hi).astype(BF16).astype(F32)
                low = part - hi - mid
                left_s[s * 128:(s + 1) * 128, :] = (hi + pltpu.roll(mid, 2 * state, 1) + pltpu.roll(low, 4 * state, 1)).astype(BF16)
            pre = jnp.dot(norm.astype(BF16), wdt4[...], preferred_element_type=F32)
            bias = bdt_ref[...].astype(F32)[None, :]
            for s in range(steps):
                v = pre[:, s * inner:(s + 1) * inner] + bias
                delta = jnp.maximum(v, 0.0) + jnp.log1p(jnp.exp(-jnp.abs(v)))
                delta_s[s] = delta
                dx_s[s] = delta * xc_s[s, pl.ds(g, 128), :].astype(F32)

            def widen(j, carry2):
                cols = pl.ds(pl.multiple_of(j * 256, 256), 256)
                wide_s[:, cols] = jnp.dot(left_s[...], spread_s[:, cols], preferred_element_type=F32)
                return carry2

            lax.fori_loop(0, state // 2, widen, 0)

            def tile(t, carry2):
                b = pl.multiple_of(t * 8, 8)
                base = (g + b) * state
                cut = [slice(l * 128, (l + 1) * 128) for l in range(tiles)]
                dl = [[delta_s[s, pl.ds(b, 8), k] for k in cut] for s in range(steps)]
                dx = [[dx_s[s, pl.ds(b, 8), k] for k in cut] for s in range(steps)]
                ys = [[jnp.zeros((8, 128), F32) for _ in cut] for _ in range(steps)]
                qs = [q_s[s, pl.ds(b, 8), :] for s in range(steps)]
                for n in range(state):
                    bs = [jnp.broadcast_to(qs[s][:, n:n + 1], (8, 128)) for s in range(steps)]
                    cs = [wide_s[pl.ds(s * 128 + b, 8), n * 128:(n + 1) * 128] for s in range(steps)]
                    cols = list(zip(bs, cs))
                    for l in range(tiles):
                        a = a_s[n:n + 1, cut[l]]
                        h = h_s[l, pl.ds(base + n, 8, stride=state), :]
                        for s in range(steps):
                            h = jnp.exp2(dl[s][l] * a) * h + dx[s][l] * cols[s][0]
                            ys[s][l] = ys[s][l] + h * cols[s][1]
                        h_s[l, pl.ds(base + n, 8, stride=state), :] = h
                for s in range(steps):
                    for l in range(tiles):
                        y_s[s, pl.ds(b, 8), cut[l]] = ys[s][l]
                return carry2

            lax.fori_loop(0, 16, tile, 0)
            for s in range(steps):
                xc = xc_s[s, pl.ds(g, 128), :].astype(F32)
                yg = ((y_s[s] + dskip_ref[...][None, :] * xc) * silu(z_s[s, pl.ds(g, 128), :].astype(F32))).astype(BF16)
                out = jnp.dot(yg, wout_ref[...], preferred_element_type=F32).astype(BF16)
                m_s[lax.rem(core + s // half, 2), c, s % half, pl.ds(r, 128), :] = out
            return carry

        lax.fori_loop(0, rows // 128, block, 0)
        for cp in h_stores(c):
            cp.start()
        m_beside(c).start()

    def chip_out(c):
        return pltpu.make_async_copy(m_s.at[3, c], (chip2_hbm, chip3_hbm)[c - WHOLE], out_sem.at[1, c])

    def m_sum(c):
        m_beside(c).wait_recv()
        for s in range(half):
            m_s[3, c, s] = (m_s[0, c, s].astype(F32) + m_s[2, c, s].astype(F32)).astype(BF16)
        if c < WHOLE:
            m_across(c).start()
        else:
            chip_out(c).start()

    def uo_out(c):
        return pltpu.make_async_copy(u_s.at[0, c], uo_hbm.at[c], out_sem.at[1, c])

    def us_out(c):
        return pltpu.make_async_copy(u_s.at[1, c], us_hbm.at[c], out_sem.at[2, c])

    def m_whole(c):
        m_across(c).wait_recv()
        for s in range(half):
            x = x_s[core * half + s, span(c), :].astype(F32)
            u_s[0, c, s] = (x + (m_s[3, c, s].astype(F32) + m_s[4, c, s].astype(F32))).astype(BF16)
        u_back(c).start()
        uo_out(c).start()

    project(0)
    pl.semaphore_wait(barrier, 2)
    p_beside(0).start()
    project(1)
    p_beside(1).start()
    p_sum(0)
    project(2)
    p_beside(2).start()
    p_sum(1)
    project(3)
    p_beside(3).start()
    p_sum(2)
    p_whole(0)

    wdt4[...] = jnp.zeros_like(wdt4)
    for s in range(steps):
        wdt4[s * width:s * width + rank, s * inner:(s + 1) * inner] = wdt_ref[...]

    def group(v):
        step, col = v // width, lax.rem(v, width)
        return step * 4 + (col >= rank).astype(jnp.int32) + (col >= rank + state).astype(jnp.int32)

    gi = group(lax.broadcasted_iota(jnp.int32, (lanes, lanes), 0))
    gj = group(lax.broadcasted_iota(jnp.int32, (lanes, lanes), 1))
    inv = jnp.where(lax.rem(gj, 4) == 0, 1.0 / rank, 1.0 / state)
    ones_s[...] = jnp.where(gi == gj, inv, 0.0).astype(BF16)
    ki = lax.broadcasted_iota(jnp.int32, spread_s.shape, 0)
    kj = lax.broadcasted_iota(jnp.int32, spread_s.shape, 1)
    spread_s[...] = ((lax.rem(ki, 2 * state) == state + kj // 128) & (ki < 6 * state)).astype(F32).astype(BF16)
    for s in range(steps):
        for ref, at in ((gdt_ref, 0), (gb_ref, rank), (gc_ref, rank + state)):
            g4_ref[:, s * width + at:s * width + at + ref.shape[0]] = ref[...].astype(F32)[None, :]
    a_s[...] = -LOG2E * jnp.exp(alog_ref[...])

    p_sum(3)
    p_whole(1)
    scan(0)
    p_whole(2)
    p_whole(3)
    m_sum(0)
    scan(1)
    m_sum(1)
    scan(2)
    m_sum(2)
    m_whole(0)
    scan(3)
    m_sum(3)
    for c in range(1, WHOLE):
        m_whole(c)
    for c in range(WHOLE):
        u_back(c).wait_recv()
        us_out(c).start()
    for c in range(CHUNKS):
        p_beside(c).wait_send()
        p_across(c).wait_send()
        p_back(c).wait_send()
        m_beside(c).wait_send()
        co_store(c).wait()
        for cp in h_stores(c):
            cp.wait()
        if c < WHOLE:
            m_across(c).wait_send()
            u_back(c).wait_send()
            uo_out(c).wait()
            us_out(c).wait()
        else:
            chip_out(c).wait()


def moe_kernel(g, calls, *refs):
    tab_ref, pos_ref = refs[:2]
    us = refs[2:2 + 2 * GROUP]
    gff_ref, wr_ref, wg_ref, wu_ref, wd_ref, h_hbm, cv_hbm = refs[2 + 2 * GROUP:9 + 2 * GROUP]
    outs = refs[-14 - 2 * GROUP:-14]
    ho_hbm, co_hbm, wg, wu, wd, sems, m_s, hot_s, in_s, out_s, prob_s, h_s, cv_s, st_sem = refs[-14:]
    _, half, rows, d_model = us[0].shape
    experts = wr_ref.shape[0]
    tokens = 2 * half * rows
    slots = hot_s.shape[0] // GROUP
    room = in_s.shape[0] // GROUP
    core = lax.rem(lax.axis_index("tp"), 2)
    active = tab_ref[0, 16 * GROUP + 1, 0]

    def copies(i):
        e = tab_ref[0, 16 * GROUP, i]
        slot = lax.rem(i, RING)
        return [pltpu.make_async_copy(src.at[e], dst.at[slot], sems.at[k, slot]) for k, (src, dst) in enumerate(((wg_ref, wg), (wu_ref, wu), (wd_ref, wd)))]

    def fetch(i):
        @pl.when(i < active)
        def _():
            for cp in copies(i):
                cp.start()

    for i in range(RING - 1):
        fetch(i)
    h_span = pl.ds(g * h_s.shape[0], h_s.shape[0])
    cv_span = pl.ds(g * cv_s.shape[1], cv_s.shape[1])
    pulls = [pltpu.make_async_copy(h_hbm.at[h_span, :], h_s, st_sem.at[0]), pltpu.make_async_copy(cv_hbm.at[:, cv_span, :], cv_s, st_sem.at[1])]
    pushes = [pltpu.make_async_copy(h_s, ho_hbm.at[h_span, :], st_sem.at[2]), pltpu.make_async_copy(cv_s, co_hbm.at[:, cv_span, :], st_sem.at[3])]
    for cp in pulls:
        cp.start()
    gain = gff_ref[...].astype(F32)[None, :]
    for j in range(GROUP):
        for k in range(2):
            src = us[k * GROUP + j]
            first = j * tokens + jnp.where(core == k, 0, half * rows)
            for s in range(half):
                u = src[0, s].astype(F32)
                m = u * lax.rsqrt(jnp.mean(u * u, axis=-1, keepdims=True) + EPSILON) * gain
                m_s[pl.ds(pl.multiple_of(first + s * rows, rows), rows), :] = m.astype(BF16)

    down = lax.broadcasted_iota(jnp.int32, (256, tokens), 0).astype(F32).astype(BF16)
    for j in range(GROUP):
        pos = pos_ref[j]

        def order(i, carry):
            r = pl.multiple_of(i * 256, 256)
            local = jnp.where((pos >= r) & (pos < r + 256), pos - r, -1).astype(F32).astype(BF16)
            hot = jnp.where(down == local, jnp.ones((), BF16), jnp.zeros((), BF16))
            hot_s[pl.ds(j * slots + r, 256), :] = hot
            m = jnp.dot(hot, m_s[j * tokens:(j + 1) * tokens, :], preferred_element_type=F32).astype(BF16)
            at = pl.ds(j * room + r, 256)
            in_s[at, :] = m
            out_s[at, :] = jnp.zeros((256, d_model), BF16)
            logits = lax.dot_general(m, wr_ref[...], (((1,), (1,)), ((), ())), preferred_element_type=F32)
            ex = jnp.exp(logits - jnp.max(logits, axis=-1, keepdims=True))
            prob_s[at, :] = ex / jnp.sum(ex, axis=-1, keepdims=True)
            return carry

        lax.fori_loop(0, slots // 256, order, 0)
    for pull, push in zip(pulls, pushes):
        pull.wait()
        push.start()

    def feed(e, slot, r, size):
        m = in_s[pl.ds(r, size), :]
        gate = jnp.dot(m, wg[slot], preferred_element_type=F32)
        up = jnp.dot(m, wu[slot], preferred_element_type=F32)
        q = (silu(gate) * up).astype(BF16)
        lane = lax.broadcasted_iota(jnp.int32, (size, experts), 1)
        prob = jnp.sum(jnp.where(lane == e, prob_s[pl.ds(r, size), :], 0.0), axis=-1, keepdims=True)
        out_s[pl.ds(r, size), :] = (prob * jnp.dot(q, wd[slot], preferred_element_type=F32)).astype(BF16)

    def expert(i, carry):
        e = tab_ref[0, 16 * GROUP, i]
        slot = lax.rem(i, RING)
        fetch(i + RING - 1)
        for cp in copies(i):
            cp.wait()

        def part(j, c1):
            start = tab_ref[0, 16 * j + e, 0] + j * room
            count = tab_ref[0, 16 * j + e, 1]
            big = (count + TILE - 1) // (2 * TILE)

            def tile(k, c2):
                feed(e, slot, pl.multiple_of(start + k * (2 * TILE), ROW_ALIGN), 2 * TILE)
                return c2

            lax.fori_loop(0, big, tile, 0)

            @pl.when(count > big * (2 * TILE))
            def _():
                feed(e, slot, pl.multiple_of(start + big * (2 * TILE), ROW_ALIGN), TILE)

            return c1

        return lax.fori_loop(0, GROUP, part, carry)

    lax.fori_loop(0, active, expert, 0)

    def restore(j, k, dst):
        first = jnp.where(core == k, 0, half * rows)
        for s in range(half):
            hot = hot_s[j * slots:(j + 1) * slots, pl.ds(pl.multiple_of(first + s * rows, rows), rows)]
            got = lax.dot_general(hot, out_s[j * room:j * room + slots, :], (((0,), (0,)), ((), ())), preferred_element_type=F32)
            dst[s] = got.astype(BF16)

    for j in range(GROUP):
        for k in range(2):
            restore(j, k, outs[k * GROUP + j])
    for cp in pushes:
        cp.wait()


def solution(mesh):
    act_spec = P(None, "dp", None)
    state_spec = P("dp", "tp", None)
    in_specs = (act_spec, state_spec, state_spec, act_spec, P(None), P(None, None, "tp"), P("tp", None), P("tp"), P("tp", None), P(None), P(None), P(None), P(None, "tp"), P("tp"), P("tp", None), P("tp"), P("tp", None), P(None), P(None, None), P(None, None, "tp"), P(None, None, "tp"), P(None, "tp", None))
    out_specs = (act_spec, state_spec, state_spec)
    across = [(0, 2), (2, 0), (1, 3), (3, 1)]
    beside = [(0, 1), (1, 0), (2, 3), (3, 2)]

    def layer_steps(x_steps, conv_state, ssm_state, expert_ids, g_in, w_in, conv_w, conv_b, w_xp, g_dt, g_b, g_c, w_dt, b_dt, a_log, d_skip, w_out, g_ff, w_router, w_gate, w_up, w_down):
        steps, batch, d_model = x_steps.shape
        inner = w_in.shape[2]
        rank = w_dt.shape[0]
        state = a_log.shape[1]
        experts, _, ffn = w_gate.shape
        width = rank + 2 * state
        half = steps // 2
        rows = batch // CHUNKS
        tokens = steps * rows
        slots = tokens + experts * ROW_ALIGN
        core = lax.rem(lax.axis_index("tp"), 2)

        conv_t = jnp.transpose(conv_state, (2, 0, 1))
        h_rows = jnp.transpose(ssm_state, (0, 2, 1)).reshape(batch * state, inner)
        alog_t = a_log.T

        ids = jnp.transpose(expert_ids, (0, 2, 1))
        pos, table = pl.pallas_call(
            routes_kernel,
            out_shape=(jax.ShapeDtypeStruct((CHUNKS, 1, tokens), jnp.int32), jax.ShapeDtypeStruct((CHUNKS // GROUP, 16 * GROUP + 8, 128), jnp.int32)),
            compiler_params=params(),
            name="routes",
        )(ids)

        vmem = pl.BlockSpec(memory_space=pltpu.VMEM)
        piece = (half, rows, d_model)
        u_first, u_second, *chips, conv_mid, h_mid = pl.pallas_call(
            mamba_kernel,
            in_specs=[HBM, HBM, HBM] + [vmem] * 13,
            out_specs=[HBM] * 6,
            out_shape=[
                jax.ShapeDtypeStruct((WHOLE,) + piece, BF16),
                jax.ShapeDtypeStruct((WHOLE,) + piece, BF16),
                jax.ShapeDtypeStruct(piece, BF16),
                jax.ShapeDtypeStruct(piece, BF16),
                jax.ShapeDtypeStruct((3, batch, inner), BF16),
                jax.ShapeDtypeStruct((batch * state, inner), F32),
            ],
            scratch_shapes=[
                pltpu.VMEM((steps, batch, d_model), BF16),
                pltpu.VMEM((3, batch, inner), BF16),
                pltpu.VMEM((3, batch, inner), BF16),
                pltpu.VMEM((inner // 128, batch * state, 128), F32),
                pltpu.VMEM((steps, batch, inner), BF16),
                pltpu.VMEM((steps, batch, inner), BF16),
                pltpu.VMEM((7, CHUNKS, rows, 2 * width), F32),
                pltpu.VMEM((5, CHUNKS) + piece, BF16),
                pltpu.VMEM((2, CHUNKS) + piece, BF16),
                pltpu.VMEM((d_model, 2 * inner), BF16),
                pltpu.VMEM((1, steps * width), F32),
                pltpu.VMEM((steps * width, steps * inner), BF16),
                pltpu.VMEM((steps * width, steps * width), BF16),
                pltpu.VMEM((128, state * 128), BF16),
                pltpu.VMEM((steps * 128, 128), BF16),
                pltpu.VMEM((steps * 128, state * 128), F32),
                pltpu.VMEM((state, inner), F32),
                pltpu.VMEM((steps, 128, 128), F32),
                pltpu.VMEM((steps, 128, inner), F32),
                pltpu.VMEM((steps, 128, inner), F32),
                pltpu.VMEM((steps, 128, inner), F32),
                pltpu.SemaphoreType.DMA((2, CHUNKS)),
                pltpu.SemaphoreType.DMA((inner // 128, CHUNKS)),
                pltpu.SemaphoreType.DMA((3, CHUNKS)),
                pltpu.SemaphoreType.DMA((inner // 128, CHUNKS)),
                pltpu.SemaphoreType.DMA((3, CHUNKS)),
                pltpu.SemaphoreType.DMA((3, CHUNKS)),
                pltpu.SemaphoreType.DMA((3, CHUNKS)),
                pltpu.SemaphoreType.DMA((3, CHUNKS)),
            ],
            compiler_params=params(collective_id=0, has_side_effects=True),
            cost_estimate=pl.CostEstimate(flops=int(8e9), bytes_accessed=int(45e6), transcendentals=0),
            name="mamba",
        )(x_steps, conv_t, h_rows, g_in, w_in, conv_w.T, conv_b, w_xp.T, g_dt, g_b, g_c, w_dt, b_dt, alog_t, d_skip, w_out)

        calls = CHUNKS // GROUP
        room = slots + 2 * TILE

        def run_moe(g, u_args, u_specs, states):
            extra = [] if states is None else list(states)
            return pl.pallas_call(
                functools.partial(moe_kernel, g, calls),
                grid=(1,),
                in_specs=[pl.BlockSpec((1, 16 * GROUP + 8, 128), lambda i: (g, 0, 0), memory_space=pltpu.SMEM), pl.BlockSpec((GROUP, 1, tokens), lambda i: (g, 0, 0))] + u_specs + [vmem, vmem] + [HBM] * (5 + len(extra)),
                out_specs=[vmem] * (2 * GROUP) + [HBM, HBM],
                out_shape=[jax.ShapeDtypeStruct(piece, BF16)] * (2 * GROUP) + [jax.ShapeDtypeStruct(h_mid.shape, F32), jax.ShapeDtypeStruct(conv_mid.shape, BF16)],
                scratch_shapes=[
                    pltpu.VMEM((RING, d_model, ffn), BF16),
                    pltpu.VMEM((RING, d_model, ffn), BF16),
                    pltpu.VMEM((RING, ffn, d_model), BF16),
                    pltpu.SemaphoreType.DMA((3, RING)),
                    pltpu.VMEM((GROUP * tokens, d_model), BF16),
                    pltpu.VMEM((GROUP * slots, tokens), BF16),
                    pltpu.VMEM((GROUP * room, d_model), BF16),
                    pltpu.VMEM((GROUP * room, d_model), BF16),
                    pltpu.VMEM((GROUP * room, experts), F32),
                    pltpu.VMEM((batch * state // calls, inner), F32),
                    pltpu.VMEM((3, batch // calls, inner), BF16),
                    pltpu.SemaphoreType.DMA((4,)),
                ],
                input_output_aliases={9 + 2 * GROUP: 2 * GROUP, 10 + 2 * GROUP: 2 * GROUP + 1} if extra else {},
                compiler_params=params(),
                cost_estimate=pl.CostEstimate(flops=int(6e9), bytes_accessed=int(40e6), transcendentals=0),
                name=f"moe{g}",
            )(table, pos, *u_args, g_ff, w_router.T, w_gate, w_up, w_down, h_mid, conv_mid, *extra)

        def both(keep, send, dtype):
            got = lax.ppermute(send, "tp", beside)
            chip = (keep.astype(F32) + got.astype(F32)).astype(dtype)
            return chip, lax.ppermute(chip, "tp", across)

        owns = {}
        spot = {}
        for c in range(WHOLE):
            spot[c] = (u_first, u_second, pl.BlockSpec((1,) + piece, lambda i, c=c: (c, 0, 0, 0)))
            owns[c] = lambda c=c: u_first[c]
        for c in range(WHOLE, CHUNKS):
            chip = chips[c - WHOLE]
            far = lax.ppermute(chip, "tp", across)
            x_own = lax.dynamic_slice(x_steps, (half * core, c * rows, 0), (half, rows, d_model))
            u_own = (x_own.astype(F32) + (chip.astype(F32) + far.astype(F32))).astype(BF16)
            u_sib = lax.ppermute(u_own, "tp", beside)
            spot[c] = (u_own[None], u_sib[None], pl.BlockSpec((1,) + piece, lambda i: (0, 0, 0, 0)))
            owns[c] = lambda u_own=u_own: u_own

        y_steps = jnp.zeros((steps, batch, d_model), BF16)
        states = None
        for g in range(calls):
            group = [spot[g * GROUP + j] for j in range(GROUP)]
            got = run_moe(g, [v[0] for v in group] + [v[1] for v in group], [v[2] for v in group] * 2, states)
            states = got[2 * GROUP:]
            for j in range(GROUP):
                c = g * GROUP + j
                chip, far = both(got[j], got[GROUP + j], BF16)
                y_own = (owns[c]().astype(F32) + (chip.astype(F32) + far.astype(F32))).astype(BF16)
                y_sib = lax.ppermute(y_own, "tp", beside)
                y_steps = lax.dynamic_update_slice(y_steps, y_own, (half * core, c * rows, 0))
                y_steps = lax.dynamic_update_slice(y_steps, y_sib, (half * (1 - core), c * rows, 0))
        ssm_out, conv_out = states
        ssm_fin = jnp.transpose(ssm_out.reshape(batch, state, inner), (0, 2, 1))
        return y_steps, jnp.transpose(conv_out, (1, 2, 0)), ssm_fin

    return jax.shard_map(layer_steps, mesh=mesh, in_specs=in_specs, out_specs=out_specs, check_vma=False)
```

```python
import functools

import jax
import jax.numpy as jnp
from jax import lax
from jax.experimental import pallas as pl
from jax.experimental.pallas import tpu as pltpu
from jax.sharding import PartitionSpec as P


EPSILON = 1e-6
CHUNKS = 4
ROW_ALIGN = 16
TILE = 128
GROUP = 2
RING = 6
WHOLE = 2
F32 = jnp.float32
BF16 = jnp.bfloat16
HBM = pl.BlockSpec(memory_space=pl.ANY)


def params(**kw):
    return pltpu.CompilerParams(vmem_limit_bytes=56 * 1024 * 1024, **kw)


def row(ref):
    return ref[...].astype(F32).reshape(1, -1)


def norm_rows(v, gain):
    return v * lax.rsqrt(jnp.mean(v * v, axis=-1, keepdims=True) + EPSILON) * gain


def mm_t(a, b):
    return lax.dot_general(a, b, (((1,), (1,)), ((), ())), preferred_element_type=F32)


def silu(v):
    return v * jax.nn.sigmoid(v)


def routes_kernel(ids_ref, pos_ref, tab_ref):
    chunks, _, tokens = pos_ref.shape
    steps = ids_ref.shape[0]
    rows = tokens // steps
    experts = 16
    upper = (lax.broadcasted_iota(jnp.int32, (tokens, tokens), 0) <= lax.broadcasted_iota(jnp.int32, (tokens, tokens), 1)).astype(F32).astype(BF16)
    before = (lax.broadcasted_iota(jnp.int32, (experts, experts), 1) < lax.broadcasted_iota(jnp.int32, (experts, experts), 0)).astype(F32).astype(BF16)
    lane = lax.broadcasted_iota(jnp.int32, (experts, 128), 1)
    number = lax.broadcasted_iota(jnp.int32, (experts, 128), 0).astype(F32)
    for c in range(chunks):
        g, k = c // GROUP, c % GROUP
        ids = jnp.concatenate([ids_ref[s, :, c * rows:(c + 1) * rows] for s in range(steps)], axis=1)
        hit = lax.broadcasted_iota(jnp.int32, (experts, tokens), 0) == ids
        hot = hit.astype(F32)
        rank = jnp.dot(hot.astype(BF16), upper, preferred_element_type=F32)
        count = jnp.broadcast_to(jnp.sum(hot, axis=1, keepdims=True), (experts, 128))
        blocks = jnp.floor((count + (ROW_ALIGN - 1)) * (1.0 / ROW_ALIGN))
        start = ROW_ALIGN * jnp.dot(before, blocks.astype(BF16), preferred_element_type=F32)
        pos_ref[c] = jnp.sum(hot * (start[:, :1] + rank - 1.0), axis=0, keepdims=True).astype(jnp.int32)
        tab_ref[g, 16 * k:16 * k + 16, :] = jnp.where(lane == 0, start, count).astype(jnp.int32)
        total = count if k == 0 else total + count
        if k == GROUP - 1:
            active = (total > 0.0).astype(F32)
            place = jnp.dot(before, active.astype(BF16), preferred_element_type=F32)
            listed = jnp.sum(jnp.where((place == lane.astype(F32)) & (active > 0.0), number, 0.0), axis=0, keepdims=True)
            tab_ref[g, 16 * GROUP:16 * GROUP + 1, :] = listed.astype(jnp.int32)
            tab_ref[g, 16 * GROUP + 1:16 * GROUP + 2, :] = jnp.sum(active, axis=0, keepdims=True).astype(jnp.int32)


LOG2E = 1.4426950408889634


def mamba_kernel(x_hbm, cs_hbm, h_hbm, g_ref, win3_ref, cw_ref, cb_ref, wxp_ref, gdt_ref, gb_ref, gc_ref, wdt_ref, bdt_ref, alog_ref, dskip_ref, wout_ref,
                 uo_hbm, us_hbm, chip2_hbm, chip3_hbm, co_hbm, ho_hbm,
                 x_s, cs_s, co_s, h_s, xc_s, z_s, p_s, m_s, u_s, win_ref, g4_ref, wdt4, ones_s, even_s, odd_s, a_s, q_s, delta_s, dx_s, y_s,
                 in_sem, h_sem, out_sem, ho_sem, psend, precv, msend, mrecv):
    steps, batch, _ = x_s.shape
    inner = cs_s.shape[2]
    state = alog_ref.shape[0]
    rank = wdt_ref.shape[0]
    width = rank + 2 * state
    lanes = steps * width
    half = steps // 2
    rows = batch // CHUNKS
    tiles = inner // 128
    me = lax.axis_index("tp")
    core = lax.rem(me, 2)
    sibling = me + 1 - 2 * core
    partner = lax.rem(me + 2, 4)

    barrier = pltpu.get_barrier_semaphore()
    for peer in (sibling, partner):
        pl.semaphore_signal(barrier, inc=1, device_id={"tp": peer}, device_id_type=pl.DeviceIdType.MESH)

    def span(c):
        return pl.ds(c * rows, rows)

    def loads(c):
        return [
            pltpu.make_async_copy(x_hbm.at[:, span(c), :], x_s.at[:, span(c), :], in_sem.at[0, c]),
            pltpu.make_async_copy(cs_hbm.at[:, span(c), :], cs_s.at[:, span(c), :], in_sem.at[1, c]),
        ]

    def state_rows(c):
        return pl.ds(c * rows * state, rows * state)

    def h_loads(c):
        return [pltpu.make_async_copy(h_hbm.at[state_rows(c), pl.ds(l * 128, 128)], h_s.at[l, state_rows(c), :], h_sem.at[l, c]) for l in range(tiles)]

    def h_stores(c):
        return [pltpu.make_async_copy(h_s.at[l, state_rows(c), :], ho_hbm.at[state_rows(c), pl.ds(l * 128, 128)], ho_sem.at[l, c]) for l in range(tiles)]

    def co_store(c):
        return pltpu.make_async_copy(co_s.at[:, span(c), :], co_hbm.at[:, span(c), :], out_sem.at[0, c])

    def remote(buf, c, src, dst, send, recv, stage, peer):
        return pltpu.make_async_remote_copy(
            src_ref=buf.at[src, c], dst_ref=buf.at[dst, c], send_sem=send.at[stage, c], recv_sem=recv.at[stage, c],
            device_id={"tp": peer}, device_id_type=pl.DeviceIdType.MESH)

    def p_beside(c):
        return remote(p_s, c, 1, 2, psend, precv, 0, sibling)

    def p_across(c):
        return remote(p_s, c, 3, 4, psend, precv, 1, partner)

    def p_back(c):
        return remote(p_s, c, 5, 6, psend, precv, 2, sibling)

    def m_beside(c):
        return remote(m_s, c, 1, 2, msend, mrecv, 0, sibling)

    def m_across(c):
        return remote(m_s, c, 3, 4, msend, mrecv, 1, partner)

    def u_back(c):
        return pltpu.make_async_remote_copy(
            src_ref=u_s.at[0, c], dst_ref=u_s.at[1, c], send_sem=msend.at[2, c], recv_sem=mrecv.at[2, c],
            device_id={"tp": sibling}, device_id_type=pl.DeviceIdType.MESH)

    for c in range(CHUNKS):
        for cp in loads(c):
            cp.start()
    for c in range(CHUNKS):
        for cp in h_loads(c):
            cp.start()

    gain = row(g_ref)
    for k in range(2):
        win_ref[:, k * inner:(k + 1) * inner] = win3_ref[:, k, :]

    def project(c):
        for cp in loads(c):
            cp.wait()

        def block(i, carry):
            r = pl.multiple_of(c * rows + i * 128, 128)
            seq = [cs_s[j, pl.ds(r, 128), :].astype(F32) for j in range(3)]
            part = []
            for s in range(steps):
                x = x_s[s, pl.ds(r, 128), :].astype(F32)
                n = norm_rows(x, gain).astype(BF16)
                xz = jnp.dot(n, win_ref[...], preferred_element_type=F32).astype(BF16)
                z_s[s, pl.ds(r, 128), :] = xz[:, inner:]
                xi = xz[:, :inner]
                if s > 0:
                    co_s[s - 1, pl.ds(r, 128), :] = xi
                seq.append(xi.astype(F32))
                acc = seq[s] * cw_ref[0:1, :].astype(F32)
                for j in range(1, 4):
                    acc = acc + seq[s + j] * cw_ref[j:j + 1, :].astype(F32)
                xc = silu(acc + row(cb_ref)).astype(BF16)
                xc_s[s, pl.ds(r, 128), :] = xc
                part.append(mm_t(xc, wxp_ref[...]))
            low = jnp.concatenate(part[:2], axis=1)
            high = jnp.concatenate(part[2:], axis=1)
            q = pl.multiple_of(i * 128, 128)
            p_s[0, c, pl.ds(q, 128), :] = jnp.where(core == 0, low, high)
            p_s[1, c, pl.ds(q, 128), :] = jnp.where(core == 0, high, low)
            return carry

        lax.fori_loop(0, rows // 128, block, 0)
        co_store(c).start()

    def p_sum(c):
        p_beside(c).wait_recv()
        p_s[3, c] = p_s[0, c] + p_s[2, c]
        p_across(c).start()

    def p_whole(c):
        p_across(c).wait_recv()
        p_s[5, c] = p_s[3, c] + p_s[4, c]
        p_back(c).start()

    def scan(c):
        p_back(c).wait_recv()
        for cp in h_loads(c):
            cp.wait()

        def block(i, carry):
            r = pl.multiple_of(i * 128, 128)
            g = pl.multiple_of(c * rows + i * 128, 128)
            own, sib = p_s[5, c, pl.ds(r, 128), :], p_s[6, c, pl.ds(r, 128), :]
            p = jnp.concatenate([jnp.where(core == 0, own, sib), jnp.where(core == 0, sib, own)], axis=1)
            sq = p * p
            s1 = sq.astype(BF16)
            rest = sq - s1.astype(F32)
            s2 = rest.astype(BF16)
            s3 = (rest - s2.astype(F32)).astype(BF16)
            mean = sum(jnp.dot(v, ones_s[...], preferred_element_type=F32) for v in (s3, s2, s1))
            norm = p * lax.rsqrt(mean + EPSILON) * g4_ref[...]
            for s in range(steps):
                first = s * width + rank
                q_s[s] = jnp.concatenate([norm[:, first:first + 2 * state], jnp.zeros((128, 128 - 2 * state), F32)], axis=1)
            pre = jnp.dot(norm.astype(BF16), wdt4[...], preferred_element_type=F32)
            bias = row(bdt_ref)
            for s in range(steps):
                v = pre[:, s * inner:(s + 1) * inner] + bias
                delta = jnp.maximum(v, 0.0) + jnp.log1p(jnp.exp(-jnp.abs(v)))
                delta_s[s] = delta
                dx_s[s] = delta * xc_s[s, pl.ds(g, 128), :].astype(F32)

            def spread(t, wide):
                b = pl.multiple_of(t * 8, 8)
                qs = [q_s[s, pl.ds(b, 8), :] for s in range(steps)]
                for n in range(2 * state):
                    for s in range(steps):
                        wide[s, n] = jnp.broadcast_to(qs[s][:, n:n + 1], (8, 128))

            def advance(t, wide):
                b = pl.multiple_of(t * 8, 8)
                base = (g + b) * state
                cut = [slice(l * 128, (l + 1) * 128) for l in range(tiles)]
                dl = [[delta_s[s, pl.ds(b, 8), k] for k in cut] for s in range(steps)]
                dx = [[dx_s[s, pl.ds(b, 8), k] for k in cut] for s in range(steps)]
                ys = [[None] * tiles for _ in range(steps)]
                for n in range(state):
                    for l in range(tiles):
                        a = a_s[n:n + 1, cut[l]]
                        spot = (l, pl.ds(base + n, 8, stride=state))
                        h = h_s[spot]
                        for s in range(steps):
                            h = jnp.exp2(dl[s][l] * a) * h + dx[s][l] * wide[s, n]
                            hc = h * wide[s, n + state]
                            ys[s][l] = hc if n == 0 else ys[s][l] + hc
                        h_s[spot] = h
                for s in range(steps):
                    for l in range(tiles):
                        y_s[s, pl.ds(b, 8), cut[l]] = ys[s][l]

            def pair(i, carry2):
                t = 2 * i
                spread(t + 1, odd_s)
                advance(t, even_s)
                spread(jnp.minimum(t + 2, 14), even_s)
                advance(t + 1, odd_s)
                return carry2

            spread(0, even_s)
            lax.fori_loop(0, 8, pair, 0)
            for s in range(steps):
                xc = xc_s[s, pl.ds(g, 128), :].astype(F32)
                yg = ((y_s[s] + row(dskip_ref) * xc) * silu(z_s[s, pl.ds(g, 128), :].astype(F32))).astype(BF16)
                out = jnp.dot(yg, wout_ref[...], preferred_element_type=F32).astype(BF16)
                m_s[lax.rem(core + s // half, 2), c, s % half, pl.ds(r, 128), :] = out
            return carry

        lax.fori_loop(0, rows // 128, block, 0)
        for cp in h_stores(c):
            cp.start()
        m_beside(c).start()

    def chip_out(c):
        return pltpu.make_async_copy(m_s.at[3, c], (chip2_hbm, chip3_hbm)[c - WHOLE], out_sem.at[1, c])

    def m_sum(c):
        m_beside(c).wait_recv()
        for s in range(half):
            m_s[3, c, s] = (m_s[0, c, s].astype(F32) + m_s[2, c, s].astype(F32)).astype(BF16)
        if c < WHOLE:
            m_across(c).start()
        else:
            chip_out(c).start()

    def uo_out(c):
        return pltpu.make_async_copy(u_s.at[0, c], uo_hbm.at[c], out_sem.at[1, c])

    def us_out(c):
        return pltpu.make_async_copy(u_s.at[1, c], us_hbm.at[c], out_sem.at[2, c])

    def m_whole(c):
        m_across(c).wait_recv()
        for s in range(half):
            x = x_s[core * half + s, span(c), :].astype(F32)
            u_s[0, c, s] = (x + (m_s[3, c, s].astype(F32) + m_s[4, c, s].astype(F32))).astype(BF16)
        u_back(c).start()
        uo_out(c).start()

    project(0)
    pl.semaphore_wait(barrier, 2)
    p_beside(0).start()
    project(1)
    p_beside(1).start()
    p_sum(0)
    project(2)
    p_beside(2).start()
    p_sum(1)
    project(3)
    p_beside(3).start()
    p_sum(2)
    p_whole(0)

    wdt4[...] = jnp.zeros_like(wdt4)
    for s in range(steps):
        wdt4[s * width:s * width + rank, s * inner:(s + 1) * inner] = wdt_ref[...]

    def group(v):
        step, col = v // width, lax.rem(v, width)
        return step * 4 + (col >= rank).astype(jnp.int32) + (col >= rank + state).astype(jnp.int32)

    gi = group(lax.broadcasted_iota(jnp.int32, (lanes, lanes), 0))
    gj = group(lax.broadcasted_iota(jnp.int32, (lanes, lanes), 1))
    inv = jnp.where(lax.rem(gj, 4) == 0, 1.0 / rank, 1.0 / state)
    ones_s[...] = jnp.where(gi == gj, inv, 0.0).astype(BF16)
    for s in range(steps):
        for ref, at in ((gdt_ref, 0), (gb_ref, rank), (gc_ref, rank + state)):
            g4_ref[:, s * width + at:s * width + at + ref.shape[0]] = row(ref)
    a_s[...] = -LOG2E * jnp.exp(alog_ref[...])

    p_sum(3)
    p_whole(1)
    scan(0)
    p_whole(2)
    p_whole(3)
    m_sum(0)
    scan(1)
    m_sum(1)
    scan(2)
    m_sum(2)
    m_whole(0)
    scan(3)
    m_sum(3)
    for c in range(1, WHOLE):
        m_whole(c)
    for c in range(WHOLE):
        u_back(c).wait_recv()
        us_out(c).start()
    for c in range(CHUNKS):
        p_beside(c).wait_send()
        p_across(c).wait_send()
        p_back(c).wait_send()
        m_beside(c).wait_send()
        co_store(c).wait()
        for cp in h_stores(c):
            cp.wait()
        if c < WHOLE:
            m_across(c).wait_send()
            u_back(c).wait_send()
            uo_out(c).wait()
            us_out(c).wait()
        else:
            chip_out(c).wait()


def moe_kernel(g, *refs):
    tab_ref, pos_ref = refs[:2]
    us = refs[2:2 + 2 * GROUP]
    gff_ref, wr_ref, wg_ref, wu_ref, wd_ref, h_hbm, cv_hbm = refs[2 + 2 * GROUP:9 + 2 * GROUP]
    outs = refs[-14 - 2 * GROUP:-14]
    ho_hbm, co_hbm, wg, wu, wd, sems, m_s, hot_s, in_s, out_s, prob_s, h_s, cv_s, st_sem = refs[-14:]
    _, half, rows, d_model = us[0].shape
    experts = wr_ref.shape[0]
    tokens = 2 * half * rows
    slots = hot_s.shape[0] // GROUP
    room = in_s.shape[0] // GROUP
    core = lax.rem(lax.axis_index("tp"), 2)
    active = tab_ref[0, 16 * GROUP + 1, 0]

    def copies(i):
        e = tab_ref[0, 16 * GROUP, i]
        slot = lax.rem(i, RING)
        return [pltpu.make_async_copy(src.at[e], dst.at[slot], sems.at[k, slot]) for k, (src, dst) in enumerate(((wg_ref, wg), (wu_ref, wu), (wd_ref, wd)))]

    def fetch(i):
        @pl.when(i < active)
        def _():
            for cp in copies(i):
                cp.start()

    for i in range(RING - 1):
        fetch(i)
    h_span = pl.ds(g * h_s.shape[0], h_s.shape[0])
    cv_span = pl.ds(g * cv_s.shape[1], cv_s.shape[1])
    pulls = [pltpu.make_async_copy(h_hbm.at[h_span, :], h_s, st_sem.at[0]), pltpu.make_async_copy(cv_hbm.at[:, cv_span, :], cv_s, st_sem.at[1])]
    pushes = [pltpu.make_async_copy(h_s, ho_hbm.at[h_span, :], st_sem.at[2]), pltpu.make_async_copy(cv_s, co_hbm.at[:, cv_span, :], st_sem.at[3])]
    for cp in pulls:
        cp.start()
    gain = row(gff_ref)
    for j in range(GROUP):
        for k in range(2):
            src = us[k * GROUP + j]
            first = j * tokens + jnp.where(core == k, 0, half * rows)
            for s in range(half):
                u = src[0, s].astype(F32)
                m = norm_rows(u, gain)
                m_s[pl.ds(pl.multiple_of(first + s * rows, rows), rows), :] = m.astype(BF16)

    down = lax.broadcasted_iota(jnp.int32, (256, tokens), 0).astype(F32).astype(BF16)
    for j in range(GROUP):
        pos = pos_ref[j]

        def order(i, carry):
            r = pl.multiple_of(i * 256, 256)
            local = jnp.where((pos >= r) & (pos < r + 256), pos - r, -1).astype(F32).astype(BF16)
            hot = jnp.where(down == local, jnp.ones((), BF16), jnp.zeros((), BF16))
            hot_s[pl.ds(j * slots + r, 256), :] = hot
            m = jnp.dot(hot, m_s[j * tokens:(j + 1) * tokens, :], preferred_element_type=F32).astype(BF16)
            at = pl.ds(j * room + r, 256)
            in_s[at, :] = m
            out_s[at, :] = jnp.zeros((256, d_model), BF16)
            logits = mm_t(m, wr_ref[...])
            ex = jnp.exp(logits - jnp.max(logits, axis=-1, keepdims=True))
            prob_s[at, :] = ex / jnp.sum(ex, axis=-1, keepdims=True)
            return carry

        lax.fori_loop(0, slots // 256, order, 0)
    for pull, push in zip(pulls, pushes):
        pull.wait()
        push.start()

    def feed(e, slot, r, size):
        m = in_s[pl.ds(r, size), :]
        gate = jnp.dot(m, wg[slot], preferred_element_type=F32)
        up = jnp.dot(m, wu[slot], preferred_element_type=F32)
        q = (silu(gate) * up).astype(BF16)
        lane = lax.broadcasted_iota(jnp.int32, (size, experts), 1)
        prob = jnp.sum(jnp.where(lane == e, prob_s[pl.ds(r, size), :], 0.0), axis=-1, keepdims=True)
        out_s[pl.ds(r, size), :] = (prob * jnp.dot(q, wd[slot], preferred_element_type=F32)).astype(BF16)

    def expert(i, carry):
        e = tab_ref[0, 16 * GROUP, i]
        slot = lax.rem(i, RING)
        fetch(i + RING - 1)
        for cp in copies(i):
            cp.wait()

        def part(j, c1):
            start = tab_ref[0, 16 * j + e, 0] + j * room
            count = tab_ref[0, 16 * j + e, 1]
            big = (count + TILE - 1) // (2 * TILE)

            def tile(k, c2):
                feed(e, slot, pl.multiple_of(start + k * (2 * TILE), ROW_ALIGN), 2 * TILE)
                return c2

            lax.fori_loop(0, big, tile, 0)

            @pl.when(count > big * (2 * TILE))
            def _():
                feed(e, slot, pl.multiple_of(start + big * (2 * TILE), ROW_ALIGN), TILE)

            return c1

        return lax.fori_loop(0, GROUP, part, carry)

    lax.fori_loop(0, active, expert, 0)

    def restore(j, k, dst):
        first = jnp.where(core == k, 0, half * rows)
        for s in range(half):
            hot = hot_s[j * slots:(j + 1) * slots, pl.ds(pl.multiple_of(first + s * rows, rows), rows)]
            got = lax.dot_general(hot, out_s[j * room:j * room + slots, :], (((0,), (0,)), ((), ())), preferred_element_type=F32)
            dst[s] = got.astype(BF16)

    for j in range(GROUP):
        for k in range(2):
            restore(j, k, outs[k * GROUP + j])
    for cp in pushes:
        cp.wait()


def solution(mesh):
    act_spec = P(None, "dp", None)
    state_spec = P("dp", "tp", None)
    in_specs = (act_spec, state_spec, state_spec, act_spec, P(None), P(None, None, "tp"), P("tp", None), P("tp"), P("tp", None), P(None), P(None), P(None), P(None, "tp"), P("tp"), P("tp", None), P("tp"), P("tp", None), P(None), P(None, None), P(None, None, "tp"), P(None, None, "tp"), P(None, "tp", None))
    out_specs = (act_spec, state_spec, state_spec)
    across = [(0, 2), (2, 0), (1, 3), (3, 1)]
    beside = [(0, 1), (1, 0), (2, 3), (3, 2)]

    def layer_steps(x_steps, conv_state, ssm_state, expert_ids, g_in, w_in, conv_w, conv_b, w_xp, g_dt, g_b, g_c, w_dt, b_dt, a_log, d_skip, w_out, g_ff, w_router, w_gate, w_up, w_down):
        steps, batch, d_model = x_steps.shape
        inner = w_in.shape[2]
        rank = w_dt.shape[0]
        state = a_log.shape[1]
        experts, _, ffn = w_gate.shape
        width = rank + 2 * state
        half = steps // 2
        rows = batch // CHUNKS
        tokens = steps * rows
        slots = tokens + experts * ROW_ALIGN
        core = lax.rem(lax.axis_index("tp"), 2)

        conv_t = jnp.transpose(conv_state, (2, 0, 1))
        h_rows = jnp.transpose(ssm_state, (0, 2, 1)).reshape(batch * state, inner)
        alog_t = a_log.T

        ids = jnp.transpose(expert_ids, (0, 2, 1))
        pos, table = pl.pallas_call(
            routes_kernel,
            out_shape=(jax.ShapeDtypeStruct((CHUNKS, 1, tokens), jnp.int32), jax.ShapeDtypeStruct((CHUNKS // GROUP, 16 * GROUP + 8, 128), jnp.int32)),
            compiler_params=params(),
            name="routes",
        )(ids)

        vmem = pl.BlockSpec(memory_space=pltpu.VMEM)
        piece = (half, rows, d_model)
        u_first, u_second, *chips, conv_mid, h_mid = pl.pallas_call(
            mamba_kernel,
            in_specs=[HBM, HBM, HBM] + [vmem] * 13,
            out_specs=[HBM] * 6,
            out_shape=[
                jax.ShapeDtypeStruct((WHOLE,) + piece, BF16),
                jax.ShapeDtypeStruct((WHOLE,) + piece, BF16),
                jax.ShapeDtypeStruct(piece, BF16),
                jax.ShapeDtypeStruct(piece, BF16),
                jax.ShapeDtypeStruct((3, batch, inner), BF16),
                jax.ShapeDtypeStruct((batch * state, inner), F32),
            ],
            scratch_shapes=[
                pltpu.VMEM((steps, batch, d_model), BF16),
                pltpu.VMEM((3, batch, inner), BF16),
                pltpu.VMEM((3, batch, inner), BF16),
                pltpu.VMEM((inner // 128, batch * state, 128), F32),
                pltpu.VMEM((steps, batch, inner), BF16),
                pltpu.VMEM((steps, batch, inner), BF16),
                pltpu.VMEM((7, CHUNKS, rows, 2 * width), F32),
                pltpu.VMEM((5, CHUNKS) + piece, BF16),
                pltpu.VMEM((2, CHUNKS) + piece, BF16),
                pltpu.VMEM((d_model, 2 * inner), BF16),
                pltpu.VMEM((1, steps * width), F32),
                pltpu.VMEM((steps * width, steps * inner), BF16),
                pltpu.VMEM((steps * width, steps * width), BF16),
                pltpu.VMEM((steps, 2 * state, 8, 128), F32),
                pltpu.VMEM((steps, 2 * state, 8, 128), F32),
                pltpu.VMEM((state, inner), F32),
                pltpu.VMEM((steps, 128, 128), F32),
                pltpu.VMEM((steps, 128, inner), F32),
                pltpu.VMEM((steps, 128, inner), F32),
                pltpu.VMEM((steps, 128, inner), F32),
                pltpu.SemaphoreType.DMA((2, CHUNKS)),
                pltpu.SemaphoreType.DMA((inner // 128, CHUNKS)),
                pltpu.SemaphoreType.DMA((3, CHUNKS)),
                pltpu.SemaphoreType.DMA((inner // 128, CHUNKS)),
                pltpu.SemaphoreType.DMA((3, CHUNKS)),
                pltpu.SemaphoreType.DMA((3, CHUNKS)),
                pltpu.SemaphoreType.DMA((3, CHUNKS)),
                pltpu.SemaphoreType.DMA((3, CHUNKS)),
            ],
            compiler_params=params(collective_id=0, has_side_effects=True),
            cost_estimate=pl.CostEstimate(flops=int(8e9), bytes_accessed=int(45e6), transcendentals=0),
            name="mamba",
        )(x_steps, conv_t, h_rows, g_in, w_in, conv_w.T, conv_b, w_xp.T, g_dt, g_b, g_c, w_dt, b_dt, alog_t, d_skip, w_out)

        calls = CHUNKS // GROUP
        room = slots + 2 * TILE

        def run_moe(g, u_args, u_specs, states):
            extra = [] if states is None else list(states)
            return pl.pallas_call(
                functools.partial(moe_kernel, g),
                grid=(1,),
                in_specs=[pl.BlockSpec((1, 16 * GROUP + 8, 128), lambda i: (g, 0, 0), memory_space=pltpu.SMEM), pl.BlockSpec((GROUP, 1, tokens), lambda i: (g, 0, 0))] + u_specs + [vmem, vmem] + [HBM] * (5 + len(extra)),
                out_specs=[vmem] * (2 * GROUP) + [HBM, HBM],
                out_shape=[jax.ShapeDtypeStruct(piece, BF16)] * (2 * GROUP) + [jax.ShapeDtypeStruct(h_mid.shape, F32), jax.ShapeDtypeStruct(conv_mid.shape, BF16)],
                scratch_shapes=[
                    pltpu.VMEM((RING, d_model, ffn), BF16),
                    pltpu.VMEM((RING, d_model, ffn), BF16),
                    pltpu.VMEM((RING, ffn, d_model), BF16),
                    pltpu.SemaphoreType.DMA((3, RING)),
                    pltpu.VMEM((GROUP * tokens, d_model), BF16),
                    pltpu.VMEM((GROUP * slots, tokens), BF16),
                    pltpu.VMEM((GROUP * room, d_model), BF16),
                    pltpu.VMEM((GROUP * room, d_model), BF16),
                    pltpu.VMEM((GROUP * room, experts), F32),
                    pltpu.VMEM((batch * state // calls, inner), F32),
                    pltpu.VMEM((3, batch // calls, inner), BF16),
                    pltpu.SemaphoreType.DMA((4,)),
                ],
                input_output_aliases={9 + 2 * GROUP: 2 * GROUP, 10 + 2 * GROUP: 2 * GROUP + 1} if extra else {},
                compiler_params=params(),
                cost_estimate=pl.CostEstimate(flops=int(6e9), bytes_accessed=int(40e6), transcendentals=0),
            )(table, pos, *u_args, g_ff, w_router.T, w_gate, w_up, w_down, h_mid, conv_mid, *extra)

        def both(keep, send, dtype):
            got = lax.ppermute(send, "tp", beside)
            chip = (keep.astype(F32) + got.astype(F32)).astype(dtype)
            return chip, lax.ppermute(chip, "tp", across)

        owns = {}
        spot = {}
        for c in range(WHOLE):
            spot[c] = (u_first, u_second, pl.BlockSpec((1,) + piece, lambda i, c=c: (c, 0, 0, 0)))
            owns[c] = lambda c=c: u_first[c]
        for c in range(WHOLE, CHUNKS):
            chip = chips[c - WHOLE]
            far = lax.ppermute(chip, "tp", across)
            x_own = lax.dynamic_slice(x_steps, (half * core, c * rows, 0), (half, rows, d_model))
            u_own = (x_own.astype(F32) + (chip.astype(F32) + far.astype(F32))).astype(BF16)
            u_sib = lax.ppermute(u_own, "tp", beside)
            spot[c] = (u_own[None], u_sib[None], pl.BlockSpec((1,) + piece, lambda i: (0, 0, 0, 0)))
            owns[c] = lambda u_own=u_own: u_own

        y_steps = jnp.zeros((steps, batch, d_model), BF16)
        states = None
        for g in range(calls):
            group = [spot[g * GROUP + j] for j in range(GROUP)]
            got = run_moe(g, [v[0] for v in group] + [v[1] for v in group], [v[2] for v in group] * 2, states)
            states = got[2 * GROUP:]
            for j in range(GROUP):
                c = g * GROUP + j
                chip, far = both(got[j], got[GROUP + j], BF16)
                y_own = (owns[c]().astype(F32) + (chip.astype(F32) + far.astype(F32))).astype(BF16)
                y_sib = lax.ppermute(y_own, "tp", beside)
                y_steps = lax.dynamic_update_slice(y_steps, y_own, (half * core, c * rows, 0))
                y_steps = lax.dynamic_update_slice(y_steps, y_sib, (half * (1 - core), c * rows, 0))
        ssm_out, conv_out = states
        ssm_fin = jnp.transpose(ssm_out.reshape(batch, state, inner), (0, 2, 1))
        return y_steps, jnp.transpose(conv_out, (1, 2, 0)), ssm_fin

    return jax.shard_map(layer_steps, mesh=mesh, in_specs=in_specs, out_specs=out_specs, check_vma=False)
```

```python
import functools

import jax
import jax.numpy as jnp
from jax import lax
from jax.experimental import pallas as pl
from jax.experimental.pallas import tpu as pltpu
from jax.sharding import PartitionSpec as P


EPSILON = 1e-6
CHUNKS = 4
ROW_ALIGN = 16
TILE = 128
GROUP = 2
RING = 6
WHOLE = 2
F32 = jnp.float32
BF16 = jnp.bfloat16
HBM = pl.BlockSpec(memory_space=pl.ANY)


def params(**kw):
    return pltpu.CompilerParams(vmem_limit_bytes=56 * 1024 * 1024, **kw)


def row(ref):
    return ref[...].astype(F32).reshape(1, -1)


def norm_rows(v, gain):
    return v * lax.rsqrt(jnp.mean(v * v, axis=-1, keepdims=True) + EPSILON) * gain


def mm_t(a, b):
    return lax.dot_general(a, b, (((1,), (1,)), ((), ())), preferred_element_type=F32)


def silu(v):
    return v * jax.nn.sigmoid(v)


def routes_kernel(ids_ref, pos_ref, tab_ref):
    chunks, _, tokens = pos_ref.shape
    steps = ids_ref.shape[0]
    rows = tokens // steps
    experts = 16
    upper = (lax.broadcasted_iota(jnp.int32, (tokens, tokens), 0) <= lax.broadcasted_iota(jnp.int32, (tokens, tokens), 1)).astype(F32).astype(BF16)
    before = (lax.broadcasted_iota(jnp.int32, (experts, experts), 1) < lax.broadcasted_iota(jnp.int32, (experts, experts), 0)).astype(F32).astype(BF16)
    lane = lax.broadcasted_iota(jnp.int32, (experts, 128), 1)
    number = lax.broadcasted_iota(jnp.int32, (experts, 128), 0).astype(F32)
    for c in range(chunks):
        g, k = c // GROUP, c % GROUP
        ids = jnp.concatenate([ids_ref[s, :, c * rows:(c + 1) * rows] for s in range(steps)], axis=1)
        hit = lax.broadcasted_iota(jnp.int32, (experts, tokens), 0) == ids
        hot = hit.astype(F32)
        rank = jnp.dot(hot.astype(BF16), upper, preferred_element_type=F32)
        count = jnp.broadcast_to(jnp.sum(hot, axis=1, keepdims=True), (experts, 128))
        blocks = jnp.floor((count + (ROW_ALIGN - 1)) * (1.0 / ROW_ALIGN))
        start = ROW_ALIGN * jnp.dot(before, blocks.astype(BF16), preferred_element_type=F32)
        pos_ref[c] = jnp.sum(hot * (start[:, :1] + rank - 1.0), axis=0, keepdims=True).astype(jnp.int32)
        tab_ref[g, 16 * k:16 * k + 16, :] = jnp.where(lane == 0, start, count).astype(jnp.int32)
        total = count if k == 0 else total + count
        if k == GROUP - 1:
            active = (total > 0.0).astype(F32)
            place = jnp.dot(before, active.astype(BF16), preferred_element_type=F32)
            listed = jnp.sum(jnp.where((place == lane.astype(F32)) & (active > 0.0), number, 0.0), axis=0, keepdims=True)
            tab_ref[g, 16 * GROUP:16 * GROUP + 1, :] = listed.astype(jnp.int32)
            tab_ref[g, 16 * GROUP + 1:16 * GROUP + 2, :] = jnp.sum(active, axis=0, keepdims=True).astype(jnp.int32)


LOG2E = 1.4426950408889634


def mamba_kernel(x_hbm, cs_hbm, h_hbm, g_ref, win3_ref, cw_ref, cb_ref, wxp_ref, gdt_ref, gb_ref, gc_ref, wdt_ref, bdt_ref, alog_ref, dskip_ref, wout_ref,
                 uo_hbm, us_hbm, chip2_hbm, chip3_hbm, co_hbm, ho_hbm,
                 x_s, cs_s, co_s, h_s, xc_s, z_s, p_s, m_s, u_s, win_ref, g4_ref, wdt4, ones_s, even_s, odd_s, a_s, q_s, delta_s, dx_s, y_s,
                 in_sem, h_sem, out_sem, ho_sem, psend, precv, msend, mrecv):
    steps, batch, _ = x_s.shape
    inner = cs_s.shape[2]
    state = alog_ref.shape[0]
    rank = wdt_ref.shape[0]
    width = rank + 2 * state
    lanes = steps * width
    half = steps // 2
    rows = batch // CHUNKS
    tiles = inner // 128
    me = lax.axis_index("tp")
    core = lax.rem(me, 2)
    sibling = me + 1 - 2 * core
    partner = lax.rem(me + 2, 4)

    barrier = pltpu.get_barrier_semaphore()
    for peer in (sibling, partner):
        pl.semaphore_signal(barrier, inc=1, device_id={"tp": peer}, device_id_type=pl.DeviceIdType.MESH)

    def span(c):
        return pl.ds(c * rows, rows)

    def loads(c):
        return [
            pltpu.make_async_copy(x_hbm.at[:, span(c), :], x_s.at[:, span(c), :], in_sem.at[0, c]),
            pltpu.make_async_copy(cs_hbm.at[:, span(c), :], cs_s.at[:, span(c), :], in_sem.at[1, c]),
        ]

    def state_rows(c):
        return pl.ds(c * rows * state, rows * state)

    def h_loads(c):
        return [pltpu.make_async_copy(h_hbm.at[state_rows(c), pl.ds(l * 128, 128)], h_s.at[l, state_rows(c), :], h_sem.at[l, c]) for l in range(tiles)]

    def h_stores(c):
        return [pltpu.make_async_copy(h_s.at[l, state_rows(c), :], ho_hbm.at[state_rows(c), pl.ds(l * 128, 128)], ho_sem.at[l, c]) for l in range(tiles)]

    def co_store(c):
        return pltpu.make_async_copy(co_s.at[:, span(c), :], co_hbm.at[:, span(c), :], out_sem.at[0, c])

    def remote(buf, c, src, dst, send, recv, stage, peer):
        return pltpu.make_async_remote_copy(
            src_ref=buf.at[src, c], dst_ref=buf.at[dst, c], send_sem=send.at[stage, c], recv_sem=recv.at[stage, c],
            device_id={"tp": peer}, device_id_type=pl.DeviceIdType.MESH)

    def p_beside(c):
        return remote(p_s, c, 1, 2, psend, precv, 0, sibling)

    def p_across(c):
        return remote(p_s, c, 3, 4, psend, precv, 1, partner)

    def p_back(c):
        return remote(p_s, c, 5, 6, psend, precv, 2, sibling)

    def m_beside(c):
        return remote(m_s, c, 1, 2, msend, mrecv, 0, sibling)

    def m_across(c):
        return remote(m_s, c, 3, 4, msend, mrecv, 1, partner)

    def u_back(c):
        return pltpu.make_async_remote_copy(
            src_ref=u_s.at[0, c], dst_ref=u_s.at[1, c], send_sem=msend.at[2, c], recv_sem=mrecv.at[2, c],
            device_id={"tp": sibling}, device_id_type=pl.DeviceIdType.MESH)

    for c in range(CHUNKS):
        for cp in loads(c):
            cp.start()
    for c in range(CHUNKS):
        for cp in h_loads(c):
            cp.start()

    gain = row(g_ref)
    for k in range(2):
        win_ref[:, k * inner:(k + 1) * inner] = win3_ref[:, k, :]

    def project(c):
        for cp in loads(c):
            cp.wait()

        def block(i, carry):
            r = pl.multiple_of(c * rows + i * 128, 128)
            seq = [cs_s[j, pl.ds(r, 128), :].astype(F32) for j in range(3)]
            part = []
            for s in range(steps):
                x = x_s[s, pl.ds(r, 128), :].astype(F32)
                n = norm_rows(x, gain).astype(BF16)
                xz = jnp.dot(n, win_ref[...], preferred_element_type=F32).astype(BF16)
                z_s[s, pl.ds(r, 128), :] = xz[:, inner:]
                xi = xz[:, :inner]
                if s > 0:
                    co_s[s - 1, pl.ds(r, 128), :] = xi
                seq.append(xi.astype(F32))
                acc = seq[s] * cw_ref[0:1, :].astype(F32)
                for j in range(1, 4):
                    acc = acc + seq[s + j] * cw_ref[j:j + 1, :].astype(F32)
                xc = silu(acc + row(cb_ref)).astype(BF16)
                xc_s[s, pl.ds(r, 128), :] = xc
                part.append(mm_t(xc, wxp_ref[...]))
            low = jnp.concatenate(part[:2], axis=1)
            high = jnp.concatenate(part[2:], axis=1)
            q = pl.multiple_of(i * 128, 128)
            p_s[0, c, pl.ds(q, 128), :] = jnp.where(core == 0, low, high)
            p_s[1, c, pl.ds(q, 128), :] = jnp.where(core == 0, high, low)
            return carry

        lax.fori_loop(0, rows // 128, block, 0)
        co_store(c).start()

    def p_sum(c):
        p_beside(c).wait_recv()
        p_s[3, c] = p_s[0, c] + p_s[2, c]
        p_across(c).start()

    def p_whole(c):
        p_across(c).wait_recv()
        p_s[5, c] = p_s[3, c] + p_s[4, c]
        p_back(c).start()

    def scan(c):
        p_back(c).wait_recv()
        for cp in h_loads(c):
            cp.wait()

        def block(i, carry):
            r = pl.multiple_of(i * 128, 128)
            g = pl.multiple_of(c * rows + i * 128, 128)
            own, sib = p_s[5, c, pl.ds(r, 128), :], p_s[6, c, pl.ds(r, 128), :]
            p = jnp.concatenate([jnp.where(core == 0, own, sib), jnp.where(core == 0, sib, own)], axis=1)
            sq = p * p
            s1 = sq.astype(BF16)
            rest = sq - s1.astype(F32)
            s2 = rest.astype(BF16)
            s3 = (rest - s2.astype(F32)).astype(BF16)
            mean = sum(jnp.dot(v, ones_s[...], preferred_element_type=F32) for v in (s3, s2, s1))
            norm = p * lax.rsqrt(mean + EPSILON) * g4_ref[...]
            for s in range(steps):
                first = s * width + rank
                q_s[s] = jnp.concatenate([norm[:, first:first + 2 * state], jnp.zeros((128, 128 - 2 * state), F32)], axis=1)
            pre = jnp.dot(norm.astype(BF16), wdt4[...], preferred_element_type=F32)
            bias = row(bdt_ref)
            for s in range(steps):
                v = pre[:, s * inner:(s + 1) * inner] + bias
                delta = jnp.maximum(v, 0.0) + jnp.log1p(jnp.exp(-jnp.abs(v)))
                delta_s[s] = delta
                dx_s[s] = delta * xc_s[s, pl.ds(g, 128), :].astype(F32)

            def spread(t, wide):
                b = pl.multiple_of(t * 8, 8)
                qs = [q_s[s, pl.ds(b, 8), :] for s in range(steps)]
                for n in range(2 * state):
                    for s in range(steps):
                        wide[s, n] = jnp.broadcast_to(qs[s][:, n:n + 1], (8, 128))

            def advance(t, wide):
                b = pl.multiple_of(t * 8, 8)
                base = (g + b) * state
                cut = [slice(l * 128, (l + 1) * 128) for l in range(tiles)]
                dl = [[delta_s[s, pl.ds(b, 8), k] for k in cut] for s in range(steps)]
                dx = [[dx_s[s, pl.ds(b, 8), k] for k in cut] for s in range(steps)]
                ys = [[None] * tiles for _ in range(steps)]
                for n in range(state):
                    for l in range(tiles):
                        a = a_s[n:n + 1, cut[l]]
                        spot = (l, pl.ds(base + n, 8, stride=state))
                        h = h_s[spot]
                        for s in range(steps):
                            h = jnp.exp2(dl[s][l] * a) * h + dx[s][l] * wide[s, n]
                            hc = h * wide[s, n + state]
                            ys[s][l] = hc if n == 0 else ys[s][l] + hc
                        h_s[spot] = h
                for s in range(steps):
                    for l in range(tiles):
                        y_s[s, pl.ds(b, 8), cut[l]] = ys[s][l]

            def pair(i, carry2):
                t = 2 * i
                spread(t + 1, odd_s)
                advance(t, even_s)
                spread(jnp.minimum(t + 2, 14), even_s)
                advance(t + 1, odd_s)
                return carry2

            spread(0, even_s)
            lax.fori_loop(0, 8, pair, 0)
            for s in range(steps):
                xc = xc_s[s, pl.ds(g, 128), :].astype(F32)
                yg = ((y_s[s] + row(dskip_ref) * xc) * silu(z_s[s, pl.ds(g, 128), :].astype(F32))).astype(BF16)
                out = jnp.dot(yg, wout_ref[...], preferred_element_type=F32).astype(BF16)
                m_s[lax.rem(core + s // half, 2), c, s % half, pl.ds(r, 128), :] = out
            return carry

        lax.fori_loop(0, rows // 128, block, 0)
        for cp in h_stores(c):
            cp.start()
        m_beside(c).start()

    def chip_out(c):
        return pltpu.make_async_copy(m_s.at[3, c], (chip2_hbm, chip3_hbm)[c - WHOLE], out_sem.at[1, c])

    def m_sum(c):
        m_beside(c).wait_recv()
        for s in range(half):
            m_s[3, c, s] = (m_s[0, c, s].astype(F32) + m_s[2, c, s].astype(F32)).astype(BF16)
        if c < WHOLE:
            m_across(c).start()
        else:
            chip_out(c).start()

    def uo_out(c):
        return pltpu.make_async_copy(u_s.at[0, c], uo_hbm.at[c], out_sem.at[1, c])

    def us_out(c):
        return pltpu.make_async_copy(u_s.at[1, c], us_hbm.at[c], out_sem.at[2, c])

    def m_whole(c):
        m_across(c).wait_recv()
        for s in range(half):
            x = x_s[core * half + s, span(c), :].astype(F32)
            u_s[0, c, s] = (x + (m_s[3, c, s].astype(F32) + m_s[4, c, s].astype(F32))).astype(BF16)
        u_back(c).start()
        uo_out(c).start()

    project(0)
    pl.semaphore_wait(barrier, 2)
    p_beside(0).start()
    project(1)
    p_beside(1).start()
    p_sum(0)
    project(2)
    p_beside(2).start()
    p_sum(1)
    project(3)
    p_beside(3).start()
    p_sum(2)
    p_whole(0)

    wdt4[...] = jnp.zeros_like(wdt4)
    for s in range(steps):
        wdt4[s * width:s * width + rank, s * inner:(s + 1) * inner] = wdt_ref[...]

    def group(v):
        step, col = v // width, lax.rem(v, width)
        return step * 4 + (col >= rank).astype(jnp.int32) + (col >= rank + state).astype(jnp.int32)

    gi = group(lax.broadcasted_iota(jnp.int32, (lanes, lanes), 0))
    gj = group(lax.broadcasted_iota(jnp.int32, (lanes, lanes), 1))
    inv = jnp.where(lax.rem(gj, 4) == 0, 1.0 / rank, 1.0 / state)
    ones_s[...] = jnp.where(gi == gj, inv, 0.0).astype(BF16)
    for s in range(steps):
        for ref, at in ((gdt_ref, 0), (gb_ref, rank), (gc_ref, rank + state)):
            g4_ref[:, s * width + at:s * width + at + ref.shape[0]] = row(ref)
    a_s[...] = -LOG2E * jnp.exp(alog_ref[...])

    p_sum(3)
    p_whole(1)
    scan(0)
    p_whole(2)
    p_whole(3)
    m_sum(0)
    scan(1)
    m_sum(1)
    scan(2)
    m_sum(2)
    m_whole(0)
    scan(3)
    m_sum(3)
    for c in range(1, WHOLE):
        m_whole(c)
    for c in range(WHOLE):
        u_back(c).wait_recv()
        us_out(c).start()
    for c in range(CHUNKS):
        p_beside(c).wait_send()
        p_across(c).wait_send()
        p_back(c).wait_send()
        m_beside(c).wait_send()
        co_store(c).wait()
        for cp in h_stores(c):
            cp.wait()
        if c < WHOLE:
            m_across(c).wait_send()
            u_back(c).wait_send()
            uo_out(c).wait()
            us_out(c).wait()
        else:
            chip_out(c).wait()


def moe_kernel(g, *refs):
    tab_ref, pos_ref = refs[:2]
    us = refs[2:2 + 2 * GROUP]
    gff_ref, wr_ref, wg_ref, wu_ref, wd_ref, h_hbm, cv_hbm = refs[2 + 2 * GROUP:9 + 2 * GROUP]
    refs = refs[9 + 2 * GROUP + (2 if g else 0):]
    outs = refs[:2 * GROUP]
    ho_hbm, co_hbm = refs[2 * GROUP:2 * GROUP + 2]
    wg, wu, wd, sems, m_s, hot_s, in_s, out_s, prob_s, h_s, cv_s, st_sem = refs[-12:]
    _, half, rows, d_model = us[0].shape
    experts = wr_ref.shape[0]
    tokens = 2 * half * rows
    slots = hot_s.shape[0] // GROUP
    room = in_s.shape[0] // GROUP
    core = lax.rem(lax.axis_index("tp"), 2)
    active = tab_ref[0, 16 * GROUP + 1, 0]

    def copies(i):
        e = tab_ref[0, 16 * GROUP, i]
        slot = lax.rem(i, RING)
        return [pltpu.make_async_copy(src.at[e], dst.at[slot], sems.at[k, slot]) for k, (src, dst) in enumerate(((wg_ref, wg), (wu_ref, wu), (wd_ref, wd)))]

    def fetch(i):
        @pl.when(i < active)
        def _():
            for cp in copies(i):
                cp.start()

    for i in range(RING - 1):
        fetch(i)
    h_span = pl.ds(g * h_s.shape[0], h_s.shape[0])
    cv_span = pl.ds(g * cv_s.shape[1], cv_s.shape[1])
    pulls = [pltpu.make_async_copy(h_hbm.at[h_span, :], h_s, st_sem.at[0]), pltpu.make_async_copy(cv_hbm.at[:, cv_span, :], cv_s, st_sem.at[1])]
    pushes = [pltpu.make_async_copy(h_s, ho_hbm.at[h_span, :], st_sem.at[2]), pltpu.make_async_copy(cv_s, co_hbm.at[:, cv_span, :], st_sem.at[3])]
    for cp in pulls:
        cp.start()
    gain = row(gff_ref)
    for j in range(GROUP):
        for k in range(2):
            src = us[k * GROUP + j]
            first = j * tokens + jnp.where(core == k, 0, half * rows)
            for s in range(half):
                u = src[0, s].astype(F32)
                m = norm_rows(u, gain)
                m_s[pl.ds(pl.multiple_of(first + s * rows, rows), rows), :] = m.astype(BF16)

    down = lax.broadcasted_iota(jnp.int32, (256, tokens), 0).astype(F32).astype(BF16)
    for j in range(GROUP):
        pos = pos_ref[j]

        def order(i, carry):
            r = pl.multiple_of(i * 256, 256)
            local = jnp.where((pos >= r) & (pos < r + 256), pos - r, -1).astype(F32).astype(BF16)
            hot = jnp.where(down == local, jnp.ones((), BF16), jnp.zeros((), BF16))
            hot_s[pl.ds(j * slots + r, 256), :] = hot
            m = jnp.dot(hot, m_s[j * tokens:(j + 1) * tokens, :], preferred_element_type=F32).astype(BF16)
            at = pl.ds(j * room + r, 256)
            in_s[at, :] = m
            out_s[at, :] = jnp.zeros((256, d_model), BF16)
            logits = mm_t(m, wr_ref[...])
            ex = jnp.exp(logits - jnp.max(logits, axis=-1, keepdims=True))
            prob_s[at, :] = ex / jnp.sum(ex, axis=-1, keepdims=True)
            return carry

        lax.fori_loop(0, slots // 256, order, 0)
    for pull, push in zip(pulls, pushes):
        pull.wait()
        push.start()

    def feed(e, slot, r, size):
        m = in_s[pl.ds(r, size), :]
        gate = jnp.dot(m, wg[slot], preferred_element_type=F32)
        up = jnp.dot(m, wu[slot], preferred_element_type=F32)
        q = (silu(gate) * up).astype(BF16)
        lane = lax.broadcasted_iota(jnp.int32, (size, experts), 1)
        prob = jnp.sum(jnp.where(lane == e, prob_s[pl.ds(r, size), :], 0.0), axis=-1, keepdims=True)
        out_s[pl.ds(r, size), :] = (prob * jnp.dot(q, wd[slot], preferred_element_type=F32)).astype(BF16)

    def expert(i, carry):
        e = tab_ref[0, 16 * GROUP, i]
        slot = lax.rem(i, RING)
        fetch(i + RING - 1)
        for cp in copies(i):
            cp.wait()

        def part(j, c1):
            start = tab_ref[0, 16 * j + e, 0] + j * room
            count = tab_ref[0, 16 * j + e, 1]
            big = (count + TILE - 1) // (2 * TILE)

            def tile(k, c2):
                feed(e, slot, pl.multiple_of(start + k * (2 * TILE), ROW_ALIGN), 2 * TILE)
                return c2

            lax.fori_loop(0, big, tile, 0)

            @pl.when(count > big * (2 * TILE))
            def _():
                feed(e, slot, pl.multiple_of(start + big * (2 * TILE), ROW_ALIGN), TILE)

            return c1

        return lax.fori_loop(0, GROUP, part, carry)

    lax.fori_loop(0, active, expert, 0)

    def restore(j, k, dst):
        first = jnp.where(core == k, 0, half * rows)
        for s in range(half):
            hot = hot_s[j * slots:(j + 1) * slots, pl.ds(pl.multiple_of(first + s * rows, rows), rows)]
            got = lax.dot_general(hot, out_s[j * room:j * room + slots, :], (((0,), (0,)), ((), ())), preferred_element_type=F32)
            dst[s] = got.astype(BF16)

    for j in range(GROUP):
        for k in range(2):
            restore(j, k, outs[k * GROUP + j])
    for cp in pushes:
        cp.wait()


def solution(mesh):
    act_spec = P(None, "dp", None)
    state_spec = P("dp", "tp", None)
    in_specs = (act_spec, state_spec, state_spec, act_spec, P(None), P(None, None, "tp"), P("tp", None), P("tp"), P("tp", None), P(None), P(None), P(None), P(None, "tp"), P("tp"), P("tp", None), P("tp"), P("tp", None), P(None), P(None, None), P(None, None, "tp"), P(None, None, "tp"), P(None, "tp", None))
    out_specs = (act_spec, state_spec, state_spec)
    across = [(0, 2), (2, 0), (1, 3), (3, 1)]
    beside = [(0, 1), (1, 0), (2, 3), (3, 2)]

    def layer_steps(x_steps, conv_state, ssm_state, expert_ids, g_in, w_in, conv_w, conv_b, w_xp, g_dt, g_b, g_c, w_dt, b_dt, a_log, d_skip, w_out, g_ff, w_router, w_gate, w_up, w_down):
        steps, batch, d_model = x_steps.shape
        inner = w_in.shape[2]
        rank = w_dt.shape[0]
        state = a_log.shape[1]
        experts, _, ffn = w_gate.shape
        width = rank + 2 * state
        half = steps // 2
        rows = batch // CHUNKS
        tokens = steps * rows
        slots = tokens + experts * ROW_ALIGN
        core = lax.rem(lax.axis_index("tp"), 2)

        conv_t = jnp.transpose(conv_state, (2, 0, 1))
        h_rows = jnp.transpose(ssm_state, (0, 2, 1)).reshape(batch * state, inner)
        alog_t = a_log.T

        ids = jnp.transpose(expert_ids, (0, 2, 1))
        pos, table = pl.pallas_call(
            routes_kernel,
            out_shape=(jax.ShapeDtypeStruct((CHUNKS, 1, tokens), jnp.int32), jax.ShapeDtypeStruct((CHUNKS // GROUP, 16 * GROUP + 8, 128), jnp.int32)),
            compiler_params=params(),
            name="routes",
        )(ids)

        vmem = pl.BlockSpec(memory_space=pltpu.VMEM)
        piece = (half, rows, d_model)
        u_first, u_second, *chips, conv_mid, h_mid = pl.pallas_call(
            mamba_kernel,
            in_specs=[HBM, HBM, HBM] + [vmem] * 13,
            out_specs=[HBM] * 6,
            out_shape=[
                jax.ShapeDtypeStruct((WHOLE,) + piece, BF16),
                jax.ShapeDtypeStruct((WHOLE,) + piece, BF16),
                jax.ShapeDtypeStruct(piece, BF16),
                jax.ShapeDtypeStruct(piece, BF16),
                jax.ShapeDtypeStruct((3, batch, inner), BF16),
                jax.ShapeDtypeStruct((batch * state, inner), F32),
            ],
            scratch_shapes=[
                pltpu.VMEM((steps, batch, d_model), BF16),
                pltpu.VMEM((3, batch, inner), BF16),
                pltpu.VMEM((3, batch, inner), BF16),
                pltpu.VMEM((inner // 128, batch * state, 128), F32),
                pltpu.VMEM((steps, batch, inner), BF16),
                pltpu.VMEM((steps, batch, inner), BF16),
                pltpu.VMEM((7, CHUNKS, rows, 2 * width), F32),
                pltpu.VMEM((5, CHUNKS) + piece, BF16),
                pltpu.VMEM((2, CHUNKS) + piece, BF16),
                pltpu.VMEM((d_model, 2 * inner), BF16),
                pltpu.VMEM((1, steps * width), F32),
                pltpu.VMEM((steps * width, steps * inner), BF16),
                pltpu.VMEM((steps * width, steps * width), BF16),
                pltpu.VMEM((steps, 2 * state, 8, 128), F32),
                pltpu.VMEM((steps, 2 * state, 8, 128), F32),
                pltpu.VMEM((state, inner), F32),
                pltpu.VMEM((steps, 128, 128), F32),
                pltpu.VMEM((steps, 128, inner), F32),
                pltpu.VMEM((steps, 128, inner), F32),
                pltpu.VMEM((steps, 128, inner), F32),
                pltpu.SemaphoreType.DMA((2, CHUNKS)),
                pltpu.SemaphoreType.DMA((inner // 128, CHUNKS)),
                pltpu.SemaphoreType.DMA((3, CHUNKS)),
                pltpu.SemaphoreType.DMA((inner // 128, CHUNKS)),
                pltpu.SemaphoreType.DMA((3, CHUNKS)),
                pltpu.SemaphoreType.DMA((3, CHUNKS)),
                pltpu.SemaphoreType.DMA((3, CHUNKS)),
                pltpu.SemaphoreType.DMA((3, CHUNKS)),
            ],
            compiler_params=params(collective_id=0, has_side_effects=True),
            cost_estimate=pl.CostEstimate(flops=int(8e9), bytes_accessed=int(45e6), transcendentals=0),
            name="mamba",
        )(x_steps, conv_t, h_rows, g_in, w_in, conv_w.T, conv_b, w_xp.T, g_dt, g_b, g_c, w_dt, b_dt, alog_t, d_skip, w_out)

        calls = CHUNKS // GROUP
        room = slots + 2 * TILE

        def run_moe(g, u_args, u_specs, states):
            extra = [] if states is None else list(states)
            return pl.pallas_call(
                functools.partial(moe_kernel, g),
                grid=(1,),
                in_specs=[pl.BlockSpec((1, 16 * GROUP + 8, 128), lambda i: (g, 0, 0), memory_space=pltpu.SMEM), pl.BlockSpec((GROUP, 1, tokens), lambda i: (g, 0, 0))] + u_specs + [vmem, vmem] + [HBM] * (5 + len(extra)),
                out_specs=[vmem] * (2 * GROUP) + [HBM, HBM] + ([] if extra else [HBM]),
                out_shape=[jax.ShapeDtypeStruct(piece, BF16)] * (2 * GROUP) + [jax.ShapeDtypeStruct(h_mid.shape, F32), jax.ShapeDtypeStruct(conv_mid.shape, BF16)] + ([] if extra else [jax.ShapeDtypeStruct(x_steps.shape, BF16)]),
                scratch_shapes=[
                    pltpu.VMEM((RING, d_model, ffn), BF16),
                    pltpu.VMEM((RING, d_model, ffn), BF16),
                    pltpu.VMEM((RING, ffn, d_model), BF16),
                    pltpu.SemaphoreType.DMA((3, RING)),
                    pltpu.VMEM((GROUP * tokens, d_model), BF16),
                    pltpu.VMEM((GROUP * slots, tokens), BF16),
                    pltpu.VMEM((GROUP * room, d_model), BF16),
                    pltpu.VMEM((GROUP * room, d_model), BF16),
                    pltpu.VMEM((GROUP * room, experts), F32),
                    pltpu.VMEM((batch * state // calls, inner), F32),
                    pltpu.VMEM((3, batch // calls, inner), BF16),
                    pltpu.SemaphoreType.DMA((4,)),
                ],
                input_output_aliases={9 + 2 * GROUP: 2 * GROUP, 10 + 2 * GROUP: 2 * GROUP + 1} if extra else {},
                compiler_params=params(),
                cost_estimate=pl.CostEstimate(flops=int(6e9), bytes_accessed=int(40e6), transcendentals=0),
            )(table, pos, *u_args, g_ff, w_router.T, w_gate, w_up, w_down, h_mid, conv_mid, *extra)

        def both(keep, send, dtype):
            got = lax.ppermute(send, "tp", beside)
            chip = (keep.astype(F32) + got.astype(F32)).astype(dtype)
            return chip, lax.ppermute(chip, "tp", across)

        owns = {}
        spot = {}
        for c in range(WHOLE):
            spot[c] = (u_first, u_second, pl.BlockSpec((1,) + piece, lambda i, c=c: (c, 0, 0, 0)))
            owns[c] = lambda c=c: u_first[c]
        for c in range(WHOLE, CHUNKS):
            chip = chips[c - WHOLE]
            far = lax.ppermute(chip, "tp", across)
            x_own = lax.dynamic_slice(x_steps, (half * core, c * rows, 0), (half, rows, d_model))
            u_own = (x_own.astype(F32) + (chip.astype(F32) + far.astype(F32))).astype(BF16)
            u_sib = lax.ppermute(u_own, "tp", beside)
            spot[c] = (u_own[None], u_sib[None], pl.BlockSpec((1,) + piece, lambda i: (0, 0, 0, 0)))
            owns[c] = lambda u_own=u_own: u_own

        states = None
        for g in range(calls):
            group = [spot[g * GROUP + j] for j in range(GROUP)]
            got = run_moe(g, [v[0] for v in group] + [v[1] for v in group], [v[2] for v in group] * 2, states)
            states = got[2 * GROUP:2 * GROUP + 2]
            if g == 0:
                y_steps = got[-1]
            for j in range(GROUP):
                c = g * GROUP + j
                chip, far = both(got[j], got[GROUP + j], BF16)
                y_own = (owns[c]().astype(F32) + (chip.astype(F32) + far.astype(F32))).astype(BF16)
                y_sib = lax.ppermute(y_own, "tp", beside)
                y_steps = lax.dynamic_update_slice(y_steps, y_own, (half * core, c * rows, 0))
                y_steps = lax.dynamic_update_slice(y_steps, y_sib, (half * (1 - core), c * rows, 0))
        ssm_out, conv_out = states
        ssm_fin = jnp.transpose(ssm_out.reshape(batch, state, inner), (0, 2, 1))
        return y_steps, jnp.transpose(conv_out, (1, 2, 0)), ssm_fin

    return jax.shard_map(layer_steps, mesh=mesh, in_specs=in_specs, out_specs=out_specs, check_vma=False)
```

```python
import functools

import jax
import jax.numpy as jnp
from jax import lax
from jax.experimental import pallas as pl
from jax.experimental.pallas import tpu as pltpu
from jax.sharding import PartitionSpec as P


EPSILON = 1e-6
CHUNKS = 4
ROW_ALIGN = 16
TILE = 128
GROUPS = ((0, 1), (2,), (3,))
LISTED = 32
ACTIVE = 33
RING = 6
WHOLE = 2
F32 = jnp.float32
BF16 = jnp.bfloat16
HBM = pl.BlockSpec(memory_space=pl.ANY)


def params(**kw):
    return pltpu.CompilerParams(vmem_limit_bytes=56 * 1024 * 1024, **kw)


def row(ref):
    return ref[...].astype(F32).reshape(1, -1)


def norm_rows(v, gain):
    return v * lax.rsqrt(jnp.mean(v * v, axis=-1, keepdims=True) + EPSILON) * gain


def mm_t(a, b):
    return lax.dot_general(a, b, (((1,), (1,)), ((), ())), preferred_element_type=F32)


def silu(v):
    return v * jax.nn.sigmoid(v)


def routes_kernel(ids_ref, pos_ref, tab_ref):
    _, _, tokens = pos_ref.shape
    steps = ids_ref.shape[0]
    rows = tokens // steps
    experts = 16
    upper = (lax.broadcasted_iota(jnp.int32, (tokens, tokens), 0) <= lax.broadcasted_iota(jnp.int32, (tokens, tokens), 1)).astype(F32).astype(BF16)
    before = (lax.broadcasted_iota(jnp.int32, (experts, experts), 1) < lax.broadcasted_iota(jnp.int32, (experts, experts), 0)).astype(F32).astype(BF16)
    lane = lax.broadcasted_iota(jnp.int32, (experts, 128), 1)
    number = lax.broadcasted_iota(jnp.int32, (experts, 128), 0).astype(F32)
    for g, k, c in [(g, k, c) for g, group in enumerate(GROUPS) for k, c in enumerate(group)]:
        ids = jnp.concatenate([ids_ref[s, :, c * rows:(c + 1) * rows] for s in range(steps)], axis=1)
        hit = lax.broadcasted_iota(jnp.int32, (experts, tokens), 0) == ids
        hot = hit.astype(F32)
        rank = jnp.dot(hot.astype(BF16), upper, preferred_element_type=F32)
        count = jnp.broadcast_to(jnp.sum(hot, axis=1, keepdims=True), (experts, 128))
        blocks = jnp.floor((count + (ROW_ALIGN - 1)) * (1.0 / ROW_ALIGN))
        start = ROW_ALIGN * jnp.dot(before, blocks.astype(BF16), preferred_element_type=F32)
        pos_ref[c] = jnp.sum(hot * (start[:, :1] + rank - 1.0), axis=0, keepdims=True).astype(jnp.int32)
        tab_ref[g, 16 * k:16 * k + 16, :] = jnp.where(lane == 0, start, count).astype(jnp.int32)
        total = count if k == 0 else total + count
        if c == GROUPS[g][-1]:
            active = (total > 0.0).astype(F32)
            place = jnp.dot(before, active.astype(BF16), preferred_element_type=F32)
            listed = jnp.sum(jnp.where((place == lane.astype(F32)) & (active > 0.0), number, 0.0), axis=0, keepdims=True)
            tab_ref[g, LISTED:LISTED + 1, :] = listed.astype(jnp.int32)
            tab_ref[g, ACTIVE:ACTIVE + 1, :] = jnp.sum(active, axis=0, keepdims=True).astype(jnp.int32)


LOG2E = 1.4426950408889634


def mamba_kernel(x_hbm, cs_hbm, h_hbm, g_ref, win3_ref, cw_ref, cb_ref, wxp_ref, gdt_ref, gb_ref, gc_ref, wdt_ref, bdt_ref, alog_ref, dskip_ref, wout_ref,
                 uo_hbm, us_hbm, chip2_hbm, chip3_hbm, co_hbm, ho_hbm,
                 x_s, cs_s, co_s, h_s, xc_s, z_s, p_s, m_s, u_s, win_ref, g4_ref, wdt4, ones_s, even_s, odd_s, a_s, q_s, delta_s, dx_s, y_s,
                 in_sem, h_sem, out_sem, ho_sem, psend, precv, msend, mrecv):
    steps, batch, _ = x_s.shape
    inner = cs_s.shape[2]
    state = alog_ref.shape[0]
    rank = wdt_ref.shape[0]
    width = rank + 2 * state
    lanes = steps * width
    half = steps // 2
    rows = batch // CHUNKS
    tiles = inner // 128
    me = lax.axis_index("tp")
    core = lax.rem(me, 2)
    sibling = me + 1 - 2 * core
    partner = lax.rem(me + 2, 4)

    barrier = pltpu.get_barrier_semaphore()
    for peer in (sibling, partner):
        pl.semaphore_signal(barrier, inc=1, device_id={"tp": peer}, device_id_type=pl.DeviceIdType.MESH)

    def span(c):
        return pl.ds(c * rows, rows)

    def loads(c):
        return [
            pltpu.make_async_copy(x_hbm.at[:, span(c), :], x_s.at[:, span(c), :], in_sem.at[0, c]),
            pltpu.make_async_copy(cs_hbm.at[:, span(c), :], cs_s.at[:, span(c), :], in_sem.at[1, c]),
        ]

    def state_rows(c):
        return pl.ds(c * rows * state, rows * state)

    def h_loads(c):
        return [pltpu.make_async_copy(h_hbm.at[state_rows(c), pl.ds(l * 128, 128)], h_s.at[l, state_rows(c), :], h_sem.at[l, c]) for l in range(tiles)]

    def h_stores(c):
        return [pltpu.make_async_copy(h_s.at[l, state_rows(c), :], ho_hbm.at[state_rows(c), pl.ds(l * 128, 128)], ho_sem.at[l, c]) for l in range(tiles)]

    def co_store(c):
        return pltpu.make_async_copy(co_s.at[:, span(c), :], co_hbm.at[:, span(c), :], out_sem.at[0, c])

    def remote(buf, c, src, dst, send, recv, stage, peer):
        return pltpu.make_async_remote_copy(
            src_ref=buf.at[src, c], dst_ref=buf.at[dst, c], send_sem=send.at[stage, c], recv_sem=recv.at[stage, c],
            device_id={"tp": peer}, device_id_type=pl.DeviceIdType.MESH)

    def p_beside(c):
        return remote(p_s, c, 1, 2, psend, precv, 0, sibling)

    def p_across(c):
        return remote(p_s, c, 3, 4, psend, precv, 1, partner)

    def p_back(c):
        return remote(p_s, c, 5, 6, psend, precv, 2, sibling)

    def m_beside(c):
        return remote(m_s, c, 1, 2, msend, mrecv, 0, sibling)

    def m_across(c):
        return remote(m_s, c, 3, 4, msend, mrecv, 1, partner)

    def u_back(c):
        return pltpu.make_async_remote_copy(
            src_ref=u_s.at[0, c], dst_ref=u_s.at[1, c], send_sem=msend.at[2, c], recv_sem=mrecv.at[2, c],
            device_id={"tp": sibling}, device_id_type=pl.DeviceIdType.MESH)

    for c in range(CHUNKS):
        for cp in loads(c):
            cp.start()
    for c in range(CHUNKS):
        for cp in h_loads(c):
            cp.start()

    gain = row(g_ref)
    for k in range(2):
        win_ref[:, k * inner:(k + 1) * inner] = win3_ref[:, k, :]

    def project(c):
        for cp in loads(c):
            cp.wait()

        def block(i, carry):
            r = pl.multiple_of(c * rows + i * 128, 128)
            seq = [cs_s[j, pl.ds(r, 128), :].astype(F32) for j in range(3)]
            part = []
            for s in range(steps):
                x = x_s[s, pl.ds(r, 128), :].astype(F32)
                n = norm_rows(x, gain).astype(BF16)
                xz = jnp.dot(n, win_ref[...], preferred_element_type=F32).astype(BF16)
                z_s[s, pl.ds(r, 128), :] = xz[:, inner:]
                xi = xz[:, :inner]
                if s > 0:
                    co_s[s - 1, pl.ds(r, 128), :] = xi
                seq.append(xi.astype(F32))
                acc = seq[s] * cw_ref[0:1, :].astype(F32)
                for j in range(1, 4):
                    acc = acc + seq[s + j] * cw_ref[j:j + 1, :].astype(F32)
                xc = silu(acc + row(cb_ref)).astype(BF16)
                xc_s[s, pl.ds(r, 128), :] = xc
                part.append(mm_t(xc, wxp_ref[...]))
            low = jnp.concatenate(part[:2], axis=1)
            high = jnp.concatenate(part[2:], axis=1)
            q = pl.multiple_of(i * 128, 128)
            p_s[0, c, pl.ds(q, 128), :] = jnp.where(core == 0, low, high)
            p_s[1, c, pl.ds(q, 128), :] = jnp.where(core == 0, high, low)
            return carry

        lax.fori_loop(0, rows // 128, block, 0)
        co_store(c).start()

    def p_sum(c):
        p_beside(c).wait_recv()
        p_s[3, c] = p_s[0, c] + p_s[2, c]
        p_across(c).start()

    def p_whole(c):
        p_across(c).wait_recv()
        p_s[5, c] = p_s[3, c] + p_s[4, c]
        p_back(c).start()

    def scan(c):
        p_back(c).wait_recv()
        for cp in h_loads(c):
            cp.wait()

        def block(i, carry):
            r = pl.multiple_of(i * 128, 128)
            g = pl.multiple_of(c * rows + i * 128, 128)
            own, sib = p_s[5, c, pl.ds(r, 128), :], p_s[6, c, pl.ds(r, 128), :]
            p = jnp.concatenate([jnp.where(core == 0, own, sib), jnp.where(core == 0, sib, own)], axis=1)
            sq = p * p
            s1 = sq.astype(BF16)
            rest = sq - s1.astype(F32)
            s2 = rest.astype(BF16)
            s3 = (rest - s2.astype(F32)).astype(BF16)
            mean = sum(jnp.dot(v, ones_s[...], preferred_element_type=F32) for v in (s3, s2, s1))
            norm = p * lax.rsqrt(mean + EPSILON) * g4_ref[...]
            for s in range(steps):
                first = s * width + rank
                q_s[s] = jnp.concatenate([norm[:, first:first + 2 * state], jnp.zeros((128, 128 - 2 * state), F32)], axis=1)
            pre = jnp.dot(norm.astype(BF16), wdt4[...], preferred_element_type=F32)
            bias = row(bdt_ref)
            for s in range(steps):
                v = pre[:, s * inner:(s + 1) * inner] + bias
                delta = jnp.maximum(v, 0.0) + jnp.log1p(jnp.exp(-jnp.abs(v)))
                delta_s[s] = delta
                dx_s[s] = delta * xc_s[s, pl.ds(g, 128), :].astype(F32)

            def spread(t, wide):
                b = pl.multiple_of(t * 8, 8)
                qs = [q_s[s, pl.ds(b, 8), :] for s in range(steps)]
                for n in range(2 * state):
                    for s in range(steps):
                        wide[s, n] = jnp.broadcast_to(qs[s][:, n:n + 1], (8, 128))

            def advance(t, wide):
                b = pl.multiple_of(t * 8, 8)
                base = (g + b) * state
                cut = [slice(l * 128, (l + 1) * 128) for l in range(tiles)]
                dl = [[delta_s[s, pl.ds(b, 8), k] for k in cut] for s in range(steps)]
                dx = [[dx_s[s, pl.ds(b, 8), k] for k in cut] for s in range(steps)]
                ys = [[None] * tiles for _ in range(steps)]
                for n in range(state):
                    for l in range(tiles):
                        a = a_s[n:n + 1, cut[l]]
                        spot = (l, pl.ds(base + n, 8, stride=state))
                        h = h_s[spot]
                        for s in range(steps):
                            h = jnp.exp2(dl[s][l] * a) * h + dx[s][l] * wide[s, n]
                            hc = h * wide[s, n + state]
                            ys[s][l] = hc if n == 0 else ys[s][l] + hc
                        h_s[spot] = h
                for s in range(steps):
                    for l in range(tiles):
                        y_s[s, pl.ds(b, 8), cut[l]] = ys[s][l]

            def pair(i, carry2):
                t = 2 * i
                spread(t + 1, odd_s)
                advance(t, even_s)
                spread(jnp.minimum(t + 2, 14), even_s)
                advance(t + 1, odd_s)
                return carry2

            spread(0, even_s)
            lax.fori_loop(0, 8, pair, 0)
            for s in range(steps):
                xc = xc_s[s, pl.ds(g, 128), :].astype(F32)
                yg = ((y_s[s] + row(dskip_ref) * xc) * silu(z_s[s, pl.ds(g, 128), :].astype(F32))).astype(BF16)
                out = jnp.dot(yg, wout_ref[...], preferred_element_type=F32).astype(BF16)
                m_s[lax.rem(core + s // half, 2), c, s % half, pl.ds(r, 128), :] = out
            return carry

        lax.fori_loop(0, rows // 128, block, 0)
        for cp in h_stores(c):
            cp.start()
        m_beside(c).start()

    def chip_out(c):
        return pltpu.make_async_copy(m_s.at[3, c], (chip2_hbm, chip3_hbm)[c - WHOLE], out_sem.at[1, c])

    def m_sum(c):
        m_beside(c).wait_recv()
        for s in range(half):
            m_s[3, c, s] = (m_s[0, c, s].astype(F32) + m_s[2, c, s].astype(F32)).astype(BF16)
        if c < WHOLE:
            m_across(c).start()
        else:
            chip_out(c).start()

    def uo_out(c):
        return pltpu.make_async_copy(u_s.at[0, c], uo_hbm.at[c], out_sem.at[1, c])

    def us_out(c):
        return pltpu.make_async_copy(u_s.at[1, c], us_hbm.at[c], out_sem.at[2, c])

    def m_whole(c):
        m_across(c).wait_recv()
        for s in range(half):
            x = x_s[core * half + s, span(c), :].astype(F32)
            u_s[0, c, s] = (x + (m_s[3, c, s].astype(F32) + m_s[4, c, s].astype(F32))).astype(BF16)
        u_back(c).start()
        uo_out(c).start()

    project(0)
    pl.semaphore_wait(barrier, 2)
    p_beside(0).start()
    project(1)
    p_beside(1).start()
    p_sum(0)
    project(2)
    p_beside(2).start()
    p_sum(1)
    project(3)
    p_beside(3).start()
    p_sum(2)
    p_whole(0)

    wdt4[...] = jnp.zeros_like(wdt4)
    for s in range(steps):
        wdt4[s * width:s * width + rank, s * inner:(s + 1) * inner] = wdt_ref[...]

    def group(v):
        step, col = v // width, lax.rem(v, width)
        return step * 4 + (col >= rank).astype(jnp.int32) + (col >= rank + state).astype(jnp.int32)

    gi = group(lax.broadcasted_iota(jnp.int32, (lanes, lanes), 0))
    gj = group(lax.broadcasted_iota(jnp.int32, (lanes, lanes), 1))
    inv = jnp.where(lax.rem(gj, 4) == 0, 1.0 / rank, 1.0 / state)
    ones_s[...] = jnp.where(gi == gj, inv, 0.0).astype(BF16)
    for s in range(steps):
        for ref, at in ((gdt_ref, 0), (gb_ref, rank), (gc_ref, rank + state)):
            g4_ref[:, s * width + at:s * width + at + ref.shape[0]] = row(ref)
    a_s[...] = -LOG2E * jnp.exp(alog_ref[...])

    p_sum(3)
    p_whole(1)
    scan(0)
    p_whole(2)
    p_whole(3)
    m_sum(0)
    scan(1)
    m_sum(1)
    scan(2)
    m_sum(2)
    m_whole(0)
    scan(3)
    m_sum(3)
    for c in range(1, WHOLE):
        m_whole(c)
    for c in range(WHOLE):
        u_back(c).wait_recv()
        us_out(c).start()
    for c in range(CHUNKS):
        p_beside(c).wait_send()
        p_across(c).wait_send()
        p_back(c).wait_send()
        m_beside(c).wait_send()
        co_store(c).wait()
        for cp in h_stores(c):
            cp.wait()
        if c < WHOLE:
            m_across(c).wait_send()
            u_back(c).wait_send()
            uo_out(c).wait()
            us_out(c).wait()
        else:
            chip_out(c).wait()


def moe_kernel(g, size, *refs):
    count_in = 2 + 2 * size
    tab_ref, pos_ref = refs[:2]
    us = refs[2:count_in]
    gff_ref, wr_ref, wg_ref, wu_ref, wd_ref, h_hbm, cv_hbm = refs[count_in:count_in + 7]
    refs = refs[count_in + (9 if g else 7):]
    outs = refs[:2 * size]
    ho_hbm, co_hbm = refs[2 * size:count_in]
    wg, wu, wd, sems, m_s, hot_s, in_s, out_s, prob_s, h_s, cv_s, st_sem = refs[-12:]
    _, half, rows, d_model = us[0].shape
    experts = wr_ref.shape[0]
    tokens = 2 * half * rows
    slots = hot_s.shape[0] // size
    room = in_s.shape[0] // size
    core = lax.rem(lax.axis_index("tp"), 2)
    active = tab_ref[0, ACTIVE, 0]

    def copies(i):
        e = tab_ref[0, LISTED, i]
        slot = lax.rem(i, RING)
        return [pltpu.make_async_copy(src.at[e], dst.at[slot], sems.at[k, slot]) for k, (src, dst) in enumerate(((wg_ref, wg), (wu_ref, wu), (wd_ref, wd)))]

    def fetch(i):
        @pl.when(i < active)
        def _():
            for cp in copies(i):
                cp.start()

    for i in range(RING - 1):
        fetch(i)
    h_span = pl.ds(GROUPS[g][0] * h_s.shape[0] // size, h_s.shape[0])
    cv_span = pl.ds(GROUPS[g][0] * cv_s.shape[1] // size, cv_s.shape[1])
    pulls = [pltpu.make_async_copy(h_hbm.at[h_span, :], h_s, st_sem.at[0]), pltpu.make_async_copy(cv_hbm.at[:, cv_span, :], cv_s, st_sem.at[1])]
    pushes = [pltpu.make_async_copy(h_s, ho_hbm.at[h_span, :], st_sem.at[2]), pltpu.make_async_copy(cv_s, co_hbm.at[:, cv_span, :], st_sem.at[3])]
    for cp in pulls:
        cp.start()
    gain = row(gff_ref)
    for j in range(size):
        for k in range(2):
            src = us[k * size + j]
            first = j * tokens + jnp.where(core == k, 0, half * rows)
            for s in range(half):
                u = src[0, s].astype(F32)
                m = norm_rows(u, gain)
                m_s[pl.ds(pl.multiple_of(first + s * rows, rows), rows), :] = m.astype(BF16)

    down = lax.broadcasted_iota(jnp.int32, (256, tokens), 0).astype(F32).astype(BF16)
    for j in range(size):
        pos = pos_ref[j]

        def order(i, carry):
            r = pl.multiple_of(i * 256, 256)
            local = jnp.where((pos >= r) & (pos < r + 256), pos - r, -1).astype(F32).astype(BF16)
            hot = jnp.where(down == local, jnp.ones((), BF16), jnp.zeros((), BF16))
            hot_s[pl.ds(j * slots + r, 256), :] = hot
            m = jnp.dot(hot, m_s[j * tokens:(j + 1) * tokens, :], preferred_element_type=F32).astype(BF16)
            at = pl.ds(j * room + r, 256)
            in_s[at, :] = m
            out_s[at, :] = jnp.zeros((256, d_model), BF16)
            logits = mm_t(m, wr_ref[...])
            ex = jnp.exp(logits - jnp.max(logits, axis=-1, keepdims=True))
            prob_s[at, :] = ex / jnp.sum(ex, axis=-1, keepdims=True)
            return carry

        lax.fori_loop(0, slots // 256, order, 0)
    for pull, push in zip(pulls, pushes):
        pull.wait()
        push.start()

    def feed(e, slot, r, size):
        m = in_s[pl.ds(r, size), :]
        gate = jnp.dot(m, wg[slot], preferred_element_type=F32)
        up = jnp.dot(m, wu[slot], preferred_element_type=F32)
        q = (silu(gate) * up).astype(BF16)
        lane = lax.broadcasted_iota(jnp.int32, (size, experts), 1)
        prob = jnp.sum(jnp.where(lane == e, prob_s[pl.ds(r, size), :], 0.0), axis=-1, keepdims=True)
        out_s[pl.ds(r, size), :] = (prob * jnp.dot(q, wd[slot], preferred_element_type=F32)).astype(BF16)

    def expert(i, carry):
        e = tab_ref[0, LISTED, i]
        slot = lax.rem(i, RING)
        fetch(i + RING - 1)
        for cp in copies(i):
            cp.wait()

        def part(j, c1):
            start = tab_ref[0, 16 * j + e, 0] + j * room
            count = tab_ref[0, 16 * j + e, 1]
            big = (count + TILE - 1) // (2 * TILE)

            def tile(k, c2):
                feed(e, slot, pl.multiple_of(start + k * (2 * TILE), ROW_ALIGN), 2 * TILE)
                return c2

            lax.fori_loop(0, big, tile, 0)

            @pl.when(count > big * (2 * TILE))
            def _():
                feed(e, slot, pl.multiple_of(start + big * (2 * TILE), ROW_ALIGN), TILE)

            return c1

        return lax.fori_loop(0, size, part, carry)

    lax.fori_loop(0, active, expert, 0)

    def restore(j, k, dst):
        first = jnp.where(core == k, 0, half * rows)
        for s in range(half):
            hot = hot_s[j * slots:(j + 1) * slots, pl.ds(pl.multiple_of(first + s * rows, rows), rows)]
            got = lax.dot_general(hot, out_s[j * room:j * room + slots, :], (((0,), (0,)), ((), ())), preferred_element_type=F32)
            dst[s] = got.astype(BF16)

    for j in range(size):
        for k in range(2):
            restore(j, k, outs[k * size + j])
    for cp in pushes:
        cp.wait()


def solution(mesh):
    act_spec = P(None, "dp", None)
    state_spec = P("dp", "tp", None)
    in_specs = (act_spec, state_spec, state_spec, act_spec, P(None), P(None, None, "tp"), P("tp", None), P("tp"), P("tp", None), P(None), P(None), P(None), P(None, "tp"), P("tp"), P("tp", None), P("tp"), P("tp", None), P(None), P(None, None), P(None, None, "tp"), P(None, None, "tp"), P(None, "tp", None))
    out_specs = (act_spec, state_spec, state_spec)
    across = [(0, 2), (2, 0), (1, 3), (3, 1)]
    beside = [(0, 1), (1, 0), (2, 3), (3, 2)]

    def layer_steps(x_steps, conv_state, ssm_state, expert_ids, g_in, w_in, conv_w, conv_b, w_xp, g_dt, g_b, g_c, w_dt, b_dt, a_log, d_skip, w_out, g_ff, w_router, w_gate, w_up, w_down):
        steps, batch, d_model = x_steps.shape
        inner = w_in.shape[2]
        rank = w_dt.shape[0]
        state = a_log.shape[1]
        experts, _, ffn = w_gate.shape
        width = rank + 2 * state
        half = steps // 2
        rows = batch // CHUNKS
        tokens = steps * rows
        slots = tokens + experts * ROW_ALIGN
        core = lax.rem(lax.axis_index("tp"), 2)

        conv_t = jnp.transpose(conv_state, (2, 0, 1))
        h_rows = jnp.transpose(ssm_state, (0, 2, 1)).reshape(batch * state, inner)
        alog_t = a_log.T

        ids = jnp.transpose(expert_ids, (0, 2, 1))
        pos, table = pl.pallas_call(
            routes_kernel,
            out_shape=(jax.ShapeDtypeStruct((CHUNKS, 1, tokens), jnp.int32), jax.ShapeDtypeStruct((len(GROUPS), ACTIVE + 7, 128), jnp.int32)),
            compiler_params=params(),
            name="routes",
        )(ids)

        vmem = pl.BlockSpec(memory_space=pltpu.VMEM)
        piece = (half, rows, d_model)
        u_first, u_second, *chips, conv_mid, h_mid = pl.pallas_call(
            mamba_kernel,
            in_specs=[HBM, HBM, HBM] + [vmem] * 13,
            out_specs=[HBM] * 6,
            out_shape=[
                jax.ShapeDtypeStruct((WHOLE,) + piece, BF16),
                jax.ShapeDtypeStruct((WHOLE,) + piece, BF16),
                jax.ShapeDtypeStruct(piece, BF16),
                jax.ShapeDtypeStruct(piece, BF16),
                jax.ShapeDtypeStruct((3, batch, inner), BF16),
                jax.ShapeDtypeStruct((batch * state, inner), F32),
            ],
            scratch_shapes=[
                pltpu.VMEM((steps, batch, d_model), BF16),
                pltpu.VMEM((3, batch, inner), BF16),
                pltpu.VMEM((3, batch, inner), BF16),
                pltpu.VMEM((inner // 128, batch * state, 128), F32),
                pltpu.VMEM((steps, batch, inner), BF16),
                pltpu.VMEM((steps, batch, inner), BF16),
                pltpu.VMEM((7, CHUNKS, rows, 2 * width), F32),
                pltpu.VMEM((5, CHUNKS) + piece, BF16),
                pltpu.VMEM((2, CHUNKS) + piece, BF16),
                pltpu.VMEM((d_model, 2 * inner), BF16),
                pltpu.VMEM((1, steps * width), F32),
                pltpu.VMEM((steps * width, steps * inner), BF16),
                pltpu.VMEM((steps * width, steps * width), BF16),
                pltpu.VMEM((steps, 2 * state, 8, 128), F32),
                pltpu.VMEM((steps, 2 * state, 8, 128), F32),
                pltpu.VMEM((state, inner), F32),
                pltpu.VMEM((steps, 128, 128), F32),
                pltpu.VMEM((steps, 128, inner), F32),
                pltpu.VMEM((steps, 128, inner), F32),
                pltpu.VMEM((steps, 128, inner), F32),
                pltpu.SemaphoreType.DMA((2, CHUNKS)),
                pltpu.SemaphoreType.DMA((inner // 128, CHUNKS)),
                pltpu.SemaphoreType.DMA((3, CHUNKS)),
                pltpu.SemaphoreType.DMA((inner // 128, CHUNKS)),
                pltpu.SemaphoreType.DMA((3, CHUNKS)),
                pltpu.SemaphoreType.DMA((3, CHUNKS)),
                pltpu.SemaphoreType.DMA((3, CHUNKS)),
                pltpu.SemaphoreType.DMA((3, CHUNKS)),
            ],
            compiler_params=params(collective_id=0, has_side_effects=True),
            cost_estimate=pl.CostEstimate(flops=int(8e9), bytes_accessed=int(45e6), transcendentals=0),
            name="mamba",
        )(x_steps, conv_t, h_rows, g_in, w_in, conv_w.T, conv_b, w_xp.T, g_dt, g_b, g_c, w_dt, b_dt, alog_t, d_skip, w_out)

        room = slots + 2 * TILE

        def run_moe(g, u_args, u_specs, states):
            extra = [] if states is None else list(states)
            size = len(GROUPS[g])
            first = GROUPS[g][0] // size
            count_in = 2 + 2 * size
            return pl.pallas_call(
                functools.partial(moe_kernel, g, size),
                grid=(1,),
                in_specs=[pl.BlockSpec((1, ACTIVE + 7, 128), lambda i: (g, 0, 0), memory_space=pltpu.SMEM), pl.BlockSpec((size, 1, tokens), lambda i: (first, 0, 0))] + u_specs + [vmem, vmem] + [HBM] * (5 + len(extra)),
                out_specs=[vmem] * (2 * size) + [HBM, HBM] + ([] if extra else [HBM]),
                out_shape=[jax.ShapeDtypeStruct(piece, BF16)] * (2 * size) + [jax.ShapeDtypeStruct(h_mid.shape, F32), jax.ShapeDtypeStruct(conv_mid.shape, BF16)] + ([] if extra else [jax.ShapeDtypeStruct(x_steps.shape, BF16)]),
                scratch_shapes=[
                    pltpu.VMEM((RING, d_model, ffn), BF16),
                    pltpu.VMEM((RING, d_model, ffn), BF16),
                    pltpu.VMEM((RING, ffn, d_model), BF16),
                    pltpu.SemaphoreType.DMA((3, RING)),
                    pltpu.VMEM((size * tokens, d_model), BF16),
                    pltpu.VMEM((size * slots, tokens), BF16),
                    pltpu.VMEM((size * room, d_model), BF16),
                    pltpu.VMEM((size * room, d_model), BF16),
                    pltpu.VMEM((size * room, experts), F32),
                    pltpu.VMEM((size * rows * state, inner), F32),
                    pltpu.VMEM((3, size * rows, inner), BF16),
                    pltpu.SemaphoreType.DMA((4,)),
                ],
                input_output_aliases={count_in + 7: 2 * size, count_in + 8: 2 * size + 1} if extra else {},
                compiler_params=params(),
                cost_estimate=pl.CostEstimate(flops=int(3e9) * size, bytes_accessed=int(40e6), transcendentals=0),
            )(table, pos, *u_args, g_ff, w_router.T, w_gate, w_up, w_down, h_mid, conv_mid, *extra)

        def both(keep, send, dtype):
            got = lax.ppermute(send, "tp", beside)
            chip = (keep.astype(F32) + got.astype(F32)).astype(dtype)
            return chip, lax.ppermute(chip, "tp", across)

        owns = {}
        spot = {}
        for c in range(WHOLE):
            spot[c] = (u_first, u_second, pl.BlockSpec((1,) + piece, lambda i, c=c: (c, 0, 0, 0)))
            owns[c] = lambda c=c: u_first[c]
        for c in range(WHOLE, CHUNKS):
            chip = chips[c - WHOLE]
            far = lax.ppermute(chip, "tp", across)
            x_own = lax.dynamic_slice(x_steps, (half * core, c * rows, 0), (half, rows, d_model))
            u_own = (x_own.astype(F32) + (chip.astype(F32) + far.astype(F32))).astype(BF16)
            u_sib = lax.ppermute(u_own, "tp", beside)
            spot[c] = (u_own[None], u_sib[None], pl.BlockSpec((1,) + piece, lambda i: (0, 0, 0, 0)))
            owns[c] = lambda u_own=u_own: u_own

        states = None
        for g, members in enumerate(GROUPS):
            size = len(members)
            group = [spot[c] for c in members]
            got = run_moe(g, [v[0] for v in group] + [v[1] for v in group], [v[2] for v in group] * 2, states)
            states = got[2 * size:2 * size + 2]
            if g == 0:
                y_steps = got[-1]
            for j, c in enumerate(members):
                chip, far = both(got[j], got[size + j], BF16)
                y_own = (owns[c]().astype(F32) + (chip.astype(F32) + far.astype(F32))).astype(BF16)
                y_sib = lax.ppermute(y_own, "tp", beside)
                y_steps = lax.dynamic_update_slice(y_steps, y_own, (half * core, c * rows, 0))
                y_steps = lax.dynamic_update_slice(y_steps, y_sib, (half * (1 - core), c * rows, 0))
        ssm_out, conv_out = states
        ssm_fin = jnp.transpose(ssm_out.reshape(batch, state, inner), (0, 2, 1))
        return y_steps, jnp.transpose(conv_out, (1, 2, 0)), ssm_fin

    return jax.shard_map(layer_steps, mesh=mesh, in_specs=in_specs, out_specs=out_specs, check_vma=False)
```

```python
import functools

import jax
import jax.numpy as jnp
from jax import lax
from jax.experimental import pallas as pl
from jax.experimental.pallas import tpu as pltpu
from jax.sharding import PartitionSpec as P


EPSILON = 1e-6
CHUNKS = 4
ROW_ALIGN = 16
TILE = 128
GROUPS = ((0, 1), (2,), (3,))
LAST = CHUNKS - 1
LISTED = 32
ACTIVE = 33
RING = 6
WHOLE = 2
F32 = jnp.float32
BF16 = jnp.bfloat16
HBM = pl.BlockSpec(memory_space=pl.ANY)


def params(**kw):
    return pltpu.CompilerParams(vmem_limit_bytes=56 * 1024 * 1024, **kw)


def row(ref):
    return ref[...].astype(F32).reshape(1, -1)


def norm_rows(v, gain):
    return v * lax.rsqrt(jnp.mean(v * v, axis=-1, keepdims=True) + EPSILON) * gain


def mm_t(a, b):
    return lax.dot_general(a, b, (((1,), (1,)), ((), ())), preferred_element_type=F32)


def silu(v):
    return v * jax.nn.sigmoid(v)


def routes_kernel(ids_ref, pos_ref, tab_ref):
    _, _, tokens = pos_ref.shape
    steps = ids_ref.shape[0]
    rows = tokens // steps
    experts = 16
    upper = (lax.broadcasted_iota(jnp.int32, (tokens, tokens), 0) <= lax.broadcasted_iota(jnp.int32, (tokens, tokens), 1)).astype(F32).astype(BF16)
    before = (lax.broadcasted_iota(jnp.int32, (experts, experts), 1) < lax.broadcasted_iota(jnp.int32, (experts, experts), 0)).astype(F32).astype(BF16)
    lane = lax.broadcasted_iota(jnp.int32, (experts, 128), 1)
    number = lax.broadcasted_iota(jnp.int32, (experts, 128), 0).astype(F32)
    for g, k, c in [(g, k, c) for g, group in enumerate(GROUPS) for k, c in enumerate(group)]:
        ids = jnp.concatenate([ids_ref[s, :, c * rows:(c + 1) * rows] for s in range(steps)], axis=1)
        hit = lax.broadcasted_iota(jnp.int32, (experts, tokens), 0) == ids
        hot = hit.astype(F32)
        rank = jnp.dot(hot.astype(BF16), upper, preferred_element_type=F32)
        count = jnp.broadcast_to(jnp.sum(hot, axis=1, keepdims=True), (experts, 128))
        blocks = jnp.floor((count + (ROW_ALIGN - 1)) * (1.0 / ROW_ALIGN))
        start = ROW_ALIGN * jnp.dot(before, blocks.astype(BF16), preferred_element_type=F32)
        pos_ref[c] = jnp.sum(hot * (start[:, :1] + rank - 1.0), axis=0, keepdims=True).astype(jnp.int32)
        tab_ref[g, 16 * k:16 * k + 16, :] = jnp.where(lane == 0, start, count).astype(jnp.int32)
        total = count if k == 0 else total + count
        if c == GROUPS[g][-1]:
            active = (total > 0.0).astype(F32)
            place = jnp.dot(before, active.astype(BF16), preferred_element_type=F32)
            listed = jnp.sum(jnp.where((place == lane.astype(F32)) & (active > 0.0), number, 0.0), axis=0, keepdims=True)
            tab_ref[g, LISTED:LISTED + 1, :] = listed.astype(jnp.int32)
            tab_ref[g, ACTIVE:ACTIVE + 1, :] = jnp.sum(active, axis=0, keepdims=True).astype(jnp.int32)


LOG2E = 1.4426950408889634


def mamba_kernel(x_hbm, cs_hbm, h_hbm, g_ref, win3_ref, cw_ref, cb_ref, wxp_ref, gdt_ref, gb_ref, gc_ref, wdt_ref, bdt_ref, alog_ref, dskip_ref, wout_ref,
                 uo_hbm, us_hbm, chip2_hbm, chip3_hbm, co_hbm, ho_hbm,
                 x_s, cs_s, co_s, h_s, xc_s, z_s, p_s, m_s, u_s, win_ref, g4_ref, wdt4, ones_s, a_s, q_s, delta_s, dx_s, y_s,
                 in_sem, h_sem, out_sem, ho_sem, psend, precv, msend, mrecv):
    steps, batch, _ = x_s.shape
    inner = cs_s.shape[2]
    state = alog_ref.shape[0]
    rank = wdt_ref.shape[0]
    width = rank + 2 * state
    lanes = steps * width
    half = steps // 2
    rows = batch // CHUNKS
    tiles = inner // 128
    me = lax.axis_index("tp")
    core = lax.rem(me, 2)
    sibling = me + 1 - 2 * core
    partner = lax.rem(me + 2, 4)

    barrier = pltpu.get_barrier_semaphore()
    for peer in (sibling, partner):
        pl.semaphore_signal(barrier, inc=1, device_id={"tp": peer}, device_id_type=pl.DeviceIdType.MESH)

    def span(c):
        return pl.ds(c * rows, rows)

    def loads(c):
        return [
            pltpu.make_async_copy(x_hbm.at[:, span(c), :], x_s.at[:, span(c), :], in_sem.at[0, c]),
            pltpu.make_async_copy(cs_hbm.at[:, span(c), :], cs_s.at[:, span(c), :], in_sem.at[1, c]),
        ]

    def state_rows(c):
        return pl.ds(c * rows * state, rows * state)

    def h_loads(c):
        return [pltpu.make_async_copy(h_hbm.at[state_rows(c), pl.ds(l * 128, 128)], h_s.at[l, state_rows(c), :], h_sem.at[l, c]) for l in range(tiles)]

    def h_stores(c):
        return [pltpu.make_async_copy(h_s.at[l, state_rows(c), :], ho_hbm.at[state_rows(c), pl.ds(l * 128, 128)], ho_sem.at[l, c]) for l in range(tiles)]

    def co_store(c):
        return pltpu.make_async_copy(co_s.at[:, span(c), :], co_hbm.at[:, span(c), :], out_sem.at[0, c])

    def remote(buf, c, src, dst, send, recv, stage, peer):
        return pltpu.make_async_remote_copy(
            src_ref=buf.at[src, c], dst_ref=buf.at[dst, c], send_sem=send.at[stage, c], recv_sem=recv.at[stage, c],
            device_id={"tp": peer}, device_id_type=pl.DeviceIdType.MESH)

    def p_beside(c):
        return remote(p_s, c, 1, 2, psend, precv, 0, sibling)

    def p_across(c):
        return remote(p_s, c, 3, 4, psend, precv, 1, partner)

    def p_back(c):
        return remote(p_s, c, 5, 6, psend, precv, 2, sibling)

    def m_beside(c):
        return remote(m_s, c, 1, 2, msend, mrecv, 0, sibling)

    def m_across(c):
        return remote(m_s, c, 3, 4, msend, mrecv, 1, partner)

    def u_back(c):
        return pltpu.make_async_remote_copy(
            src_ref=u_s.at[0, c], dst_ref=u_s.at[1, c], send_sem=msend.at[2, c], recv_sem=mrecv.at[2, c],
            device_id={"tp": sibling}, device_id_type=pl.DeviceIdType.MESH)

    for c in range(CHUNKS):
        for cp in loads(c):
            cp.start()
    for c in range(CHUNKS):
        for cp in h_loads(c):
            cp.start()

    gain = row(g_ref)
    for k in range(2):
        win_ref[:, k * inner:(k + 1) * inner] = win3_ref[:, k, :]

    def project(c):
        for cp in loads(c):
            cp.wait()

        def block(i, carry):
            r = pl.multiple_of(c * rows + i * 128, 128)
            seq = [cs_s[j, pl.ds(r, 128), :].astype(F32) for j in range(3)]
            part = []
            for s in range(steps):
                x = x_s[s, pl.ds(r, 128), :].astype(F32)
                n = norm_rows(x, gain).astype(BF16)
                xz = jnp.dot(n, win_ref[...], preferred_element_type=F32).astype(BF16)
                z_s[s, pl.ds(r, 128), :] = xz[:, inner:]
                xi = xz[:, :inner]
                if s > 0:
                    co_s[s - 1, pl.ds(r, 128), :] = xi
                seq.append(xi.astype(F32))
                acc = seq[s] * cw_ref[0:1, :].astype(F32)
                for j in range(1, 4):
                    acc = acc + seq[s + j] * cw_ref[j:j + 1, :].astype(F32)
                xc = silu(acc + row(cb_ref)).astype(BF16)
                xc_s[s, pl.ds(r, 128), :] = xc
                part.append(mm_t(xc, wxp_ref[...]))
            low = jnp.concatenate(part[:2], axis=1)
            high = jnp.concatenate(part[2:], axis=1)
            q = pl.multiple_of(i * 128, 128)
            p_s[0, c, pl.ds(q, 128), :] = jnp.where(core == 0, low, high)
            p_s[1, c, pl.ds(q, 128), :] = jnp.where(core == 0, high, low)
            return carry

        lax.fori_loop(0, rows // 128, block, 0)
        co_store(c).start()

    def p_sum(c):
        p_beside(c).wait_recv()
        p_s[3, c] = p_s[0, c] + p_s[2, c]
        p_across(c).start()

    def p_whole(c):
        p_across(c).wait_recv()
        p_s[5, c] = p_s[3, c] + p_s[4, c]
        p_back(c).start()

    def scan(c, between=None):
        p_back(c).wait_recv()
        for cp in h_loads(c):
            cp.wait()

        def block(i, carry):
            r = pl.multiple_of(i * 128, 128)
            g = pl.multiple_of(c * rows + i * 128, 128)
            own, sib = p_s[5, c, pl.ds(r, 128), :], p_s[6, c, pl.ds(r, 128), :]
            p = jnp.concatenate([jnp.where(core == 0, own, sib), jnp.where(core == 0, sib, own)], axis=1)
            sq = p * p
            s1 = sq.astype(BF16)
            rest = sq - s1.astype(F32)
            s2 = rest.astype(BF16)
            s3 = (rest - s2.astype(F32)).astype(BF16)
            mean = sum(jnp.dot(v, ones_s[...], preferred_element_type=F32) for v in (s3, s2, s1))
            norm = p * lax.rsqrt(mean + EPSILON) * g4_ref[...]
            for s in range(steps):
                first = s * width + rank
                q_s[s] = jnp.concatenate([norm[:, first:first + 2 * state], jnp.zeros((128, 128 - 2 * state), F32)], axis=1)
            pre = jnp.dot(norm.astype(BF16), wdt4[...], preferred_element_type=F32)
            bias = row(bdt_ref)
            for s in range(steps):
                v = pre[:, s * inner:(s + 1) * inner] + bias
                delta = jnp.maximum(v, 0.0) + jnp.log1p(jnp.exp(-jnp.abs(v)))
                delta_s[s] = delta
                dx_s[s] = delta * xc_s[s, pl.ds(g, 128), :].astype(F32)

            def tile(t, carry2):
                b = pl.multiple_of(t * 8, 8)
                base = (g + b) * state
                cut = [slice(l * 128, (l + 1) * 128) for l in range(tiles)]
                dl = [[delta_s[s, pl.ds(b, 8), k] for k in cut] for s in range(steps)]
                dx = [[dx_s[s, pl.ds(b, 8), k] for k in cut] for s in range(steps)]
                qs = [q_s[s, pl.ds(b, 8), :] for s in range(steps)]
                ys = [[None] * tiles for _ in range(steps)]
                for n in range(state):
                    bs = [jnp.broadcast_to(qs[s][:, n:n + 1], (8, 128)) for s in range(steps)]
                    cs = [jnp.broadcast_to(qs[s][:, n + state:n + state + 1], (8, 128)) for s in range(steps)]
                    for l in range(tiles):
                        a = a_s[n:n + 1, cut[l]]
                        spot = (l, pl.ds(base + n, 8, stride=state))
                        h = h_s[spot]
                        for s in range(steps):
                            h = jnp.exp2(dl[s][l] * a) * h + dx[s][l] * bs[s]
                            hc = h * cs[s]
                            ys[s][l] = hc if n == 0 else ys[s][l] + hc
                        h_s[spot] = h
                for s in range(steps):
                    for l in range(tiles):
                        y_s[s, pl.ds(b, 8), cut[l]] = ys[s][l]
                return carry2

            lax.fori_loop(0, 16, tile, 0, unroll=2)
            for s in range(steps):
                xc = xc_s[s, pl.ds(g, 128), :].astype(F32)
                yg = ((y_s[s] + row(dskip_ref) * xc) * silu(z_s[s, pl.ds(g, 128), :].astype(F32))).astype(BF16)
                out = jnp.dot(yg, wout_ref[...], preferred_element_type=F32).astype(BF16)
                m_s[lax.rem(core + s // half, 2), c, s % half, pl.ds(r, 128), :] = out
            return carry

        if between is None:
            lax.fori_loop(0, rows // 128, block, 0)
        else:
            lax.fori_loop(0, 1, block, 0)
            between()
            lax.fori_loop(1, rows // 128, block, 0)
        for cp in h_stores(c):
            cp.start()
        m_beside(c).start()

    def chip_out(c):
        return pltpu.make_async_copy(m_s.at[3, c], (chip2_hbm, chip3_hbm)[c - WHOLE], out_sem.at[1, c])

    def m_sum(c):
        m_beside(c).wait_recv()
        for s in range(half):
            m_s[3, c, s] = (m_s[0, c, s].astype(F32) + m_s[2, c, s].astype(F32)).astype(BF16)
        if c < WHOLE:
            m_across(c).start()
        else:
            chip_out(c).start()

    def uo_out(c):
        return pltpu.make_async_copy(u_s.at[0, c], uo_hbm.at[c], out_sem.at[1, c])

    def us_out(c):
        return pltpu.make_async_copy(u_s.at[1, c], us_hbm.at[c], out_sem.at[2, c])

    def m_whole(c):
        m_across(c).wait_recv()
        for s in range(half):
            x = x_s[core * half + s, span(c), :].astype(F32)
            u_s[0, c, s] = (x + (m_s[3, c, s].astype(F32) + m_s[4, c, s].astype(F32))).astype(BF16)
        u_back(c).start()
        uo_out(c).start()

    project(0)
    pl.semaphore_wait(barrier, 2)
    p_beside(0).start()
    project(1)
    p_beside(1).start()
    p_sum(0)
    project(2)
    p_beside(2).start()
    p_sum(1)
    project(3)
    p_beside(3).start()
    p_sum(2)
    p_whole(0)

    wdt4[...] = jnp.zeros_like(wdt4)
    for s in range(steps):
        wdt4[s * width:s * width + rank, s * inner:(s + 1) * inner] = wdt_ref[...]

    def group(v):
        step, col = v // width, lax.rem(v, width)
        return step * 4 + (col >= rank).astype(jnp.int32) + (col >= rank + state).astype(jnp.int32)

    gi = group(lax.broadcasted_iota(jnp.int32, (lanes, lanes), 0))
    gj = group(lax.broadcasted_iota(jnp.int32, (lanes, lanes), 1))
    inv = jnp.where(lax.rem(gj, 4) == 0, 1.0 / rank, 1.0 / state)
    ones_s[...] = jnp.where(gi == gj, inv, 0.0).astype(BF16)
    for s in range(steps):
        for ref, at in ((gdt_ref, 0), (gb_ref, rank), (gc_ref, rank + state)):
            g4_ref[:, s * width + at:s * width + at + ref.shape[0]] = row(ref)
    a_s[...] = -LOG2E * jnp.exp(alog_ref[...])

    p_sum(3)
    scan(0)
    p_whole(1)
    p_whole(2)
    m_sum(0)
    p_whole(3)
    scan(1)
    m_sum(1)
    scan(2)
    m_sum(2)
    m_whole(0)
    scan(3, lambda: m_whole(1))
    m_sum(3)
    for c in range(WHOLE):
        u_back(c).wait_recv()
        us_out(c).start()
    for c in range(CHUNKS):
        p_beside(c).wait_send()
        p_across(c).wait_send()
        p_back(c).wait_send()
        m_beside(c).wait_send()
        co_store(c).wait()
        for cp in h_stores(c):
            cp.wait()
        if c < WHOLE:
            m_across(c).wait_send()
            u_back(c).wait_send()
            uo_out(c).wait()
            us_out(c).wait()
        else:
            chip_out(c).wait()


def moe_kernel(g, size, *refs):
    count_in = 2 + 2 * size
    tab_ref, pos_ref = refs[:2]
    us = refs[2:count_in]
    gff_ref, wr_ref, wg_ref, wu_ref, wd_ref, h_hbm, cv_hbm = refs[count_in:count_in + 7]
    refs = refs[count_in + (9 if g else 7):]
    outs = refs[:2 * size]
    ho_hbm, co_hbm = refs[2 * size:count_in]
    wg, wu, wd, sems, m_s, hot_s, in_s, out_s, prob_s, h_s, cv_s, st_sem = refs[-12:]
    _, half, rows, d_model = us[0].shape
    experts = wr_ref.shape[0]
    tokens = 2 * half * rows
    slots = hot_s.shape[0] // size
    room = in_s.shape[0] // size
    core = lax.rem(lax.axis_index("tp"), 2)
    active = tab_ref[0, ACTIVE, 0]

    def copies(i):
        e = tab_ref[0, LISTED, i]
        slot = lax.rem(i, RING)
        return [pltpu.make_async_copy(src.at[e], dst.at[slot], sems.at[k, slot]) for k, (src, dst) in enumerate(((wg_ref, wg), (wu_ref, wu), (wd_ref, wd)))]

    def fetch(i):
        @pl.when(i < active)
        def _():
            for cp in copies(i):
                cp.start()

    for i in range(RING - 1):
        fetch(i)
    h_span = pl.ds(GROUPS[g][0] * h_s.shape[0] // size, h_s.shape[0])
    cv_span = pl.ds(GROUPS[g][0] * cv_s.shape[1] // size, cv_s.shape[1])
    pulls = [pltpu.make_async_copy(h_hbm.at[h_span, :], h_s, st_sem.at[0]), pltpu.make_async_copy(cv_hbm.at[:, cv_span, :], cv_s, st_sem.at[1])]
    pushes = [pltpu.make_async_copy(h_s, ho_hbm.at[h_span, :], st_sem.at[2]), pltpu.make_async_copy(cv_s, co_hbm.at[:, cv_span, :], st_sem.at[3])]
    for cp in pulls:
        cp.start()
    gain = row(gff_ref)
    for j in range(size):
        for k in range(2):
            src = us[k * size + j]
            first = j * tokens + jnp.where(core == k, 0, half * rows)
            for s in range(half):
                u = src[0, s].astype(F32)
                m = norm_rows(u, gain)
                m_s[pl.ds(pl.multiple_of(first + s * rows, rows), rows), :] = m.astype(BF16)

    down = lax.broadcasted_iota(jnp.int32, (256, tokens), 0).astype(F32).astype(BF16)
    for j in range(size):
        pos = pos_ref[j]

        def order(i, carry):
            r = pl.multiple_of(i * 256, 256)
            local = jnp.where((pos >= r) & (pos < r + 256), pos - r, -1).astype(F32).astype(BF16)
            hot = jnp.where(down == local, jnp.ones((), BF16), jnp.zeros((), BF16))
            hot_s[pl.ds(j * slots + r, 256), :] = hot
            m = jnp.dot(hot, m_s[j * tokens:(j + 1) * tokens, :], preferred_element_type=F32).astype(BF16)
            at = pl.ds(j * room + r, 256)
            in_s[at, :] = m
            out_s[at, :] = jnp.zeros((256, d_model), BF16)
            logits = mm_t(m, wr_ref[...])
            ex = jnp.exp(logits - jnp.max(logits, axis=-1, keepdims=True))
            prob_s[at, :] = ex / jnp.sum(ex, axis=-1, keepdims=True)
            return carry

        lax.fori_loop(0, slots // 256, order, 0, unroll=True)
    for pull, push in zip(pulls, pushes):
        pull.wait()
        push.start()

    def feed(e, slot, r, size):
        m = in_s[pl.ds(r, size), :]
        gate = jnp.dot(m, wg[slot], preferred_element_type=F32)
        up = jnp.dot(m, wu[slot], preferred_element_type=F32)
        q = (silu(gate) * up).astype(BF16)
        lane = lax.broadcasted_iota(jnp.int32, (size, experts), 1)
        prob = jnp.sum(jnp.where(lane == e, prob_s[pl.ds(r, size), :], 0.0), axis=-1, keepdims=True)
        out_s[pl.ds(r, size), :] = (prob * jnp.dot(q, wd[slot], preferred_element_type=F32)).astype(BF16)

    def expert(i, carry):
        e = tab_ref[0, LISTED, i]
        slot = lax.rem(i, RING)
        fetch(i + RING - 1)
        for cp in copies(i):
            cp.wait()

        def part(j, c1):
            start = tab_ref[0, 16 * j + e, 0] + j * room
            count = tab_ref[0, 16 * j + e, 1]
            big = (count + TILE - 1) // (2 * TILE)

            def tile(k, c2):
                feed(e, slot, pl.multiple_of(start + k * (2 * TILE), ROW_ALIGN), 2 * TILE)
                return c2

            lax.fori_loop(0, big, tile, 0)

            @pl.when(count > big * (2 * TILE))
            def _():
                feed(e, slot, pl.multiple_of(start + big * (2 * TILE), ROW_ALIGN), TILE)

            return c1

        return lax.fori_loop(0, size, part, carry)

    lax.fori_loop(0, active, expert, 0)

    def restore(j, k, dst):
        first = jnp.where(core == k, 0, half * rows)
        for s in range(half):
            hot = hot_s[j * slots:(j + 1) * slots, pl.ds(pl.multiple_of(first + s * rows, rows), rows)]
            got = lax.dot_general(hot, out_s[j * room:j * room + slots, :], (((0,), (0,)), ((), ())), preferred_element_type=F32)
            dst[s] = got.astype(BF16)

    for j in range(size):
        for k in range(2):
            restore(j, k, outs[k * size + j])
    for cp in pushes:
        cp.wait()


def solution(mesh):
    act_spec = P(None, "dp", None)
    state_spec = P("dp", "tp", None)
    in_specs = (act_spec, state_spec, state_spec, act_spec, P(None), P(None, None, "tp"), P("tp", None), P("tp"), P("tp", None), P(None), P(None), P(None), P(None, "tp"), P("tp"), P("tp", None), P("tp"), P("tp", None), P(None), P(None, None), P(None, None, "tp"), P(None, None, "tp"), P(None, "tp", None))
    out_specs = (act_spec, state_spec, state_spec)
    across = [(0, 2), (2, 0), (1, 3), (3, 1)]
    beside = [(0, 1), (1, 0), (2, 3), (3, 2)]

    def layer_steps(x_steps, conv_state, ssm_state, expert_ids, g_in, w_in, conv_w, conv_b, w_xp, g_dt, g_b, g_c, w_dt, b_dt, a_log, d_skip, w_out, g_ff, w_router, w_gate, w_up, w_down):
        steps, batch, d_model = x_steps.shape
        inner = w_in.shape[2]
        rank = w_dt.shape[0]
        state = a_log.shape[1]
        experts, _, ffn = w_gate.shape
        width = rank + 2 * state
        half = steps // 2
        rows = batch // CHUNKS
        tokens = steps * rows
        slots = tokens + experts * ROW_ALIGN
        core = lax.rem(lax.axis_index("tp"), 2)

        conv_t = jnp.transpose(conv_state, (2, 0, 1))
        h_rows = jnp.transpose(ssm_state, (0, 2, 1)).reshape(batch * state, inner)
        alog_t = a_log.T

        ids = jnp.transpose(expert_ids, (0, 2, 1))
        pos, table = pl.pallas_call(
            routes_kernel,
            out_shape=(jax.ShapeDtypeStruct((CHUNKS, 1, tokens), jnp.int32), jax.ShapeDtypeStruct((len(GROUPS), ACTIVE + 7, 128), jnp.int32)),
            compiler_params=params(),
            name="routes",
        )(ids)

        vmem = pl.BlockSpec(memory_space=pltpu.VMEM)
        piece = (half, rows, d_model)
        u_first, u_second, *chips, conv_mid, h_mid = pl.pallas_call(
            mamba_kernel,
            in_specs=[HBM, HBM, HBM] + [vmem] * 13,
            out_specs=[HBM] * 6,
            out_shape=[
                jax.ShapeDtypeStruct((WHOLE,) + piece, BF16),
                jax.ShapeDtypeStruct((WHOLE,) + piece, BF16),
                jax.ShapeDtypeStruct(piece, BF16),
                jax.ShapeDtypeStruct(piece, BF16),
                jax.ShapeDtypeStruct((3, batch, inner), BF16),
                jax.ShapeDtypeStruct((batch * state, inner), F32),
            ],
            scratch_shapes=[
                pltpu.VMEM((steps, batch, d_model), BF16),
                pltpu.VMEM((3, batch, inner), BF16),
                pltpu.VMEM((3, batch, inner), BF16),
                pltpu.VMEM((inner // 128, batch * state, 128), F32),
                pltpu.VMEM((steps, batch, inner), BF16),
                pltpu.VMEM((steps, batch, inner), BF16),
                pltpu.VMEM((7, CHUNKS, rows, 2 * width), F32),
                pltpu.VMEM((5, CHUNKS) + piece, BF16),
                pltpu.VMEM((2, CHUNKS) + piece, BF16),
                pltpu.VMEM((d_model, 2 * inner), BF16),
                pltpu.VMEM((1, steps * width), F32),
                pltpu.VMEM((steps * width, steps * inner), BF16),
                pltpu.VMEM((steps * width, steps * width), BF16),
                pltpu.VMEM((state, inner), F32),
                pltpu.VMEM((steps, 128, 128), F32),
                pltpu.VMEM((steps, 128, inner), F32),
                pltpu.VMEM((steps, 128, inner), F32),
                pltpu.VMEM((steps, 128, inner), F32),
                pltpu.SemaphoreType.DMA((2, CHUNKS)),
                pltpu.SemaphoreType.DMA((inner // 128, CHUNKS)),
                pltpu.SemaphoreType.DMA((3, CHUNKS)),
                pltpu.SemaphoreType.DMA((inner // 128, CHUNKS)),
                pltpu.SemaphoreType.DMA((3, CHUNKS)),
                pltpu.SemaphoreType.DMA((3, CHUNKS)),
                pltpu.SemaphoreType.DMA((3, CHUNKS)),
                pltpu.SemaphoreType.DMA((3, CHUNKS)),
            ],
            compiler_params=params(collective_id=0, has_side_effects=True),
            cost_estimate=pl.CostEstimate(flops=int(8e9), bytes_accessed=int(45e6), transcendentals=0),
            name="mamba",
        )(x_steps, conv_t, h_rows, g_in, w_in, conv_w.T, conv_b, w_xp.T, g_dt, g_b, g_c, w_dt, b_dt, alog_t, d_skip, w_out)

        room = slots + 2 * TILE

        def run_moe(g, u_args, u_specs, states):
            extra = [] if states is None else list(states)
            size = len(GROUPS[g])
            first = GROUPS[g][0] // size
            count_in = 2 + 2 * size
            return pl.pallas_call(
                functools.partial(moe_kernel, g, size),
                grid=(1,),
                in_specs=[pl.BlockSpec((1, ACTIVE + 7, 128), lambda i: (g, 0, 0), memory_space=pltpu.SMEM), pl.BlockSpec((size, 1, tokens), lambda i: (first, 0, 0))] + u_specs + [vmem, vmem] + [HBM] * (5 + len(extra)),
                out_specs=[vmem] * (2 * size) + [HBM, HBM] + ([] if extra else [HBM]),
                out_shape=[jax.ShapeDtypeStruct(piece, BF16)] * (2 * size) + [jax.ShapeDtypeStruct(h_mid.shape, F32), jax.ShapeDtypeStruct(conv_mid.shape, BF16)] + ([] if extra else [jax.ShapeDtypeStruct(x_steps.shape, BF16)]),
                scratch_shapes=[
                    pltpu.VMEM((RING, d_model, ffn), BF16),
                    pltpu.VMEM((RING, d_model, ffn), BF16),
                    pltpu.VMEM((RING, ffn, d_model), BF16),
                    pltpu.SemaphoreType.DMA((3, RING)),
                    pltpu.VMEM((size * tokens, d_model), BF16),
                    pltpu.VMEM((size * slots, tokens), BF16),
                    pltpu.VMEM((size * room, d_model), BF16),
                    pltpu.VMEM((size * room, d_model), BF16),
                    pltpu.VMEM((size * room, experts), F32),
                    pltpu.VMEM((size * rows * state, inner), F32),
                    pltpu.VMEM((3, size * rows, inner), BF16),
                    pltpu.SemaphoreType.DMA((4,)),
                ],
                input_output_aliases={count_in + 7: 2 * size, count_in + 8: 2 * size + 1} if extra else {},
                compiler_params=params(),
                cost_estimate=pl.CostEstimate(flops=int(3e9) * size, bytes_accessed=int(40e6), transcendentals=0),
            )(table, pos, *u_args, g_ff, w_router.T, w_gate, w_up, w_down, h_mid, conv_mid, *extra)

        def both(keep, send, dtype):
            got = lax.ppermute(send, "tp", beside)
            chip = (keep.astype(F32) + got.astype(F32)).astype(dtype)
            return chip, lax.ppermute(chip, "tp", across)

        owns = {}
        spot = {}
        for c in range(WHOLE):
            spot[c] = (u_first, u_second, pl.BlockSpec((1,) + piece, lambda i, c=c: (c, 0, 0, 0)))
            owns[c] = lambda c=c: u_first[c]
        for c in range(WHOLE, CHUNKS):
            chip = chips[c - WHOLE]
            far = lax.ppermute(chip, "tp", across)
            x_own = lax.dynamic_slice(x_steps, (half * core, c * rows, 0), (half, rows, d_model))
            u_own = (x_own.astype(F32) + (chip.astype(F32) + far.astype(F32))).astype(BF16)
            u_sib = lax.ppermute(u_own, "tp", beside)
            spot[c] = (u_own[None], u_sib[None], pl.BlockSpec((1,) + piece, lambda i: (0, 0, 0, 0)))
            owns[c] = lambda u_own=u_own: u_own

        states = None
        pieces = {}
        for g, members in enumerate(GROUPS):
            size = len(members)
            group = [spot[c] for c in members]
            got = run_moe(g, [v[0] for v in group] + [v[1] for v in group], [v[2] for v in group] * 2, states)
            states = got[2 * size:2 * size + 2]
            if g == 0:
                y_steps = got[-1]
            for j, c in enumerate(members):
                chip, far = both(got[j], got[size + j], BF16)
                y_own = (owns[c]().astype(F32) + (chip.astype(F32) + far.astype(F32))).astype(BF16)
                y_sib = lax.ppermute(y_own, "tp", beside)
                pieces[c] = (y_own, y_sib)
        for some in (range(LAST), (LAST,)):
            for k in range(2):
                for c in some:
                    y_steps = lax.dynamic_update_slice(y_steps, pieces[c][k], (half * lax.rem(core + k, 2), c * rows, 0))
        ssm_out, conv_out = states
        ssm_fin = jnp.transpose(ssm_out.reshape(batch, state, inner), (0, 2, 1))
        return y_steps, jnp.transpose(conv_out, (1, 2, 0)), ssm_fin

    return jax.shard_map(layer_steps, mesh=mesh, in_specs=in_specs, out_specs=out_specs, check_vma=False)
```

```python
import functools

import jax
import jax.numpy as jnp
from jax import lax
from jax.experimental import pallas as pl
from jax.experimental.pallas import tpu as pltpu
from jax.sharding import PartitionSpec as P


EPSILON = 1e-6
CHUNKS = 4
ROW_ALIGN = 16
TILE = 128
GROUPS = ((0, 1), (2,), (3,))
LAST = len(GROUPS) - 1
LISTED = 32
ACTIVE = 33
RING = 6
WHOLE = 2
F32 = jnp.float32
BF16 = jnp.bfloat16
HBM = pl.BlockSpec(memory_space=pl.ANY)


def whole(shape):
    return pl.BlockSpec(shape, lambda *_: (0,) * len(shape))


def params(**kw):
    return pltpu.CompilerParams(vmem_limit_bytes=56 * 1024 * 1024, **kw)


def row(ref):
    return ref[...].astype(F32).reshape(1, -1)


def norm_rows(v, gain):
    return v * lax.rsqrt(jnp.mean(v * v, axis=-1, keepdims=True) + EPSILON) * gain


def mm_t(a, b):
    return lax.dot_general(a, b, (((1,), (1,)), ((), ())), preferred_element_type=F32)


def silu(v):
    return v * jax.nn.sigmoid(v)


def routes_kernel(ids_ref, pos_ref, tab_ref):
    _, _, tokens = pos_ref.shape
    steps = ids_ref.shape[0]
    rows = tokens // steps
    experts = 16
    upper = (lax.broadcasted_iota(jnp.int32, (tokens, tokens), 0) <= lax.broadcasted_iota(jnp.int32, (tokens, tokens), 1)).astype(F32).astype(BF16)
    before = (lax.broadcasted_iota(jnp.int32, (experts, experts), 1) < lax.broadcasted_iota(jnp.int32, (experts, experts), 0)).astype(F32).astype(BF16)
    lane = lax.broadcasted_iota(jnp.int32, (experts, 128), 1)
    number = lax.broadcasted_iota(jnp.int32, (experts, 128), 0).astype(F32)
    for g, k, c in [(g, k, c) for g, group in enumerate(GROUPS) for k, c in enumerate(group)]:
        ids = jnp.concatenate([ids_ref[s, :, c * rows:(c + 1) * rows] for s in range(steps)], axis=1)
        hit = lax.broadcasted_iota(jnp.int32, (experts, tokens), 0) == ids
        hot = hit.astype(F32)
        rank = jnp.dot(hot.astype(BF16), upper, preferred_element_type=F32)
        count = jnp.broadcast_to(jnp.sum(hot, axis=1, keepdims=True), (experts, 128))
        blocks = jnp.floor((count + (ROW_ALIGN - 1)) * (1.0 / ROW_ALIGN))
        start = ROW_ALIGN * jnp.dot(before, blocks.astype(BF16), preferred_element_type=F32)
        pos_ref[c] = jnp.sum(hot * (start[:, :1] + rank - 1.0), axis=0, keepdims=True).astype(jnp.int32)
        tab_ref[g, 16 * k:16 * k + 16, :] = jnp.where(lane == 0, start, count).astype(jnp.int32)
        total = count if k == 0 else total + count
        if c == GROUPS[g][-1]:
            active = (total > 0.0).astype(F32)
            place = jnp.dot(before, active.astype(BF16), preferred_element_type=F32)
            listed = jnp.sum(jnp.where((place == lane.astype(F32)) & (active > 0.0), number, 0.0), axis=0, keepdims=True)
            tab_ref[g, LISTED:LISTED + 1, :] = listed.astype(jnp.int32)
            tab_ref[g, ACTIVE:ACTIVE + 1, :] = jnp.sum(active, axis=0, keepdims=True).astype(jnp.int32)


LOG2E = 1.4426950408889634


def mamba_kernel(x_hbm, cs_hbm, h_hbm, g_ref, win3_ref, cw_ref, cb_ref, wxp_ref, gdt_ref, gb_ref, gc_ref, wdt_ref, bdt_ref, alog_ref, dskip_ref, wout_ref,
                 uo_hbm, us_hbm, chip2_hbm, chip3_hbm, co_hbm, ho_hbm,
                 x_s, cs_s, co_s, h_s, xc_s, z_s, p_s, m_s, u_s, win_ref, g4_ref, wdt4, ones_s, a_s, q_s, delta_s, dx_s, y_s,
                 in_sem, h_sem, out_sem, ho_sem, psend, precv, msend, mrecv):
    steps, batch, _ = x_s.shape
    inner = cs_s.shape[2]
    state = alog_ref.shape[0]
    rank = wdt_ref.shape[0]
    width = rank + 2 * state
    lanes = steps * width
    half = steps // 2
    rows = batch // CHUNKS
    tiles = inner // 128
    me = lax.axis_index("tp")
    core = lax.rem(me, 2)
    sibling = me + 1 - 2 * core
    partner = lax.rem(me + 2, 4)

    barrier = pltpu.get_barrier_semaphore()
    for peer in (sibling, partner):
        pl.semaphore_signal(barrier, inc=1, device_id={"tp": peer}, device_id_type=pl.DeviceIdType.MESH)

    def span(c):
        return pl.ds(c * rows, rows)

    def loads(c):
        return [
            pltpu.make_async_copy(x_hbm.at[:, span(c), :], x_s.at[:, span(c), :], in_sem.at[0, c]),
            pltpu.make_async_copy(cs_hbm.at[:, span(c), :], cs_s.at[:, span(c), :], in_sem.at[1, c]),
        ]

    def state_rows(c):
        return pl.ds(c * rows * state, rows * state)

    def h_loads(c):
        return [pltpu.make_async_copy(h_hbm.at[state_rows(c), pl.ds(l * 128, 128)], h_s.at[l, state_rows(c), :], h_sem.at[l, c]) for l in range(tiles)]

    def h_stores(c):
        return [pltpu.make_async_copy(h_s.at[l, state_rows(c), :], ho_hbm.at[state_rows(c), pl.ds(l * 128, 128)], ho_sem.at[l, c]) for l in range(tiles)]

    def co_store(c):
        return pltpu.make_async_copy(co_s.at[:, span(c), :], co_hbm.at[:, span(c), :], out_sem.at[0, c])

    def remote(buf, c, src, dst, send, recv, stage, peer):
        return pltpu.make_async_remote_copy(
            src_ref=buf.at[src, c], dst_ref=buf.at[dst, c], send_sem=send.at[stage, c], recv_sem=recv.at[stage, c],
            device_id={"tp": peer}, device_id_type=pl.DeviceIdType.MESH)

    def p_beside(c):
        return remote(p_s, c, 1, 2, psend, precv, 0, sibling)

    def p_across(c):
        return remote(p_s, c, 3, 4, psend, precv, 1, partner)

    def p_back(c):
        return remote(p_s, c, 5, 6, psend, precv, 2, sibling)

    def m_beside(c):
        return remote(m_s, c, 1, 2, msend, mrecv, 0, sibling)

    def m_across(c):
        return remote(m_s, c, 3, 4, msend, mrecv, 1, partner)

    def u_back(c):
        return pltpu.make_async_remote_copy(
            src_ref=u_s.at[0, c], dst_ref=u_s.at[1, c], send_sem=msend.at[2, c], recv_sem=mrecv.at[2, c],
            device_id={"tp": sibling}, device_id_type=pl.DeviceIdType.MESH)

    for c in range(CHUNKS):
        for cp in loads(c):
            cp.start()
    for c in range(CHUNKS):
        for cp in h_loads(c):
            cp.start()

    gain = row(g_ref)
    for k in range(2):
        win_ref[:, k * inner:(k + 1) * inner] = win3_ref[:, k, :]

    def project(c):
        for cp in loads(c):
            cp.wait()

        def block(i, carry):
            r = pl.multiple_of(c * rows + i * 128, 128)
            seq = [cs_s[j, pl.ds(r, 128), :].astype(F32) for j in range(3)]
            part = []
            for s in range(steps):
                x = x_s[s, pl.ds(r, 128), :].astype(F32)
                n = norm_rows(x, gain).astype(BF16)
                xz = jnp.dot(n, win_ref[...], preferred_element_type=F32).astype(BF16)
                z_s[s, pl.ds(r, 128), :] = xz[:, inner:]
                xi = xz[:, :inner]
                if s > 0:
                    co_s[s - 1, pl.ds(r, 128), :] = xi
                seq.append(xi.astype(F32))
                acc = seq[s] * cw_ref[0:1, :].astype(F32)
                for j in range(1, 4):
                    acc = acc + seq[s + j] * cw_ref[j:j + 1, :].astype(F32)
                xc = silu(acc + row(cb_ref)).astype(BF16)
                xc_s[s, pl.ds(r, 128), :] = xc
                part.append(mm_t(xc, wxp_ref[...]))
            low = jnp.concatenate(part[:2], axis=1)
            high = jnp.concatenate(part[2:], axis=1)
            q = pl.multiple_of(i * 128, 128)
            p_s[0, c, pl.ds(q, 128), :] = jnp.where(core == 0, low, high)
            p_s[1, c, pl.ds(q, 128), :] = jnp.where(core == 0, high, low)
            return carry

        lax.fori_loop(0, rows // 128, block, 0)
        co_store(c).start()

    def p_sum(c):
        p_beside(c).wait_recv()
        p_s[3, c] = p_s[0, c] + p_s[2, c]
        p_across(c).start()

    def p_whole(c):
        p_across(c).wait_recv()
        p_s[5, c] = p_s[3, c] + p_s[4, c]
        p_back(c).start()

    def scan(c, between=None):
        p_back(c).wait_recv()
        for cp in h_loads(c):
            cp.wait()

        def block(i, carry):
            r = pl.multiple_of(i * 128, 128)
            g = pl.multiple_of(c * rows + i * 128, 128)
            own, sib = p_s[5, c, pl.ds(r, 128), :], p_s[6, c, pl.ds(r, 128), :]
            p = jnp.concatenate([jnp.where(core == 0, own, sib), jnp.where(core == 0, sib, own)], axis=1)
            sq = p * p
            s1 = sq.astype(BF16)
            rest = sq - s1.astype(F32)
            s2 = rest.astype(BF16)
            s3 = (rest - s2.astype(F32)).astype(BF16)
            mean = sum(jnp.dot(v, ones_s[...], preferred_element_type=F32) for v in (s3, s2, s1))
            norm = p * lax.rsqrt(mean + EPSILON) * g4_ref[...]
            for s in range(steps):
                first = s * width + rank
                q_s[s] = jnp.concatenate([norm[:, first:first + 2 * state], jnp.zeros((128, 128 - 2 * state), F32)], axis=1)
            pre = jnp.dot(norm.astype(BF16), wdt4[...], preferred_element_type=F32)
            bias = row(bdt_ref)
            for s in range(steps):
                v = pre[:, s * inner:(s + 1) * inner] + bias
                delta = jnp.maximum(v, 0.0) + jnp.log1p(jnp.exp(-jnp.abs(v)))
                delta_s[s] = delta
                dx_s[s] = delta * xc_s[s, pl.ds(g, 128), :].astype(F32)

            def tile(t, carry2):
                b = pl.multiple_of(t * 8, 8)
                base = (g + b) * state
                cut = [slice(l * 128, (l + 1) * 128) for l in range(tiles)]
                dl = [[delta_s[s, pl.ds(b, 8), k] for k in cut] for s in range(steps)]
                dx = [[dx_s[s, pl.ds(b, 8), k] for k in cut] for s in range(steps)]
                qs = [q_s[s, pl.ds(b, 8), :] for s in range(steps)]
                ys = [[None] * tiles for _ in range(steps)]
                for n in range(state):
                    bs = [jnp.broadcast_to(qs[s][:, n:n + 1], (8, 128)) for s in range(steps)]
                    cs = [jnp.broadcast_to(qs[s][:, n + state:n + state + 1], (8, 128)) for s in range(steps)]
                    for l in range(tiles):
                        a = a_s[n:n + 1, cut[l]]
                        spot = (l, pl.ds(base + n, 8, stride=state))
                        h = h_s[spot]
                        for s in range(steps):
                            h = jnp.exp2(dl[s][l] * a) * h + dx[s][l] * bs[s]
                            hc = h * cs[s]
                            ys[s][l] = hc if n == 0 else ys[s][l] + hc
                        h_s[spot] = h
                for s in range(steps):
                    for l in range(tiles):
                        y_s[s, pl.ds(b, 8), cut[l]] = ys[s][l]
                return carry2

            lax.fori_loop(0, 16, tile, 0, unroll=2)
            for s in range(steps):
                xc = xc_s[s, pl.ds(g, 128), :].astype(F32)
                yg = ((y_s[s] + row(dskip_ref) * xc) * silu(z_s[s, pl.ds(g, 128), :].astype(F32))).astype(BF16)
                out = jnp.dot(yg, wout_ref[...], preferred_element_type=F32).astype(BF16)
                m_s[lax.rem(core + s // half, 2), c, s % half, pl.ds(r, 128), :] = out
            return carry

        if between is None:
            lax.fori_loop(0, rows // 128, block, 0)
        else:
            lax.fori_loop(0, 1, block, 0)
            between()
            lax.fori_loop(1, rows // 128, block, 0)
        for cp in h_stores(c):
            cp.start()
        m_beside(c).start()

    def chip_out(c):
        return pltpu.make_async_copy(m_s.at[3, c], (chip2_hbm, chip3_hbm)[c - WHOLE], out_sem.at[1, c])

    def m_sum(c):
        m_beside(c).wait_recv()
        for s in range(half):
            m_s[3, c, s] = (m_s[0, c, s].astype(F32) + m_s[2, c, s].astype(F32)).astype(BF16)
        if c < WHOLE:
            m_across(c).start()
        else:
            chip_out(c).start()

    def uo_out(c):
        return pltpu.make_async_copy(u_s.at[0, c], uo_hbm.at[:, span(c), :], out_sem.at[1, c])

    def us_out(c):
        return pltpu.make_async_copy(u_s.at[1, c], us_hbm.at[:, span(c), :], out_sem.at[2, c])

    def m_whole(c):
        m_across(c).wait_recv()
        for s in range(half):
            x = x_s[core * half + s, span(c), :].astype(F32)
            u_s[0, c, s] = (x + (m_s[3, c, s].astype(F32) + m_s[4, c, s].astype(F32))).astype(BF16)
        u_back(c).start()
        uo_out(c).start()

    project(0)
    pl.semaphore_wait(barrier, 2)
    p_beside(0).start()
    project(1)
    p_beside(1).start()
    p_sum(0)
    project(2)
    p_beside(2).start()
    p_sum(1)
    project(3)
    p_beside(3).start()
    p_sum(2)
    p_whole(0)

    wdt4[...] = jnp.zeros_like(wdt4)
    for s in range(steps):
        wdt4[s * width:s * width + rank, s * inner:(s + 1) * inner] = wdt_ref[...]

    def group(v):
        step, col = v // width, lax.rem(v, width)
        return step * 4 + (col >= rank).astype(jnp.int32) + (col >= rank + state).astype(jnp.int32)

    gi = group(lax.broadcasted_iota(jnp.int32, (lanes, lanes), 0))
    gj = group(lax.broadcasted_iota(jnp.int32, (lanes, lanes), 1))
    inv = jnp.where(lax.rem(gj, 4) == 0, 1.0 / rank, 1.0 / state)
    ones_s[...] = jnp.where(gi == gj, inv, 0.0).astype(BF16)
    for s in range(steps):
        for ref, at in ((gdt_ref, 0), (gb_ref, rank), (gc_ref, rank + state)):
            g4_ref[:, s * width + at:s * width + at + ref.shape[0]] = row(ref)
    a_s[...] = -LOG2E * jnp.exp(alog_ref[...])

    p_sum(3)
    scan(0)
    p_whole(1)
    p_whole(2)
    m_sum(0)
    p_whole(3)
    scan(1)
    m_sum(1)
    scan(2)
    m_sum(2)
    m_whole(0)
    scan(3, lambda: m_whole(1))
    m_sum(3)
    for c in range(WHOLE):
        u_back(c).wait_recv()
        us_out(c).start()
    for c in range(CHUNKS):
        p_beside(c).wait_send()
        p_across(c).wait_send()
        p_back(c).wait_send()
        m_beside(c).wait_send()
        co_store(c).wait()
        for cp in h_stores(c):
            cp.wait()
        if c < WHOLE:
            m_across(c).wait_send()
            u_back(c).wait_send()
            uo_out(c).wait()
            us_out(c).wait()
        else:
            chip_out(c).wait()


def moe_kernel(g, size, *refs):
    count_in = 2 + 2 * size
    tab_ref, pos_ref = refs[:2]
    us = refs[2:count_in]
    gff_ref, wr_ref, wg_ref, wu_ref, wd_ref, h_hbm, cv_hbm = refs[count_in:count_in + 7]
    refs = refs[count_in + (9 if g else 7):]
    outs = refs[:2]
    ho_hbm, co_hbm = refs[2:4]
    wg, wu, wd, sems, m_s, hot_s, in_s, out_s, prob_s, h_s, cv_s, st_sem = refs[-12:]
    half, rows, d_model = us[0].shape
    experts = wr_ref.shape[0]
    tokens = 2 * half * rows
    slots = hot_s.shape[0] // size
    room = in_s.shape[0] // size
    core = lax.rem(lax.axis_index("tp"), 2)
    active = tab_ref[0, ACTIVE, 0]

    def copies(i):
        e = tab_ref[0, LISTED, i]
        slot = lax.rem(i, RING)
        return [pltpu.make_async_copy(src.at[e], dst.at[slot], sems.at[k, slot]) for k, (src, dst) in enumerate(((wg_ref, wg), (wu_ref, wu), (wd_ref, wd)))]

    def fetch(i):
        @pl.when(i < active)
        def _():
            for cp in copies(i):
                cp.start()

    for i in range(RING - 1):
        fetch(i)
    h_span = pl.ds(GROUPS[g][0] * h_s.shape[0] // size, h_s.shape[0])
    cv_span = pl.ds(GROUPS[g][0] * cv_s.shape[1] // size, cv_s.shape[1])
    pulls = [pltpu.make_async_copy(h_hbm.at[h_span, :], h_s, st_sem.at[0]), pltpu.make_async_copy(cv_hbm.at[:, cv_span, :], cv_s, st_sem.at[1])]
    pushes = [pltpu.make_async_copy(h_s, ho_hbm.at[h_span, :], st_sem.at[2]), pltpu.make_async_copy(cv_s, co_hbm.at[:, cv_span, :], st_sem.at[3])]
    for cp in pulls:
        cp.start()
    gain = row(gff_ref)
    for j in range(size):
        for k in range(2):
            src = us[k * size + j]
            first = j * tokens + jnp.where(core == k, 0, half * rows)
            for s in range(half):
                u = src[s].astype(F32)
                m = norm_rows(u, gain)
                m_s[pl.ds(pl.multiple_of(first + s * rows, rows), rows), :] = m.astype(BF16)

    down = lax.broadcasted_iota(jnp.int32, (256, tokens), 0).astype(F32).astype(BF16)
    for j in range(size):
        pos = pos_ref[j]

        def order(i, carry):
            r = pl.multiple_of(i * 256, 256)
            local = jnp.where((pos >= r) & (pos < r + 256), pos - r, -1).astype(F32).astype(BF16)
            hot = jnp.where(down == local, jnp.ones((), BF16), jnp.zeros((), BF16))
            hot_s[pl.ds(j * slots + r, 256), :] = hot
            m = jnp.dot(hot, m_s[j * tokens:(j + 1) * tokens, :], preferred_element_type=F32).astype(BF16)
            at = pl.ds(j * room + r, 256)
            in_s[at, :] = m
            out_s[at, :] = jnp.zeros((256, d_model), BF16)
            logits = mm_t(m, wr_ref[...])
            ex = jnp.exp(logits - jnp.max(logits, axis=-1, keepdims=True))
            prob_s[at, :] = ex / jnp.sum(ex, axis=-1, keepdims=True)
            return carry

        lax.fori_loop(0, slots // 256, order, 0, unroll=True)
    for pull, push in zip(pulls, pushes):
        pull.wait()
        push.start()

    def feed(e, slot, r, size):
        m = in_s[pl.ds(r, size), :]
        gate = jnp.dot(m, wg[slot], preferred_element_type=F32)
        up = jnp.dot(m, wu[slot], preferred_element_type=F32)
        q = (silu(gate) * up).astype(BF16)
        lane = lax.broadcasted_iota(jnp.int32, (size, experts), 1)
        prob = jnp.sum(jnp.where(lane == e, prob_s[pl.ds(r, size), :], 0.0), axis=-1, keepdims=True)
        out_s[pl.ds(r, size), :] = (prob * jnp.dot(q, wd[slot], preferred_element_type=F32)).astype(BF16)

    def expert(i, carry):
        e = tab_ref[0, LISTED, i]
        slot = lax.rem(i, RING)
        fetch(i + RING - 1)
        for cp in copies(i):
            cp.wait()

        def part(j, c1):
            start = tab_ref[0, 16 * j + e, 0] + j * room
            count = tab_ref[0, 16 * j + e, 1]
            big = (count + TILE - 1) // (2 * TILE)

            def tile(k, c2):
                feed(e, slot, pl.multiple_of(start + k * (2 * TILE), ROW_ALIGN), 2 * TILE)
                return c2

            lax.fori_loop(0, big, tile, 0)

            @pl.when(count > big * (2 * TILE))
            def _():
                feed(e, slot, pl.multiple_of(start + big * (2 * TILE), ROW_ALIGN), TILE)

            return c1

        return lax.fori_loop(0, size, part, carry)

    lax.fori_loop(0, active, expert, 0)

    def restore(j, k, dst):
        first = jnp.where(core == k, 0, half * rows)
        for s in range(half):
            hot = hot_s[j * slots:(j + 1) * slots, pl.ds(pl.multiple_of(first + s * rows, rows), rows)]
            got = lax.dot_general(hot, out_s[j * room:j * room + slots, :], (((0,), (0,)), ((), ())), preferred_element_type=F32)
            dst[s, j * rows:(j + 1) * rows, :] = got.astype(BF16)

    for j in range(size):
        for k in range(2):
            restore(j, k, outs[k])
    for cp in pushes:
        cp.wait()


def solution(mesh):
    act_spec = P(None, "dp", None)
    state_spec = P("dp", "tp", None)
    in_specs = (act_spec, state_spec, state_spec, act_spec, P(None), P(None, None, "tp"), P("tp", None), P("tp"), P("tp", None), P(None), P(None), P(None), P(None, "tp"), P("tp"), P("tp", None), P("tp"), P("tp", None), P(None), P(None, None), P(None, None, "tp"), P(None, None, "tp"), P(None, "tp", None))
    out_specs = (act_spec, state_spec, state_spec)
    across = [(0, 2), (2, 0), (1, 3), (3, 1)]
    beside = [(0, 1), (1, 0), (2, 3), (3, 2)]

    def layer_steps(x_steps, conv_state, ssm_state, expert_ids, g_in, w_in, conv_w, conv_b, w_xp, g_dt, g_b, g_c, w_dt, b_dt, a_log, d_skip, w_out, g_ff, w_router, w_gate, w_up, w_down):
        steps, batch, d_model = x_steps.shape
        inner = w_in.shape[2]
        rank = w_dt.shape[0]
        state = a_log.shape[1]
        experts, _, ffn = w_gate.shape
        width = rank + 2 * state
        half = steps // 2
        rows = batch // CHUNKS
        tokens = steps * rows
        slots = tokens + experts * ROW_ALIGN
        core = lax.rem(lax.axis_index("tp"), 2)

        conv_t = jnp.transpose(conv_state, (2, 0, 1))
        h_rows = jnp.transpose(ssm_state, (0, 2, 1)).reshape(batch * state, inner)
        alog_t = a_log.T

        ids = jnp.transpose(expert_ids, (0, 2, 1))
        pos, table = pl.pallas_call(
            routes_kernel,
            out_shape=(jax.ShapeDtypeStruct((CHUNKS, 1, tokens), jnp.int32), jax.ShapeDtypeStruct((len(GROUPS), ACTIVE + 7, 128), jnp.int32)),
            compiler_params=params(),
            name="routes",
        )(ids)

        vmem = pl.BlockSpec(memory_space=pltpu.VMEM)
        piece = (half, rows, d_model)
        u_first, u_second, *chips, conv_mid, h_mid = pl.pallas_call(
            mamba_kernel,
            in_specs=[HBM, HBM, HBM] + [vmem] * 13,
            out_specs=[HBM] * 6,
            out_shape=[
                jax.ShapeDtypeStruct((half, WHOLE * rows, d_model), BF16),
                jax.ShapeDtypeStruct((half, WHOLE * rows, d_model), BF16),
                jax.ShapeDtypeStruct(piece, BF16),
                jax.ShapeDtypeStruct(piece, BF16),
                jax.ShapeDtypeStruct((3, batch, inner), BF16),
                jax.ShapeDtypeStruct((batch * state, inner), F32),
            ],
            scratch_shapes=[
                pltpu.VMEM((steps, batch, d_model), BF16),
                pltpu.VMEM((3, batch, inner), BF16),
                pltpu.VMEM((3, batch, inner), BF16),
                pltpu.VMEM((inner // 128, batch * state, 128), F32),
                pltpu.VMEM((steps, batch, inner), BF16),
                pltpu.VMEM((steps, batch, inner), BF16),
                pltpu.VMEM((7, CHUNKS, rows, 2 * width), F32),
                pltpu.VMEM((5, CHUNKS) + piece, BF16),
                pltpu.VMEM((2, CHUNKS) + piece, BF16),
                pltpu.VMEM((d_model, 2 * inner), BF16),
                pltpu.VMEM((1, steps * width), F32),
                pltpu.VMEM((steps * width, steps * inner), BF16),
                pltpu.VMEM((steps * width, steps * width), BF16),
                pltpu.VMEM((state, inner), F32),
                pltpu.VMEM((steps, 128, 128), F32),
                pltpu.VMEM((steps, 128, inner), F32),
                pltpu.VMEM((steps, 128, inner), F32),
                pltpu.VMEM((steps, 128, inner), F32),
                pltpu.SemaphoreType.DMA((2, CHUNKS)),
                pltpu.SemaphoreType.DMA((inner // 128, CHUNKS)),
                pltpu.SemaphoreType.DMA((3, CHUNKS)),
                pltpu.SemaphoreType.DMA((inner // 128, CHUNKS)),
                pltpu.SemaphoreType.DMA((3, CHUNKS)),
                pltpu.SemaphoreType.DMA((3, CHUNKS)),
                pltpu.SemaphoreType.DMA((3, CHUNKS)),
                pltpu.SemaphoreType.DMA((3, CHUNKS)),
            ],
            compiler_params=params(collective_id=0, has_side_effects=True),
            cost_estimate=pl.CostEstimate(flops=int(8e9), bytes_accessed=int(45e6), transcendentals=0),
            name="mamba",
        )(x_steps, conv_t, h_rows, g_in, w_in, conv_w.T, conv_b, w_xp.T, g_dt, g_b, g_c, w_dt, b_dt, alog_t, d_skip, w_out)

        room = slots + 2 * TILE

        def run_moe(g, u_args, u_specs, states):
            extra = [] if states is None else list(states)
            size = len(GROUPS[g])
            first = GROUPS[g][0] // size
            count_in = 2 + 2 * size
            return pl.pallas_call(
                functools.partial(moe_kernel, g, size),
                grid=(1,),
                in_specs=[pl.BlockSpec((1, ACTIVE + 7, 128), lambda i: (g, 0, 0), memory_space=pltpu.SMEM), pl.BlockSpec((size, 1, tokens), lambda i: (first, 0, 0))] + u_specs + [vmem, vmem] + [HBM] * (5 + len(extra)),
                out_specs=[vmem] * 2 + [HBM, HBM] + ([] if extra else [HBM]),
                out_shape=[jax.ShapeDtypeStruct((half, size * rows, d_model), BF16)] * 2 + [jax.ShapeDtypeStruct(h_mid.shape, F32), jax.ShapeDtypeStruct(conv_mid.shape, BF16)] + ([] if extra else [jax.ShapeDtypeStruct(x_steps.shape, BF16)]),
                scratch_shapes=[
                    pltpu.VMEM((RING, d_model, ffn), BF16),
                    pltpu.VMEM((RING, d_model, ffn), BF16),
                    pltpu.VMEM((RING, ffn, d_model), BF16),
                    pltpu.SemaphoreType.DMA((3, RING)),
                    pltpu.VMEM((size * tokens, d_model), BF16),
                    pltpu.VMEM((size * slots, tokens), BF16),
                    pltpu.VMEM((size * room, d_model), BF16),
                    pltpu.VMEM((size * room, d_model), BF16),
                    pltpu.VMEM((size * room, experts), F32),
                    pltpu.VMEM((size * rows * state, inner), F32),
                    pltpu.VMEM((3, size * rows, inner), BF16),
                    pltpu.SemaphoreType.DMA((4,)),
                ],
                input_output_aliases={count_in + 7: 2, count_in + 8: 3} if extra else {},
                compiler_params=params(),
                cost_estimate=pl.CostEstimate(flops=int(3e9) * size, bytes_accessed=int(40e6), transcendentals=0),
            )(table, pos, *u_args, g_ff, w_router.T, w_gate, w_up, w_down, h_mid, conv_mid, *extra)

        def both(keep, send, dtype):
            got = lax.ppermute(send, "tp", beside)
            chip = (keep.astype(F32) + got.astype(F32)).astype(dtype)
            return chip, lax.ppermute(chip, "tp", across)

        spot = {c: (u_first, u_second, pl.BlockSpec(piece, lambda i, c=c: (0, c, 0))) for c in range(WHOLE)}
        for c in range(WHOLE, CHUNKS):
            chip = chips[c - WHOLE]
            far = lax.ppermute(chip, "tp", across)
            x_own = lax.dynamic_slice(x_steps, (half * core, c * rows, 0), (half, rows, d_model))
            u_own = (x_own.astype(F32) + (chip.astype(F32) + far.astype(F32))).astype(BF16)
            u_sib = lax.ppermute(u_own, "tp", beside)
            spot[c] = (u_own, u_sib, whole(piece))

        states = None
        pieces = {}
        for g, members in enumerate(GROUPS):
            group = [spot[c] for c in members]
            got = run_moe(g, [v[0] for v in group] + [v[1] for v in group], [v[2] for v in group] * 2, states)
            states = got[2:4]
            if g == 0:
                y_steps = got[-1]
            chip, far = both(got[0], got[1], BF16)
            y_own = (group[0][0].astype(F32) + (chip.astype(F32) + far.astype(F32))).astype(BF16)
            pieces[g] = (y_own, lax.ppermute(y_own, "tp", beside))
        for some in (range(LAST), (LAST,)):
            for k in range(2):
                for g in some:
                    y_steps = lax.dynamic_update_slice(y_steps, pieces[g][k], (half * lax.rem(core + k, 2), GROUPS[g][0] * rows, 0))
        ssm_out, conv_out = states
        ssm_fin = jnp.transpose(ssm_out.reshape(batch, state, inner), (0, 2, 1))
        return y_steps, jnp.transpose(conv_out, (1, 2, 0)), ssm_fin

    return jax.shard_map(layer_steps, mesh=mesh, in_specs=in_specs, out_specs=out_specs, check_vma=False)
```

```python
import functools

import jax
import jax.numpy as jnp
from jax import lax
from jax.experimental import pallas as pl
from jax.experimental.pallas import tpu as pltpu
from jax.sharding import PartitionSpec as P


EPSILON = 1e-6
CHUNKS = 4
ROW_ALIGN = 16
TILE = 128
FEW = 32
GROUPS = ((0, 1), (2,), (3,))
LAST = len(GROUPS) - 1
LISTED = 32
ACTIVE = 33
RING = 6
WHOLE = 2
F32 = jnp.float32
BF16 = jnp.bfloat16
HBM = pl.BlockSpec(memory_space=pl.ANY)


def whole(shape):
    return pl.BlockSpec(shape, lambda *_: (0,) * len(shape))


def params(**kw):
    return pltpu.CompilerParams(vmem_limit_bytes=56 * 1024 * 1024, **kw)


def row(ref):
    return ref[...].astype(F32).reshape(1, -1)


def norm_rows(v, gain):
    return v * lax.rsqrt(jnp.mean(v * v, axis=-1, keepdims=True) + EPSILON) * gain


def mm_t(a, b):
    return lax.dot_general(a, b, (((1,), (1,)), ((), ())), preferred_element_type=F32)


def silu(v):
    return v * jax.nn.sigmoid(v)


def routes_kernel(ids_ref, pos_ref, tab_ref):
    _, _, tokens = pos_ref.shape
    steps = ids_ref.shape[0]
    rows = tokens // steps
    experts = 16
    upper = (lax.broadcasted_iota(jnp.int32, (tokens, tokens), 0) <= lax.broadcasted_iota(jnp.int32, (tokens, tokens), 1)).astype(F32).astype(BF16)
    before = (lax.broadcasted_iota(jnp.int32, (experts, experts), 1) < lax.broadcasted_iota(jnp.int32, (experts, experts), 0)).astype(F32).astype(BF16)
    lane = lax.broadcasted_iota(jnp.int32, (experts, 128), 1)
    number = lax.broadcasted_iota(jnp.int32, (experts, 128), 0).astype(F32)
    for g, k, c in [(g, k, c) for g, group in enumerate(GROUPS) for k, c in enumerate(group)]:
        ids = jnp.concatenate([ids_ref[s, :, c * rows:(c + 1) * rows] for s in range(steps)], axis=1)
        hit = lax.broadcasted_iota(jnp.int32, (experts, tokens), 0) == ids
        hot = hit.astype(F32)
        rank = jnp.dot(hot.astype(BF16), upper, preferred_element_type=F32)
        count = jnp.broadcast_to(jnp.sum(hot, axis=1, keepdims=True), (experts, 128))
        blocks = jnp.floor((count + (ROW_ALIGN - 1)) * (1.0 / ROW_ALIGN))
        start = ROW_ALIGN * jnp.dot(before, blocks.astype(BF16), preferred_element_type=F32)
        pos_ref[c] = jnp.sum(hot * (start[:, :1] + rank - 1.0), axis=0, keepdims=True).astype(jnp.int32)
        tab_ref[g, 16 * k:16 * k + 16, :] = jnp.where(lane == 0, start, count).astype(jnp.int32)
        total = count if k == 0 else total + count
        if c == GROUPS[g][-1]:
            active = (total > 0.0).astype(F32)
            place = jnp.dot(before, active.astype(BF16), preferred_element_type=F32)
            listed = jnp.sum(jnp.where((place == lane.astype(F32)) & (active > 0.0), number, 0.0), axis=0, keepdims=True)
            tab_ref[g, LISTED:LISTED + 1, :] = listed.astype(jnp.int32)
            tab_ref[g, ACTIVE:ACTIVE + 1, :] = jnp.sum(active, axis=0, keepdims=True).astype(jnp.int32)


LOG2E = 1.4426950408889634


def mamba_kernel(x_hbm, cs_hbm, h_hbm, g_ref, win3_ref, cw_ref, cb_ref, wxp_ref, gdt_ref, gb_ref, gc_ref, wdt_ref, bdt_ref, alog_ref, dskip_ref, wout_ref,
                 uo_hbm, us_hbm, chip2_hbm, chip3_hbm, co_hbm, ho_hbm,
                 x_s, cs_s, co_s, h_s, xc_s, z_s, p_s, m_s, u_s, win_ref, g4_ref, wdt4, ones_s, a_s, q_s, delta_s, dx_s, y_s,
                 in_sem, h_sem, out_sem, ho_sem, psend, precv, msend, mrecv):
    steps, batch, _ = x_s.shape
    inner = cs_s.shape[2]
    state = alog_ref.shape[0]
    rank = wdt_ref.shape[0]
    width = rank + 2 * state
    lanes = steps * width
    half = steps // 2
    rows = batch // CHUNKS
    tiles = inner // 128
    me = lax.axis_index("tp")
    core = lax.rem(me, 2)
    sibling = me + 1 - 2 * core
    partner = lax.rem(me + 2, 4)

    barrier = pltpu.get_barrier_semaphore()
    for peer in (sibling, partner):
        pl.semaphore_signal(barrier, inc=1, device_id={"tp": peer}, device_id_type=pl.DeviceIdType.MESH)

    def span(c):
        return pl.ds(c * rows, rows)

    def loads(c):
        return [
            pltpu.make_async_copy(x_hbm.at[:, span(c), :], x_s.at[:, span(c), :], in_sem.at[0, c]),
            pltpu.make_async_copy(cs_hbm.at[:, span(c), :], cs_s.at[:, span(c), :], in_sem.at[1, c]),
        ]

    def state_rows(c):
        return pl.ds(c * rows * state, rows * state)

    def h_loads(c):
        return [pltpu.make_async_copy(h_hbm.at[state_rows(c), pl.ds(l * 128, 128)], h_s.at[l, state_rows(c), :], h_sem.at[l, c]) for l in range(tiles)]

    def h_stores(c):
        return [pltpu.make_async_copy(h_s.at[l, state_rows(c), :], ho_hbm.at[state_rows(c), pl.ds(l * 128, 128)], ho_sem.at[l, c]) for l in range(tiles)]

    def co_store(c):
        return pltpu.make_async_copy(co_s.at[:, span(c), :], co_hbm.at[:, span(c), :], out_sem.at[0, c])

    def remote(buf, c, src, dst, send, recv, stage, peer):
        return pltpu.make_async_remote_copy(
            src_ref=buf.at[src, c], dst_ref=buf.at[dst, c], send_sem=send.at[stage, c], recv_sem=recv.at[stage, c],
            device_id={"tp": peer}, device_id_type=pl.DeviceIdType.MESH)

    def p_beside(c):
        return remote(p_s, c, 1, 2, psend, precv, 0, sibling)

    def p_across(c):
        return remote(p_s, c, 3, 4, psend, precv, 1, partner)

    def p_back(c):
        return remote(p_s, c, 5, 6, psend, precv, 2, sibling)

    def m_beside(c):
        return remote(m_s, c, 1, 2, msend, mrecv, 0, sibling)

    def m_across(c):
        return remote(m_s, c, 3, 4, msend, mrecv, 1, partner)

    def u_back(c):
        return pltpu.make_async_remote_copy(
            src_ref=u_s.at[0, c], dst_ref=u_s.at[1, c], send_sem=msend.at[2, c], recv_sem=mrecv.at[2, c],
            device_id={"tp": sibling}, device_id_type=pl.DeviceIdType.MESH)

    for c in range(CHUNKS):
        for cp in loads(c):
            cp.start()
    for c in range(CHUNKS):
        for cp in h_loads(c):
            cp.start()

    gain = row(g_ref)
    for k in range(2):
        win_ref[:, k * inner:(k + 1) * inner] = win3_ref[:, k, :]

    def project(c):
        for cp in loads(c):
            cp.wait()

        def block(i, carry):
            r = pl.multiple_of(c * rows + i * 128, 128)
            seq = [cs_s[j, pl.ds(r, 128), :].astype(F32) for j in range(3)]
            part = []
            for s in range(steps):
                x = x_s[s, pl.ds(r, 128), :].astype(F32)
                n = norm_rows(x, gain).astype(BF16)
                xz = jnp.dot(n, win_ref[...], preferred_element_type=F32).astype(BF16)
                z_s[s, pl.ds(r, 128), :] = xz[:, inner:]
                xi = xz[:, :inner]
                if s > 0:
                    co_s[s - 1, pl.ds(r, 128), :] = xi
                seq.append(xi.astype(F32))
                acc = seq[s] * cw_ref[0:1, :].astype(F32)
                for j in range(1, 4):
                    acc = acc + seq[s + j] * cw_ref[j:j + 1, :].astype(F32)
                xc = silu(acc + row(cb_ref)).astype(BF16)
                xc_s[s, pl.ds(r, 128), :] = xc
                part.append(mm_t(xc, wxp_ref[...]))
            low = jnp.concatenate(part[:2], axis=1)
            high = jnp.concatenate(part[2:], axis=1)
            q = pl.multiple_of(i * 128, 128)
            p_s[0, c, pl.ds(q, 128), :] = jnp.where(core == 0, low, high)
            p_s[1, c, pl.ds(q, 128), :] = jnp.where(core == 0, high, low)
            return carry

        lax.fori_loop(0, rows // 128, block, 0)
        co_store(c).start()

    def p_sum(c):
        p_beside(c).wait_recv()
        p_s[3, c] = p_s[0, c] + p_s[2, c]
        p_across(c).start()

    def p_whole(c):
        p_across(c).wait_recv()
        p_s[5, c] = p_s[3, c] + p_s[4, c]
        p_back(c).start()

    def scan(c, between=None):
        p_back(c).wait_recv()
        for cp in h_loads(c):
            cp.wait()

        def block(i, carry):
            r = pl.multiple_of(i * 128, 128)
            g = pl.multiple_of(c * rows + i * 128, 128)
            own, sib = p_s[5, c, pl.ds(r, 128), :], p_s[6, c, pl.ds(r, 128), :]
            p = jnp.concatenate([jnp.where(core == 0, own, sib), jnp.where(core == 0, sib, own)], axis=1)
            sq = p * p
            s1 = sq.astype(BF16)
            rest = sq - s1.astype(F32)
            s2 = rest.astype(BF16)
            s3 = (rest - s2.astype(F32)).astype(BF16)
            mean = sum(jnp.dot(v, ones_s[...], preferred_element_type=F32) for v in (s3, s2, s1))
            norm = p * lax.rsqrt(mean + EPSILON) * g4_ref[...]
            for s in range(steps):
                first = s * width + rank
                q_s[s] = jnp.concatenate([norm[:, first:first + 2 * state], jnp.zeros((128, 128 - 2 * state), F32)], axis=1)
            pre = jnp.dot(norm.astype(BF16), wdt4[...], preferred_element_type=F32)
            bias = row(bdt_ref)
            for s in range(steps):
                v = pre[:, s * inner:(s + 1) * inner] + bias
                delta = jnp.maximum(v, 0.0) + jnp.log1p(jnp.exp(-jnp.abs(v)))
                delta_s[s] = delta
                dx_s[s] = delta * xc_s[s, pl.ds(g, 128), :].astype(F32)

            def tile(t, carry2):
                b = pl.multiple_of(t * 8, 8)
                base = (g + b) * state
                cut = [slice(l * 128, (l + 1) * 128) for l in range(tiles)]
                dl = [[delta_s[s, pl.ds(b, 8), k] for k in cut] for s in range(steps)]
                dx = [[dx_s[s, pl.ds(b, 8), k] for k in cut] for s in range(steps)]
                qs = [q_s[s, pl.ds(b, 8), :] for s in range(steps)]
                ys = [[None] * tiles for _ in range(steps)]
                for n in range(state):
                    bs = [jnp.broadcast_to(qs[s][:, n:n + 1], (8, 128)) for s in range(steps)]
                    cs = [jnp.broadcast_to(qs[s][:, n + state:n + state + 1], (8, 128)) for s in range(steps)]
                    for l in range(tiles):
                        a = a_s[n:n + 1, cut[l]]
                        spot = (l, pl.ds(base + n, 8, stride=state))
                        h = h_s[spot]
                        for s in range(steps):
                            h = jnp.exp2(dl[s][l] * a) * h + dx[s][l] * bs[s]
                            hc = h * cs[s]
                            ys[s][l] = hc if n == 0 else ys[s][l] + hc
                        h_s[spot] = h
                for s in range(steps):
                    for l in range(tiles):
                        y_s[s, pl.ds(b, 8), cut[l]] = ys[s][l]
                return carry2

            lax.fori_loop(0, 16, tile, 0, unroll=2)
            for s in range(steps):
                xc = xc_s[s, pl.ds(g, 128), :].astype(F32)
                yg = ((y_s[s] + row(dskip_ref) * xc) * silu(z_s[s, pl.ds(g, 128), :].astype(F32))).astype(BF16)
                out = jnp.dot(yg, wout_ref[...], preferred_element_type=F32).astype(BF16)
                m_s[lax.rem(core + s // half, 2), c, s % half, pl.ds(r, 128), :] = out
            return carry

        if between is None:
            lax.fori_loop(0, rows // 128, block, 0)
        else:
            lax.fori_loop(0, 1, block, 0)
            between()
            lax.fori_loop(1, rows // 128, block, 0)
        for cp in h_stores(c):
            cp.start()
        m_beside(c).start()

    def chip_out(c):
        return pltpu.make_async_copy(m_s.at[3, c], (chip2_hbm, chip3_hbm)[c - WHOLE], out_sem.at[1, c])

    def m_sum(c):
        m_beside(c).wait_recv()
        for s in range(half):
            m_s[3, c, s] = (m_s[0, c, s].astype(F32) + m_s[2, c, s].astype(F32)).astype(BF16)
        if c < WHOLE:
            m_across(c).start()
        else:
            chip_out(c).start()

    def uo_out(c):
        return pltpu.make_async_copy(u_s.at[0, c], uo_hbm.at[:, span(c), :], out_sem.at[1, c])

    def us_out(c):
        return pltpu.make_async_copy(u_s.at[1, c], us_hbm.at[:, span(c), :], out_sem.at[2, c])

    def m_whole(c):
        m_across(c).wait_recv()
        for s in range(half):
            x = x_s[core * half + s, span(c), :].astype(F32)
            u_s[0, c, s] = (x + (m_s[3, c, s].astype(F32) + m_s[4, c, s].astype(F32))).astype(BF16)
        u_back(c).start()
        uo_out(c).start()

    project(0)
    pl.semaphore_wait(barrier, 2)
    p_beside(0).start()
    project(1)
    p_beside(1).start()
    p_sum(0)
    project(2)
    p_beside(2).start()
    p_sum(1)
    project(3)
    p_beside(3).start()
    p_sum(2)
    p_whole(0)

    wdt4[...] = jnp.zeros_like(wdt4)
    for s in range(steps):
        wdt4[s * width:s * width + rank, s * inner:(s + 1) * inner] = wdt_ref[...]

    def group(v):
        step, col = v // width, lax.rem(v, width)
        return step * 4 + (col >= rank).astype(jnp.int32) + (col >= rank + state).astype(jnp.int32)

    gi = group(lax.broadcasted_iota(jnp.int32, (lanes, lanes), 0))
    gj = group(lax.broadcasted_iota(jnp.int32, (lanes, lanes), 1))
    inv = jnp.where(lax.rem(gj, 4) == 0, 1.0 / rank, 1.0 / state)
    ones_s[...] = jnp.where(gi == gj, inv, 0.0).astype(BF16)
    for s in range(steps):
        for ref, at in ((gdt_ref, 0), (gb_ref, rank), (gc_ref, rank + state)):
            g4_ref[:, s * width + at:s * width + at + ref.shape[0]] = row(ref)
    a_s[...] = -LOG2E * jnp.exp(alog_ref[...])

    p_sum(3)
    scan(0)
    p_whole(1)
    p_whole(2)
    m_sum(0)
    p_whole(3)
    scan(1)
    m_sum(1)
    scan(2)
    m_sum(2)
    m_whole(0)
    scan(3, lambda: m_whole(1))
    m_sum(3)
    for c in range(WHOLE):
        u_back(c).wait_recv()
        us_out(c).start()
    for c in range(CHUNKS):
        p_beside(c).wait_send()
        p_across(c).wait_send()
        p_back(c).wait_send()
        m_beside(c).wait_send()
        co_store(c).wait()
        for cp in h_stores(c):
            cp.wait()
        if c < WHOLE:
            m_across(c).wait_send()
            u_back(c).wait_send()
            uo_out(c).wait()
            us_out(c).wait()
        else:
            chip_out(c).wait()


def moe_kernel(g, size, *refs):
    count_in = 2 + 2 * size
    tab_ref, pos_ref = refs[:2]
    us = refs[2:count_in]
    gff_ref, wr_ref, wg_ref, wu_ref, wd_ref, h_hbm, cv_hbm = refs[count_in:count_in + 7]
    refs = refs[count_in + (9 if g else 7):]
    outs = refs[:2]
    ho_hbm, co_hbm = refs[2:4]
    wg, wu, wd, sems, m_s, hot_s, in_s, out_s, prob_s, h_s, cv_s, st_sem = refs[-12:]
    half, rows, d_model = us[0].shape
    experts = wr_ref.shape[0]
    tokens = 2 * half * rows
    slots = hot_s.shape[0] // size
    room = in_s.shape[0] // size
    core = lax.rem(lax.axis_index("tp"), 2)
    active = tab_ref[0, ACTIVE, 0]

    def copies(i):
        e = tab_ref[0, LISTED, i]
        slot = lax.rem(i, RING)
        return [pltpu.make_async_copy(src.at[e], dst.at[slot], sems.at[k, slot]) for k, (src, dst) in enumerate(((wg_ref, wg), (wu_ref, wu), (wd_ref, wd)))]

    def fetch(i):
        @pl.when(i < active)
        def _():
            for cp in copies(i):
                cp.start()

    for i in range(RING - 1):
        fetch(i)
    h_span = pl.ds(GROUPS[g][0] * h_s.shape[0] // size, h_s.shape[0])
    cv_span = pl.ds(GROUPS[g][0] * cv_s.shape[1] // size, cv_s.shape[1])
    pulls = [pltpu.make_async_copy(h_hbm.at[h_span, :], h_s, st_sem.at[0]), pltpu.make_async_copy(cv_hbm.at[:, cv_span, :], cv_s, st_sem.at[1])]
    pushes = [pltpu.make_async_copy(h_s, ho_hbm.at[h_span, :], st_sem.at[2]), pltpu.make_async_copy(cv_s, co_hbm.at[:, cv_span, :], st_sem.at[3])]
    for cp in pulls:
        cp.start()
    gain = row(gff_ref)
    for j in range(size):
        for k in range(2):
            src = us[k * size + j]
            first = j * tokens + jnp.where(core == k, 0, half * rows)
            for s in range(half):
                u = src[s].astype(F32)
                m = norm_rows(u, gain)
                m_s[pl.ds(pl.multiple_of(first + s * rows, rows), rows), :] = m.astype(BF16)

    down = lax.broadcasted_iota(jnp.int32, (256, tokens), 0).astype(F32).astype(BF16)
    for j in range(size):
        pos = pos_ref[j]

        def order(i, carry):
            r = pl.multiple_of(i * 256, 256)
            local = jnp.where((pos >= r) & (pos < r + 256), pos - r, -1).astype(F32).astype(BF16)
            hot = jnp.where(down == local, jnp.ones((), BF16), jnp.zeros((), BF16))
            hot_s[pl.ds(j * slots + r, 256), :] = hot
            m = jnp.dot(hot, m_s[j * tokens:(j + 1) * tokens, :], preferred_element_type=F32).astype(BF16)
            at = pl.ds(j * room + r, 256)
            in_s[at, :] = m
            out_s[at, :] = jnp.zeros((256, d_model), BF16)
            logits = mm_t(m, wr_ref[...])
            ex = jnp.exp(logits - jnp.max(logits, axis=-1, keepdims=True))
            prob_s[at, :] = ex / jnp.sum(ex, axis=-1, keepdims=True)
            return carry

        lax.fori_loop(0, slots // 256, order, 0, unroll=True)
    for pull, push in zip(pulls, pushes):
        pull.wait()
        push.start()

    def feed(e, slot, r, size):
        m = in_s[pl.ds(r, size), :]
        gate = jnp.dot(m, wg[slot], preferred_element_type=F32)
        up = jnp.dot(m, wu[slot], preferred_element_type=F32)
        q = (silu(gate) * up).astype(BF16)
        lane = lax.broadcasted_iota(jnp.int32, (size, experts), 1)
        prob = jnp.sum(jnp.where(lane == e, prob_s[pl.ds(r, size), :], 0.0), axis=-1, keepdims=True)
        out_s[pl.ds(r, size), :] = (prob * jnp.dot(q, wd[slot], preferred_element_type=F32)).astype(BF16)

    def expert(i, carry):
        e = tab_ref[0, LISTED, i]
        slot = lax.rem(i, RING)
        fetch(i + RING - 1)
        for cp in copies(i):
            cp.wait()

        def part(j, c1):
            start = tab_ref[0, 16 * j + e, 0] + j * room
            count = tab_ref[0, 16 * j + e, 1]
            big = (count + TILE - 1) // (2 * TILE)

            def tile(k, c2):
                feed(e, slot, pl.multiple_of(start + k * (2 * TILE), ROW_ALIGN), 2 * TILE)
                return c2

            lax.fori_loop(0, big, tile, 0)

            left = count - big * (2 * TILE)
            for most, least in ((TILE, FEW), (FEW, 0)):
                @pl.when((left > least) & (left <= most))
                def _():
                    feed(e, slot, pl.multiple_of(start + big * (2 * TILE), ROW_ALIGN), most)

            return c1

        return lax.fori_loop(0, size, part, carry)

    lax.fori_loop(0, active, expert, 0)

    def restore(j, k, dst):
        first = jnp.where(core == k, 0, half * rows)
        for s in range(half):
            hot = hot_s[j * slots:(j + 1) * slots, pl.ds(pl.multiple_of(first + s * rows, rows), rows)]
            got = lax.dot_general(hot, out_s[j * room:j * room + slots, :], (((0,), (0,)), ((), ())), preferred_element_type=F32)
            dst[s, j * rows:(j + 1) * rows, :] = got.astype(BF16)

    for j in range(size):
        for k in range(2):
            restore(j, k, outs[k])
    for cp in pushes:
        cp.wait()


def solution(mesh):
    act_spec = P(None, "dp", None)
    state_spec = P("dp", "tp", None)
    in_specs = (act_spec, state_spec, state_spec, act_spec, P(None), P(None, None, "tp"), P("tp", None), P("tp"), P("tp", None), P(None), P(None), P(None), P(None, "tp"), P("tp"), P("tp", None), P("tp"), P("tp", None), P(None), P(None, None), P(None, None, "tp"), P(None, None, "tp"), P(None, "tp", None))
    out_specs = (act_spec, state_spec, state_spec)
    across = [(0, 2), (2, 0), (1, 3), (3, 1)]
    beside = [(0, 1), (1, 0), (2, 3), (3, 2)]

    def layer_steps(x_steps, conv_state, ssm_state, expert_ids, g_in, w_in, conv_w, conv_b, w_xp, g_dt, g_b, g_c, w_dt, b_dt, a_log, d_skip, w_out, g_ff, w_router, w_gate, w_up, w_down):
        steps, batch, d_model = x_steps.shape
        inner = w_in.shape[2]
        rank = w_dt.shape[0]
        state = a_log.shape[1]
        experts, _, ffn = w_gate.shape
        width = rank + 2 * state
        half = steps // 2
        rows = batch // CHUNKS
        tokens = steps * rows
        slots = tokens + experts * ROW_ALIGN
        core = lax.rem(lax.axis_index("tp"), 2)

        conv_t = jnp.transpose(conv_state, (2, 0, 1))
        h_rows = jnp.transpose(ssm_state, (0, 2, 1)).reshape(batch * state, inner)
        alog_t = a_log.T

        ids = jnp.transpose(expert_ids, (0, 2, 1))
        pos, table = pl.pallas_call(
            routes_kernel,
            out_shape=(jax.ShapeDtypeStruct((CHUNKS, 1, tokens), jnp.int32), jax.ShapeDtypeStruct((len(GROUPS), ACTIVE + 7, 128), jnp.int32)),
            compiler_params=params(),
            name="routes",
        )(ids)

        vmem = pl.BlockSpec(memory_space=pltpu.VMEM)
        piece = (half, rows, d_model)
        u_first, u_second, *chips, conv_mid, h_mid = pl.pallas_call(
            mamba_kernel,
            in_specs=[HBM, HBM, HBM] + [vmem] * 13,
            out_specs=[HBM] * 6,
            out_shape=[
                jax.ShapeDtypeStruct((half, WHOLE * rows, d_model), BF16),
                jax.ShapeDtypeStruct((half, WHOLE * rows, d_model), BF16),
                jax.ShapeDtypeStruct(piece, BF16),
                jax.ShapeDtypeStruct(piece, BF16),
                jax.ShapeDtypeStruct((3, batch, inner), BF16),
                jax.ShapeDtypeStruct((batch * state, inner), F32),
            ],
            scratch_shapes=[
                pltpu.VMEM((steps, batch, d_model), BF16),
                pltpu.VMEM((3, batch, inner), BF16),
                pltpu.VMEM((3, batch, inner), BF16),
                pltpu.VMEM((inner // 128, batch * state, 128), F32),
                pltpu.VMEM((steps, batch, inner), BF16),
                pltpu.VMEM((steps, batch, inner), BF16),
                pltpu.VMEM((7, CHUNKS, rows, 2 * width), F32),
                pltpu.VMEM((5, CHUNKS) + piece, BF16),
                pltpu.VMEM((2, CHUNKS) + piece, BF16),
                pltpu.VMEM((d_model, 2 * inner), BF16),
                pltpu.VMEM((1, steps * width), F32),
                pltpu.VMEM((steps * width, steps * inner), BF16),
                pltpu.VMEM((steps * width, steps * width), BF16),
                pltpu.VMEM((state, inner), F32),
                pltpu.VMEM((steps, 128, 128), F32),
                pltpu.VMEM((steps, 128, inner), F32),
                pltpu.VMEM((steps, 128, inner), F32),
                pltpu.VMEM((steps, 128, inner), F32),
                pltpu.SemaphoreType.DMA((2, CHUNKS)),
                pltpu.SemaphoreType.DMA((inner // 128, CHUNKS)),
                pltpu.SemaphoreType.DMA((3, CHUNKS)),
                pltpu.SemaphoreType.DMA((inner // 128, CHUNKS)),
                pltpu.SemaphoreType.DMA((3, CHUNKS)),
                pltpu.SemaphoreType.DMA((3, CHUNKS)),
                pltpu.SemaphoreType.DMA((3, CHUNKS)),
                pltpu.SemaphoreType.DMA((3, CHUNKS)),
            ],
            compiler_params=params(collective_id=0, has_side_effects=True),
            cost_estimate=pl.CostEstimate(flops=int(8e9), bytes_accessed=int(45e6), transcendentals=0),
            name="mamba",
        )(x_steps, conv_t, h_rows, g_in, w_in, conv_w.T, conv_b, w_xp.T, g_dt, g_b, g_c, w_dt, b_dt, alog_t, d_skip, w_out)

        room = slots + 2 * TILE

        def run_moe(g, u_args, u_specs, states):
            extra = [] if states is None else list(states)
            size = len(GROUPS[g])
            first = GROUPS[g][0] // size
            count_in = 2 + 2 * size
            return pl.pallas_call(
                functools.partial(moe_kernel, g, size),
                grid=(1,),
                in_specs=[pl.BlockSpec((1, ACTIVE + 7, 128), lambda i: (g, 0, 0), memory_space=pltpu.SMEM), pl.BlockSpec((size, 1, tokens), lambda i: (first, 0, 0))] + u_specs + [vmem, vmem] + [HBM] * (5 + len(extra)),
                out_specs=[vmem] * 2 + [HBM, HBM] + ([] if extra else [HBM]),
                out_shape=[jax.ShapeDtypeStruct((half, size * rows, d_model), BF16)] * 2 + [jax.ShapeDtypeStruct(h_mid.shape, F32), jax.ShapeDtypeStruct(conv_mid.shape, BF16)] + ([] if extra else [jax.ShapeDtypeStruct(x_steps.shape, BF16)]),
                scratch_shapes=[
                    pltpu.VMEM((RING, d_model, ffn), BF16),
                    pltpu.VMEM((RING, d_model, ffn), BF16),
                    pltpu.VMEM((RING, ffn, d_model), BF16),
                    pltpu.SemaphoreType.DMA((3, RING)),
                    pltpu.VMEM((size * tokens, d_model), BF16),
                    pltpu.VMEM((size * slots, tokens), BF16),
                    pltpu.VMEM((size * room, d_model), BF16),
                    pltpu.VMEM((size * room, d_model), BF16),
                    pltpu.VMEM((size * room, experts), F32),
                    pltpu.VMEM((size * rows * state, inner), F32),
                    pltpu.VMEM((3, size * rows, inner), BF16),
                    pltpu.SemaphoreType.DMA((4,)),
                ],
                input_output_aliases={count_in + 7: 2, count_in + 8: 3} if extra else {},
                compiler_params=params(),
                cost_estimate=pl.CostEstimate(flops=int(3e9) * size, bytes_accessed=int(40e6), transcendentals=0),
            )(table, pos, *u_args, g_ff, w_router.T, w_gate, w_up, w_down, h_mid, conv_mid, *extra)

        def both(keep, send, dtype):
            got = lax.ppermute(send, "tp", beside)
            chip = (keep.astype(F32) + got.astype(F32)).astype(dtype)
            return chip, lax.ppermute(chip, "tp", across)

        spot = {c: (u_first, u_second, pl.BlockSpec(piece, lambda i, c=c: (0, c, 0))) for c in range(WHOLE)}
        for c in range(WHOLE, CHUNKS):
            chip = chips[c - WHOLE]
            far = lax.ppermute(chip, "tp", across)
            x_own = lax.dynamic_slice(x_steps, (half * core, c * rows, 0), (half, rows, d_model))
            u_own = (x_own.astype(F32) + (chip.astype(F32) + far.astype(F32))).astype(BF16)
            u_sib = lax.ppermute(u_own, "tp", beside)
            spot[c] = (u_own, u_sib, whole(piece))

        states = None
        pieces = {}
        for g, members in enumerate(GROUPS):
            group = [spot[c] for c in members]
            got = run_moe(g, [v[0] for v in group] + [v[1] for v in group], [v[2] for v in group] * 2, states)
            states = got[2:4]
            if g == 0:
                y_steps = got[-1]
            chip, far = both(got[0], got[1], BF16)
            y_own = (group[0][0].astype(F32) + (chip.astype(F32) + far.astype(F32))).astype(BF16)
            pieces[g] = (y_own, lax.ppermute(y_own, "tp", beside))
        for some in (range(LAST), (LAST,)):
            for k in range(2):
                for g in some:
                    y_steps = lax.dynamic_update_slice(y_steps, pieces[g][k], (half * lax.rem(core + k, 2), GROUPS[g][0] * rows, 0))
        ssm_out, conv_out = states
        ssm_fin = jnp.transpose(ssm_out.reshape(batch, state, inner), (0, 2, 1))
        return y_steps, jnp.transpose(conv_out, (1, 2, 0)), ssm_fin

    return jax.shard_map(layer_steps, mesh=mesh, in_specs=in_specs, out_specs=out_specs, check_vma=False)
```
